256 devices in a mesh: level: 2 (over core), gx: 4 (over x), yz: 32 (over z, y).
Axes of the slice: x: 4, y: 4, z: 8, core: 2. Of those that a mesh axis runs over, the one named last changes fastest.
Arguments:
- init_field: float32 [128, 512, 256], P('gx', 'yz'), may hold values from -6 to 6
- source: float32 [128, 512, 256], P('gx', 'yz'), may hold values from -4 to 4
- damping: float32 [128, 512, 256], P('gx', 'yz'), may hold values from 0.05 to 2
Outputs:
- final_states: float32 [2, 128, 512, 256], P('level', 'gx', 'yz')
The draws below stay inside these ranges and needn't reach their ends.
All inputs are finite; a program needn't handle non-finite values.
Results may differ from the reference program's by a relative error of at most 0.0001.
Values sent between devices are 32-bit elements; how exact they have to be, the bound alone decides.
No kernel may reach another device: no remote copies, remote signals or barrier semaphores. Data moves between devices by JAX's collectives and lax.ppermute only.
A program may use at most 64 MiB of HBM per device.

```python
import math
import jax
import jax.numpy as jnp

STEPS = 3
ITERS = 3
NX = 128
NY = 512
NZ = 256


def block_scale(rng, extent, split, low, high):
    level, own = 1.0, jax.random.fold_in(rng, 6)
    for position, parts in split:
        steps = jnp.exp(jax.random.uniform(jax.random.fold_in(own, position), (parts,), jnp.float32, low / len(split), high / len(split)))
        level = level * jnp.repeat(steps, extent[position] // parts).reshape([-1 if axis == position else 1 for axis in range(len(extent))])
    return level


def noise(stream_key, shape, deviation, most, shards=(), dtype=jnp.bfloat16):
    gain = block_scale(stream_key, shape, shards, -0.22, 0.18) if shards else 1.0
    array = jax.random.normal(stream_key, shape, jnp.float32) * deviation * gain
    return jnp.minimum(jnp.maximum(array, -most), most).astype(dtype)


def setup_inputs(seed: int = 0) -> dict:
    keys = jax.random.split(jax.random.key(seed), 4)
    init_field = noise(keys[0], (NX, NY, NZ), 1.0, 6.0, ((0, 4), (1, 32)), jnp.float32)
    source = noise(keys[1], (NX, NY, NZ), 0.5, 4.0, ((0, 4), (1, 32)), jnp.float32)
    damping = jnp.clip(jnp.exp(math.log(2.0) - 3.6888794 * jax.random.uniform(keys[2], (NX, NY, NZ), jnp.float32) ** block_scale(keys[2], (NX, NY, NZ), ((0, 4), (1, 32)), -0.2, 0.2)), 0.05, 2.0)
    return dict(init_field=init_field, source=source, damping=damping)


diffusion_number = 1.0


def stencil(field, damping):
    padded = jnp.pad(field, 1)
    beside = padded[2:, 1:-1, 1:-1] + padded[:-2, 1:-1, 1:-1]
    beside = beside + padded[1:-1, 2:, 1:-1] + padded[1:-1, :-2, 1:-1]
    beside = beside + padded[1:-1, 1:-1, 2:] + padded[1:-1, 1:-1, :-2]
    return damping * field + diffusion_number * (6.0 * field - beside)


def solve(target, guess, damping):
    answer = guess
    resid = target - (answer + stencil(answer, damping))
    direction = resid
    norm_now = jnp.sum(resid * resid)
    for step in range(ITERS):
        image = direction + stencil(direction, damping)
        alpha = norm_now / jnp.sum(direction * image)
        answer = answer + alpha * direction
        resid = resid - alpha * image
        if step + 1 < ITERS:
            norm_next = jnp.sum(resid * resid)
            direction = resid + (norm_next / norm_now) * direction
            norm_now = norm_next
    return answer


def reference(init_field, source, damping):
    states = [init_field]
    for step in range(STEPS):
        states.append(solve(states[-1] + source, states[-1], damping))
    corrected = init_field
    for step in range(STEPS):
        extra = 0.5 * stencil(states[step + 1] - states[step], damping)
        corrected = solve(corrected + source + extra, corrected, damping)
    return jnp.stack([states[-1], corrected])
```

```python
import math

import jax
import jax.numpy as jnp
import numpy as np
from jax import lax
from jax.experimental import pallas as pl
from jax.experimental.pallas import tpu as pltpu
from jax.sharding import PartitionSpec as P

STEPS = 3
ITERS = 3
DIFFUSION = 1.0
CENTRE, RADIUS = 8.0, 7.0
HALF = 6
TOP = 2 * HALF
MOMENTS = 2 * TOP
NODES = 128
WIDE = HALF + 1
ROWS = 8
NOISE_GAIN = 4.0
ERROR_BOUND = 4e-5

AXES = ("gx", "yz")
CHECK_AT, FIELD_AT = 32, 47
LOW_AT = 64


def chebyshev_tables():
    angle = np.pi * (np.arange(NODES) + 0.5) / NODES
    exact = np.cos(np.arange(32)[:, None] * angle[None])
    first = np.round(exact * 2048.0) / 2048.0
    second = np.round((exact - first) * 2.0**23) / 2.0**23
    parts = np.concatenate([first, second, exact - first - second, exact])
    return parts.astype(np.float32), (CENTRE + RADIUS * exact[1:2]).astype(np.float32)


def total(values):
    return jnp.sum(values, axis=1, keepdims=True)


def two_sum(a, b):
    s = a + b
    t = s - a
    return s, (a - (s - t)) + (b - t)


def plus(a, b):
    s, e = two_sum(a[0], b[0])
    return two_sum(s, e + (a[1] + b[1]))


def times(scale, a):
    return scale * a[0], scale * a[1]


def halves(values):
    wide = 4097.0 * values
    high = wide - (wide - values)
    return high, values - high


def split_sum(values, axis=None):
    count = values.size if axis is None else values.shape[axis]
    most = jnp.max(jnp.abs(values), axis=axis, keepdims=True)
    unit = (4.0 * count) * most
    high = (values + unit) - unit
    return jnp.sum(high, axis=axis, keepdims=True), jnp.sum(values - high, axis=axis, keepdims=True)


def spectral_solve(resid, weight, nodes, noise):
    direction = resid
    answer = jnp.zeros_like(resid)
    norm_now = total(weight * resid * resid)
    noise_now = noise * total(resid * resid)
    error = jnp.zeros_like(norm_now)
    for step in range(ITERS):
        image = nodes * direction
        product = total(weight * direction * image)
        length = total(weight * direction * direction)
        noise_product = noise * total(direction * image)
        alpha = norm_now / product
        error = error + alpha * (noise_now / norm_now + noise_product / product) * jnp.sqrt(length)
        answer = answer + alpha * direction
        resid = resid - alpha * image
        if step + 1 < ITERS:
            norm_next = total(weight * resid * resid)
            noise_now = noise * total(resid * resid)
            direction = resid + (norm_next / norm_now) * direction
            norm_now = norm_next
    return answer, error


def coefficients(high, low, tables, nodes):
    table = tables[96:128]
    place = lax.broadcasted_iota(jnp.int32, (32, 1), 0)
    raw = high[:32], low[:32]
    base = tuple(jnp.where(place % 2 == 0, r[0:1], r[1:2]) for r in raw)
    shifted = plus(times(2.0, raw), times(-1.0, base))
    used = place < MOMENTS
    moment = tuple(jnp.where(used, jnp.where(place < 2, r, m), 0.0) for r, m in zip(raw, shifted))
    factor = jnp.where(place == 0, 1.0 / NODES, 2.0 / NODES)
    big, small = halves(factor * moment[0])
    small = small + factor * moment[1]
    parts = big * tables[:32]
    rest = big * tables[32:64] + small * tables[:32] + (big * tables[64:96] + small * tables[32:64])
    pieces = (parts, rest)
    count = 32
    while count > 1:
        count //= 2
        pieces = plus(tuple(p[:count] for p in pieces), tuple(p[count : 2 * count] for p in pieces))
    weight = pieces[0] + pieces[1]
    worst = jnp.zeros((1, 1), jnp.float32)
    at = lambda pair, k: (pair[0][k : k + 1], pair[1][k : k + 1])
    for k in range(1, TOP):
        gap = plus(times(2.0, at((high, low), CHECK_AT + k)), times(-1.0, at(moment, 2)))
        gap = plus(gap, times(-1.0, at(moment, 2 * k)))
        worst = jnp.maximum(worst, jnp.abs(gap[0] + gap[1]))
    noise = (worst + 1e-10 * high[0:1]) * (NOISE_GAIN / NODES)
    dots = high
    above = nodes - 1.0
    one = jnp.ones_like(nodes)
    path = [jnp.zeros_like(nodes)]
    second = path[0]
    errors = [jnp.zeros((1, 1), jnp.float32), jnp.zeros((1, 1), jnp.float32)]
    for step in range(STEPS):
        change, error = spectral_solve(one - above * path[-1], weight, nodes, noise)
        path.append(path[-1] + change)
        errors[0] = errors[0] + error
    for step in range(STEPS):
        resid = one - above * second + 0.5 * above * (path[step + 1] - path[step])
        change, error = spectral_solve(resid, weight, nodes, noise)
        second = second + change
        errors[1] = errors[1] + error
    results = []
    for values, error in ((path[-1], errors[0]), (second, errors[0] + errors[1])):
        part = total(table[:16] * values) * (2.0 / NODES)
        row = lax.broadcasted_iota(jnp.int32, (16, 1), 0)
        part = jnp.where(row == 0, 0.5 * part, part)
        part = jnp.where(row < TOP, part, 0.0)
        cross = jnp.sum(part * dots[FIELD_AT + 1 : FIELD_AT + 17], axis=0, keepdims=True)
        square = dots[FIELD_AT : FIELD_AT + 1] + 2.0 * cross + total(weight * values * values)
        fine = (error * error <= ERROR_BOUND * ERROR_BOUND * square) & (error >= 0.0)
        results.append((part, fine))
    return results


def pack_rows_kernel(u, f, d, to_high, to_low):
    nx, ny, _ = u.shape
    for n, ref in enumerate((u, f, d)):
        to_high[n * nx : (n + 1) * nx] = ref[:, ny - ROWS :, :]
        to_low[n * nx : (n + 1) * nx] = ref[:, :ROWS, :]


def pack_planes_kernel(u, f, d, low, high, to_high, to_low):
    nx, ny, _ = u.shape
    at = 0
    for n, (ref, width) in enumerate(((u, WIDE), (f, HALF), (d, HALF))):
        for out, start in ((to_high, nx - width), (to_low, 0)):
            out[at : at + width, :ROWS] = low[n * nx + start : n * nx + start + width]
            out[at : at + width, ROWS : ROWS + ny] = ref[start : start + width]
            out[at : at + width, ROWS + ny :] = high[n * nx + start : n * nx + start + width]
        at += width


def pack_vector_kernel(v, low, high, to_high, to_low):
    nx, ny, _ = v.shape
    for out, start in ((to_high, nx - HALF), (to_low, 0)):
        out[:, :ROWS] = low[start : start + HALF]
        out[:, ROWS : ROWS + ny] = v[start : start + HALF]
        out[:, ROWS + ny :] = high[start : start + HALF]


def beside(ref, i):
    here = ref[i]
    lane = lax.broadcasted_iota(jnp.int32, here.shape, 1)
    last = here.shape[1] - 1
    right = jnp.where(lane == last, 0.0, pltpu.roll(here, last, 1))
    left = jnp.where(lane == 0, 0.0, pltpu.roll(here, 1, 1))
    rows = pltpu.roll(here, 1, 0) + pltpu.roll(here, here.shape[0] - 1, 0)
    return here, (ref[i + 1] + ref[i - 1]) + rows + (right + left)


def row_mask(shape, ny):
    row = lax.broadcasted_iota(jnp.int32, shape, 0)
    here, count = lax.axis_index("yz"), lax.axis_size("yz")
    low = jnp.where(here == 0, ROWS, 0)
    high = jnp.where(here == count - 1, ROWS + ny, 2 * ROWS + ny)
    return jnp.where((row >= low) & (row < high), 1.0, 0.0)


def plane_range(nx, halo):
    here, count = lax.axis_index("gx"), lax.axis_size("gx")
    return jnp.where(here == 0, WIDE, WIDE - halo), jnp.where(here == count - 1, WIDE + nx, WIDE + nx + halo)


def put(row, index, values):
    lane = lax.broadcasted_iota(jnp.int32, row.shape, 1)
    high, low = split_sum(values)
    return jnp.where(lane == index, high, jnp.where(lane == index + LOW_AT, low, row))


def own_dots(nx, loads, pairs):
    def body(i, sums):
        planes = loads(i)
        return tuple(s + planes[a] * planes[b] for s, (a, b) in zip(sums, pairs))

    shape = jax.eval_shape(loads, 0)[0].shape
    start = tuple(jnp.zeros(shape, jnp.float32) for _ in pairs)
    return lax.fori_loop(0, nx, body, start, unroll=2)


def first_kernel(u, f, d, ylow, yhigh, xlow, xhigh, basis, scale, to_high, to_low, dots, wide_u, va, vb):
    nx, ny, nz = u.shape
    high = ROWS + ny
    for n, (ref, width, dst) in enumerate(((u, WIDE, wide_u), (d, HALF, scale))):
        at = 0 if n == 0 else WIDE + HALF
        dst[WIDE - width : WIDE] = xlow[at : at + width]
        dst[WIDE + nx : WIDE + nx + width] = xhigh[at : at + width]
        src = 0 if n == 0 else 2 * nx
        dst[WIDE : WIDE + nx, :ROWS] = ylow[src : src + nx]
        dst[WIDE : WIDE + nx, ROWS:high] = ref[...]
        dst[WIDE : WIDE + nx, high:] = yhigh[src : src + nx]
    va[WIDE - HALF : WIDE] = xlow[WIDE : WIDE + HALF]
    va[WIDE + nx : WIDE + nx + HALF] = xhigh[WIDE : WIDE + HALF]
    va[WIDE : WIDE + nx, :ROWS] = ylow[nx : 2 * nx]
    va[WIDE : WIDE + nx, ROWS:high] = f[...]
    va[WIDE : WIDE + nx, high:] = yhigh[nx : 2 * nx]
    none = jnp.zeros((WIDE,) + va.shape[1:], jnp.float32)
    vb[:WIDE] = none
    vb[WIDE + nx :] = none
    va[0] = none[0]
    va[2 * WIDE + nx - 1] = none[0]
    scale[0] = none[0]
    scale[2 * WIDE + nx - 1] = none[0]
    keep = row_mask(va.shape[1:], ny)
    pull = keep * (2.0 / RADIUS * DIFFUSION)

    def start(i, _):
        here, around = beside(wide_u, i)
        damp = scale[i]
        va[i] = keep * (va[i] - (damp * here + DIFFUSION * (6.0 * here - around)))
        scale[i] = keep * ((2.0 / RADIUS) * (damp + (1.0 + 6.0 * DIFFUSION - CENTRE)))
        return 0

    lax.fori_loop(*plane_range(nx, HALF), start, 0)
    row = jnp.zeros((8, 128), jnp.float32)
    now, other = va, vb
    own = pl.ds(ROWS, ny)

    def save(k, ref):
        def body(i, _):
            basis[k, i] = ref[i + WIDE, own, :]
            return 0

        lax.fori_loop(0, nx, body, 0, unroll=4)

    save(0, va)
    s = own_dots(nx, lambda i: (u[i], va[i + WIDE, own, :]), ((0, 0), (0, 1), (1, 1)))
    for at, value in zip((FIELD_AT, FIELD_AT + 1, 0), s):
        row = put(row, at, value)
    for k in range(HALF):
        src, dst = (va, vb) if k % 2 == 0 else (vb, va)
        halo = HALF - 1 - k

        def step(i, _):
            here, around = beside(src, i)
            twice = scale[i] * here - pull * around
            dst[i] = 0.5 * twice if k == 0 else twice - dst[i]
            return 0

        lax.fori_loop(*plane_range(nx, halo), step, 0)
        save(k + 1, dst)
        loads = lambda i: (u[i], src[i + WIDE, own, :], dst[i + WIDE, own, :]) + ((basis[k - 1, i],) if k else ())
        pairs = ((0, 2), (1, 2), (2, 2)) + (((3, 2),) if k else ())
        s = own_dots(nx, loads, pairs)
        where = (FIELD_AT + 2 + k, 2 * k + 1, 2 * k + 2, CHECK_AT + k)
        for at, value in zip(where, s):
            row = put(row, at, value)
    to_high[...] = basis[HALF, :, ny - ROWS :, :]
    to_low[...] = basis[HALF, :, :ROWS, :]
    dots[...] = row


def second_kernel(u, first, scale, ylow, yhigh, xlow, xhigh, before, basis, dots, va, vb, prior):
    _, nx, ny, nz = first.shape
    high = ROWS + ny
    va[WIDE - HALF : WIDE] = xlow[...]
    va[WIDE + nx : WIDE + nx + HALF] = xhigh[...]
    va[WIDE : WIDE + nx, :ROWS] = ylow[...]
    va[WIDE : WIDE + nx, ROWS:high] = first[HALF]
    va[WIDE : WIDE + nx, high:] = yhigh[...]
    none = jnp.zeros((WIDE,) + va.shape[1:], jnp.float32)
    vb[:WIDE] = none
    vb[WIDE + nx :] = none
    keep = row_mask(va.shape[1:], ny)
    pull = keep * (2.0 / RADIUS * DIFFUSION)
    row = before[...]
    own = pl.ds(ROWS, ny)
    for j in range(HALF):
        src, dst = (va, vb) if j % 2 == 0 else (vb, va)

        def step(i, _):
            here, around = beside(src, i)
            twice = scale[i] * here - pull * around
            dst[i] = 0.5 * twice if j == 0 else twice - dst[i]
            return 0

        lax.fori_loop(*plane_range(nx, HALF - 1 - j), step, 0)
        get = lambda k, i: first[k, i] if k <= HALF else basis[k - HALF - 1, i]
        k = HALF + j

        def body(i, sums):
            new = 2.0 * dst[i + WIDE, own, :] - first[HALF - 1 - j, i]
            if j + 1 < HALF:
                basis[j, i] = new
            terms = [get(k, i) * new, get(k - 1, i) * new]
            if j + 1 < HALF:
                terms += [new * new, u[i] * new]
            return tuple(a + b for a, b in zip(sums, terms))

        count = 4 if j + 1 < HALF else 2
        sums = tuple(jnp.zeros((ny, nz), jnp.float32) for _ in range(count))
        sums = lax.fori_loop(0, nx, body, sums, unroll=2)
        where = (2 * k + 1, CHECK_AT + k, 2 * k + 2, FIELD_AT + 2 + k)
        for at, value in zip(where, sums):
            row = put(row, at, value)
    dots[...] = jnp.broadcast_to(row[0:1], dots.shape)


def finish_kernel(gathered, tables, nodes, u, first, second, out, flag):
    nx, ny, nz = u.shape
    turned = gathered[...].T
    high, low = split_sum(turned[:LOW_AT], 1)
    high, low = two_sum(high, low + total(turned[LOW_AT:]))
    (lower, fine_low), (upper, fine_up) = coefficients(high, low, tables[...], nodes[...])
    level = lax.axis_index("level")
    part = jnp.where(level == 0, lower, upper)
    flag[...] = jnp.broadcast_to(jnp.where(fine_low & fine_up, 1.0, 0.0), flag.shape)
    factors = [jnp.broadcast_to(part[k : k + 1], (8, 128)) for k in range(TOP)]

    def body(i, _):
        for r in range(0, ny, 8):
            for c in range(0, nz, 128):
                at = (i, pl.ds(r, 8), pl.ds(c, 128))
                value = u[at]
                for k in range(TOP):
                    ref, n = (first, k) if k <= HALF else (second, k - HALF - 1)
                    value = value + factors[k] * ref[(n,) + at]
                out[at] = value
        return 0

    lax.fori_loop(0, nx, body, 0)


def call(kernel, outs, args, scratch=(), limit=30 << 20):
    whole = pl.BlockSpec(memory_space=pltpu.VMEM)
    return pl.pallas_call(
        kernel,
        out_shape=[jax.ShapeDtypeStruct(s, jnp.float32) for s in outs],
        in_specs=[whole] * len(args),
        out_specs=[whole] * len(outs),
        scratch_shapes=[pltpu.VMEM(s, jnp.float32) for s in scratch],
        compiler_params=pltpu.CompilerParams(vmem_limit_bytes=limit),
        name=kernel.__name__,
    )(*args)


def both_ways(up, down, axis):
    size = lax.axis_size(axis)
    route = [(i, i + 1) for i in range(size - 1)]
    return lax.ppermute(up, axis, route), lax.ppermute(down, axis, [(b, a) for a, b in route])


def stencil(field, damping):
    low, high = both_ways(field[-1:], field[:1], "gx")
    left, right = both_ways(field[:, -1:], field[:, :1], "yz")
    tall = jnp.concatenate([low, field, high], axis=0)
    long = jnp.concatenate([left, field, right], axis=1)
    zero = jnp.zeros_like(field[:, :, :1])
    near = tall[2:] + tall[:-2] + long[:, 2:] + long[:, :-2]
    near = near + jnp.concatenate([field[:, :, 1:], zero], axis=2) + jnp.concatenate([zero, field[:, :, :-1]], axis=2)
    return damping * field + DIFFUSION * (6.0 * field - near)


def dot(a, b):
    value = jnp.sum(a * b)
    for axis in AXES:
        value = lax.psum(value, axis)
    return value


def solve(target, guess, damping):
    resid = target - (guess + stencil(guess, damping))

    def step(_, state):
        answer, resid, direction, norm_now = state
        image = direction + stencil(direction, damping)
        alpha = norm_now / dot(direction, image)
        answer = answer + alpha * direction
        resid = resid - alpha * image
        norm_next = dot(resid, resid)
        return answer, resid, resid + (norm_next / norm_now) * direction, norm_next

    return lax.fori_loop(0, ITERS, step, (guess, resid, resid, dot(resid, resid)))[0]


def step_by_step(init_field, source, damping):
    def body(_, carry):
        lower, upper = carry
        fresh = solve(lower + source, lower, damping)
        extra = 0.5 * stencil(fresh - lower, damping)
        return fresh, solve(upper + source + extra, upper, damping)

    lower, upper = lax.fori_loop(0, STEPS, body, (init_field, init_field))
    return jnp.where(lax.axis_index("level") == 1, upper, lower)


def per_device(u, f, d):
    nx, ny, nz = u.shape
    tall = 2 * ROWS + ny
    ups, downs = call(pack_rows_kernel, [(3 * nx, ROWS, nz)] * 2, (u, f, d))
    ylow, yhigh = both_ways(ups, downs, "yz")
    edge = (WIDE + 2 * HALF, tall, nz)
    ups, downs = call(pack_planes_kernel, [edge] * 2, (u, f, d, ylow, yhigh))
    xlow, xhigh = both_ways(ups, downs, "gx")
    padded = (nx + 2 * WIDE, tall, nz)
    first, scale, ups, downs, dots = call(
        first_kernel,
        [(HALF + 1, nx, ny, nz), padded, (nx, ROWS, nz), (nx, ROWS, nz), (8, 128)],
        (u, f, d, ylow, yhigh, xlow, xhigh),
        [padded] * 3,
    )
    ylow, yhigh = both_ways(ups, downs, "yz")
    ups, downs = call(pack_vector_kernel, [(HALF, tall, nz)] * 2, (first[HALF], ylow, yhigh))
    xlow, xhigh = both_ways(ups, downs, "gx")
    parts = lax.axis_size(AXES)
    second, dots = call(
        second_kernel,
        [(HALF - 1, nx, ny, nz), (parts, 128)],
        (u, first, scale, ylow, yhigh, xlow, xhigh, dots),
        [padded] * 2 + [(8, 128)],
    )
    gathered = lax.all_to_all(dots.reshape(parts, 1, 128), AXES, 0, 0).reshape(parts, 128)
    tables, nodes = chebyshev_tables()
    fast, flag = call(
        finish_kernel,
        [(nx, ny, nz), (8, 128)],
        (gathered, jnp.asarray(tables), jnp.asarray(nodes), u, first, second),
    )
    state = lax.cond(flag[0, 0] > 0.5, lambda: fast, lambda: step_by_step(u, f, d))
    return state[None]


def solution(mesh):
    placed = P("gx", "yz", None)
    return jax.shard_map(
        per_device,
        mesh=mesh,
        in_specs=(placed, placed, placed),
        out_specs=P("level", "gx", "yz", None),
        check_vma=False,
    )
```

```python
import math

import jax
import jax.numpy as jnp
import numpy as np
from jax import lax
from jax.experimental import pallas as pl
from jax.experimental.pallas import tpu as pltpu
from jax.sharding import PartitionSpec as P

STEPS = 3
ITERS = 3
DIFFUSION = 1.0
CENTRE, RADIUS = 8.0, 7.0
HALF = 6
TOP = 2 * HALF
MOMENTS = 2 * TOP
NODES = 128
WIDE = HALF + 1
ROWS = 8
NOISE_GAIN = 4.0
ERROR_BOUND = 4e-5

AXES = ("gx", "yz")
CHECK_AT, FIELD_AT = 32, 47
LOW_AT = 64


def chebyshev_tables():
    angle = np.pi * (np.arange(NODES) + 0.5) / NODES
    exact = np.cos(np.arange(32)[:, None] * angle[None])
    first = np.round(exact * 2048.0) / 2048.0
    second = np.round((exact - first) * 2.0**23) / 2.0**23
    parts = np.concatenate([first, second, exact - first - second, exact])
    return parts.astype(np.float32), (CENTRE + RADIUS * exact[1:2]).astype(np.float32)


def total(values):
    return jnp.sum(values, axis=1, keepdims=True)


def two_sum(a, b):
    s = a + b
    t = s - a
    return s, (a - (s - t)) + (b - t)


def plus(a, b):
    s, e = two_sum(a[0], b[0])
    return two_sum(s, e + (a[1] + b[1]))


def times(scale, a):
    return scale * a[0], scale * a[1]


def halves(values):
    wide = 4097.0 * values
    high = wide - (wide - values)
    return high, values - high


def split_sum(values, axis=None):
    count = values.size if axis is None else values.shape[axis]
    most = jnp.max(jnp.abs(values), axis=axis, keepdims=True)
    unit = (4.0 * count) * most
    high = (values + unit) - unit
    return jnp.sum(high, axis=axis, keepdims=True), jnp.sum(values - high, axis=axis, keepdims=True)


def spectral_solve(resid, weight, nodes, noise):
    direction = resid
    answer = jnp.zeros_like(resid)
    norm_now = total(weight * resid * resid)
    noise_now = noise * total(resid * resid)
    error = jnp.zeros_like(norm_now)
    for step in range(ITERS):
        image = nodes * direction
        product = total(weight * direction * image)
        length = total(weight * direction * direction)
        noise_product = noise * total(direction * image)
        alpha = norm_now / product
        error = error + alpha * (noise_now / norm_now + noise_product / product) * jnp.sqrt(length)
        answer = answer + alpha * direction
        resid = resid - alpha * image
        if step + 1 < ITERS:
            norm_next = total(weight * resid * resid)
            noise_now = noise * total(resid * resid)
            direction = resid + (norm_next / norm_now) * direction
            norm_now = norm_next
    return answer, error


def coefficients(high, low, tables, nodes):
    table = tables[96:128]
    place = lax.broadcasted_iota(jnp.int32, (32, 1), 0)
    raw = high[:32], low[:32]
    base = tuple(jnp.where(place % 2 == 0, r[0:1], r[1:2]) for r in raw)
    shifted = plus(times(2.0, raw), times(-1.0, base))
    used = place < MOMENTS
    moment = tuple(jnp.where(used, jnp.where(place < 2, r, m), 0.0) for r, m in zip(raw, shifted))
    factor = jnp.where(place == 0, 1.0 / NODES, 2.0 / NODES)
    big, small = halves(factor * moment[0])
    small = small + factor * moment[1]
    parts = big * tables[:32]
    rest = big * tables[32:64] + small * tables[:32] + (big * tables[64:96] + small * tables[32:64])
    pieces = (parts, rest)
    count = 32
    while count > 1:
        count //= 2
        pieces = plus(tuple(p[:count] for p in pieces), tuple(p[count : 2 * count] for p in pieces))
    weight = pieces[0] + pieces[1]
    worst = jnp.zeros((1, 1), jnp.float32)
    at = lambda pair, k: (pair[0][k : k + 1], pair[1][k : k + 1])
    for k in range(1, TOP):
        gap = plus(times(2.0, at((high, low), CHECK_AT + k)), times(-1.0, at(moment, 2)))
        gap = plus(gap, times(-1.0, at(moment, 2 * k)))
        worst = jnp.maximum(worst, jnp.abs(gap[0] + gap[1]))
    noise = (worst + 1e-10 * high[0:1]) * (NOISE_GAIN / NODES)
    dots = high
    above = nodes - 1.0
    one = jnp.ones_like(nodes)
    path = [jnp.zeros_like(nodes)]
    second = path[0]
    errors = [jnp.zeros((1, 1), jnp.float32), jnp.zeros((1, 1), jnp.float32)]
    for step in range(STEPS):
        change, error = spectral_solve(one - above * path[-1], weight, nodes, noise)
        path.append(path[-1] + change)
        errors[0] = errors[0] + error
    for step in range(STEPS):
        resid = one - above * second + 0.5 * above * (path[step + 1] - path[step])
        change, error = spectral_solve(resid, weight, nodes, noise)
        second = second + change
        errors[1] = errors[1] + error
    results = []
    for values, error in ((path[-1], errors[0]), (second, errors[0] + errors[1])):
        part = total(table[:16] * values) * (2.0 / NODES)
        row = lax.broadcasted_iota(jnp.int32, (16, 1), 0)
        part = jnp.where(row == 0, 0.5 * part, part)
        part = jnp.where(row < TOP, part, 0.0)
        cross = jnp.sum(part * dots[FIELD_AT + 1 : FIELD_AT + 17], axis=0, keepdims=True)
        square = dots[FIELD_AT : FIELD_AT + 1] + 2.0 * cross + total(weight * values * values)
        fine = (error * error <= ERROR_BOUND * ERROR_BOUND * square) & (error >= 0.0)
        results.append((part, fine))
    return results


PAD = 8
OWN = PAD + ROWS


def half_of(ref, rows):
    level = lax.axis_index("level")
    return jnp.where(level == 0, ref[:, rows, :128], ref[:, rows, 128:])


def pack_rows_kernel(u, f, d, to_high, to_low):
    nx, ny, _ = u.shape
    for n, ref in enumerate((u, f, d)):
        to_high[n * nx : (n + 1) * nx] = half_of(ref, slice(ny - ROWS, ny))
        to_low[n * nx : (n + 1) * nx] = half_of(ref, slice(0, ROWS))


def pack_planes_kernel(u, f, d, low, high, to_high, to_low):
    nx, ny, _ = u.shape
    at = 0
    for n, (ref, width) in enumerate(((u, WIDE), (f, HALF), (d, HALF))):
        for out, start in ((to_high, nx - width), (to_low, 0)):
            out[at : at + width, :ROWS] = low[n * nx + start : n * nx + start + width]
            out[at : at + width, ROWS : ROWS + ny] = half_of(ref.at[start : start + width], slice(0, ny))
            out[at : at + width, ROWS + ny :] = high[n * nx + start : n * nx + start + width]
        at += width


def pack_vector_kernel(v, low, high, to_high, to_low):
    nx, _, ny, _ = v.shape
    for out, start in ((to_high, nx - HALF), (to_low, 0)):
        out[:, :, :ROWS] = low[start : start + HALF]
        out[:, :, ROWS : ROWS + ny] = v[start : start + HALF]
        out[:, :, ROWS + ny :] = high[start : start + HALF]


def beside(ref, i, start, count):
    here = [ref[i, c, start : start + count] for c in range(2)]
    lane = lax.broadcasted_iota(jnp.int32, (count, 128), 1)
    left = [pltpu.roll(v, 1, 1) for v in here]
    right = [pltpu.roll(v, 127, 1) for v in here]
    along = (
        jnp.where(lane == 0, 0.0, left[0]) + jnp.where(lane == 127, right[1], right[0]),
        jnp.where(lane == 0, left[0], left[1]) + jnp.where(lane == 127, 0.0, right[1]),
    )
    around = []
    for c in range(2):
        planes = ref[i + 1, c, start : start + count] + ref[i - 1, c, start : start + count]
        rows = ref[i, c, start - 1 : start - 1 + count] + ref[i, c, start + 1 : start + 1 + count]
        around.append((planes + rows) + along[c])
    return here, around


def row_mask(ny):
    row = lax.broadcasted_iota(jnp.int32, (ny + 2 * ROWS, 128), 0)
    here, count = lax.axis_index("yz"), lax.axis_size("yz")
    low = jnp.where(here == 0, ROWS, 0)
    high = jnp.where(here == count - 1, ROWS + ny, 2 * ROWS + ny)
    return jnp.where((row >= low) & (row < high), 1.0, 0.0)


def over_planes(nx, halo, body, own_body=None):
    here, count = lax.axis_index("gx"), lax.axis_size("gx")
    below = jnp.where(here == 0, 0.0, 1.0)
    above = jnp.where(here == count - 1, 0.0, 1.0)
    for j in range(halo):
        body(WIDE - halo + j, below)
    for j in range(halo):
        body(WIDE + nx + j, above)

    def inner(i, _):
        body(i + WIDE, None)
        return 0

    if own_body is None:
        lax.fori_loop(0, nx, inner, 0, unroll=4)


def put(row, index, values):
    lane = lax.broadcasted_iota(jnp.int32, row.shape, 1)
    high, low = split_sum(values)
    return jnp.where(lane == index, high, jnp.where(lane == index + LOW_AT, low, row))


def fill_edges(dst, low, high, nx):
    width = low.shape[0]
    dst[WIDE - width : WIDE, :, PAD:-PAD] = low
    dst[WIDE + nx : WIDE + nx + width, :, PAD:-PAD] = high


def clear(ref, nx, width):
    tall = ref.shape[2]
    side = jnp.zeros((2, PAD, 128), jnp.float32)
    whole = jnp.zeros((2, tall, 128), jnp.float32)

    def margins(i, _):
        ref[i, :, :PAD] = side
        ref[i, :, tall - PAD :] = side
        return 0

    lax.fori_loop(0, nx + 2 * WIDE, margins, 0)
    for j in range(width):
        ref[j] = whole
        ref[WIDE + nx + (WIDE - width) + j] = whole


def recur(src, dst, scale, pull, first_step, rows):
    start, count = rows
    offset = start - PAD
    factor = pull[offset : offset + count]

    def body(i, mask):
        here, around = beside(src, i, start, count)
        weight = factor if mask is None else factor * mask
        made = []
        for c in range(2):
            at = (i, c, slice(start, start + count))
            twice = scale[at] * here[c] - weight * around[c]
            new = 0.5 * twice if first_step else twice - dst[at]
            dst[at] = new
            made.append(new)
        return made

    return body


def first_kernel(u, f, d, *refs):
    mine, theirs = refs[:4], refs[4:8]
    basis, scale, to_high, to_low, wide_u, va, vb = refs[8:]
    nx, ny, _ = u.shape
    level = lax.axis_index("level")
    for ref in (wide_u, va, vb):
        clear(ref, nx, WIDE if ref is vb else 0)
    va[0, :, PAD:-PAD] = jnp.zeros((2, ny + 2 * ROWS, 128), jnp.float32)
    va[2 * WIDE + nx - 1, :, PAD:-PAD] = jnp.zeros((2, ny + 2 * ROWS, 128), jnp.float32)
    at = 0
    for n, (ref, width, dst) in enumerate(((u, WIDE, wide_u), (f, HALF, va), (d, HALF, scale))):
        for (ylow, yhigh, xlow, xhigh), c in ((mine, level), (theirs, 1 - level)):
            dst[WIDE - width : WIDE, c, PAD:-PAD] = xlow[at : at + width]
            dst[WIDE + nx : WIDE + nx + width, c, PAD:-PAD] = xhigh[at : at + width]
            dst[WIDE : WIDE + nx, c, PAD:OWN] = ylow[n * nx : (n + 1) * nx]
            dst[WIDE : WIDE + nx, c, OWN + ny : OWN + ny + ROWS] = yhigh[n * nx : (n + 1) * nx]
        for c in range(2):
            dst[WIDE : WIDE + nx, c, OWN : OWN + ny] = ref[:, :, c * 128 : (c + 1) * 128]
        at += width
    keep = row_mask(ny)
    pull = keep * (2.0 / RADIUS * DIFFUSION)
    rows = (PAD, ny + 2 * ROWS)

    def start(i, mask):
        here, around = beside(wide_u, i, *rows)
        inside = keep if mask is None else keep * mask
        for c in range(2):
            at = (i, c, slice(PAD, PAD + rows[1]))
            damp = scale[at]
            va[at] = inside * (va[at] - (damp * here[c] + DIFFUSION * (6.0 * here[c] - around[c])))
            scale[at] = inside * ((2.0 / RADIUS) * (damp + (1.0 + 6.0 * DIFFUSION - CENTRE)))

    over_planes(nx, HALF, start)

    def save(i, _):
        basis[0, i] = va[i + WIDE, :, OWN : OWN + ny]
        return 0

    lax.fori_loop(0, nx, save, 0, unroll=4)
    for k in range(HALF):
        src, dst = (va, vb) if k % 2 == 0 else (vb, va)
        last = k == HALF - 1
        step = recur(src, dst, scale, pull, k == 0, (OWN, ny) if last else rows)

        def body(i, mask, step=step, k=k, last=last):
            made = step(i, mask)
            if mask is None:
                for c in range(2):
                    basis[k + 1, i - WIDE, c] = made[c] if last else made[c][ROWS : ROWS + ny]

        over_planes(nx, HALF - 1 - k, body)
    to_high[...] = basis[HALF, :, :, ny - ROWS :, :]
    to_low[...] = basis[HALF, :, :, :ROWS, :]


def first_dots_kernel(u, basis, dots):
    count, nx, _, ny, _ = basis.shape
    row = jnp.zeros((8, 128), jnp.float32)
    for k in range(count):

        def body(i, sums, k=k):
            terms = [[] for _ in sums]
            for c in range(2):
                own = u[i, :, c * 128 : (c + 1) * 128]
                new = basis[k, i, c]
                parts = [own * new, new * new]
                if k == 0:
                    parts.append(own * own)
                else:
                    parts.append(basis[k - 1, i, c] * new)
                if k > 1:
                    parts.append(basis[k - 2, i, c] * new)
                for t, p in zip(terms, parts):
                    t.append(p)
            return tuple((s[0] + t[0], s[1] + t[1]) for s, t in zip(sums, terms))

        zero = jnp.zeros((ny, 128), jnp.float32)
        sums = lax.fori_loop(0, nx, body, ((zero, zero),) * (4 if k > 1 else 3), unroll=4)
        where = (FIELD_AT + 1 + k, 2 * k, FIELD_AT if k == 0 else 2 * k - 1, CHECK_AT + k - 1)
        for at, (a, b) in zip(where, sums):
            row = put(row, at, jnp.concatenate([a, b], axis=0))
    dots[...] = row


def second_kernel(u, first, scale, ylow, yhigh, xlow, xhigh, before, basis, dots, va, vb):
    _, nx, _, ny, _ = first.shape
    clear(va, nx, 0)
    clear(vb, nx, WIDE)
    fill_edges(va, xlow[...], xhigh[...], nx)
    va[0, :, PAD:-PAD] = jnp.zeros((2, ny + 2 * ROWS, 128), jnp.float32)
    va[2 * WIDE + nx - 1, :, PAD:-PAD] = jnp.zeros((2, ny + 2 * ROWS, 128), jnp.float32)
    va[WIDE : WIDE + nx, :, PAD:OWN] = ylow[...]
    va[WIDE : WIDE + nx, :, OWN : OWN + ny] = first[HALF]
    va[WIDE : WIDE + nx, :, OWN + ny : OWN + ny + ROWS] = yhigh[...]
    pull = row_mask(ny) * (2.0 / RADIUS * DIFFUSION)
    rows = (PAD, ny + 2 * ROWS)
    row = before[...]
    get = lambda k, i, c: first[k, i, c] if k <= HALF else basis[k - HALF - 1, i, c]
    for j in range(HALF):
        src, dst = (va, vb) if j % 2 == 0 else (vb, va)
        last = j == HALF - 1
        step = recur(src, dst, scale, pull, j == 0, (OWN, ny) if last else rows)
        over_planes(nx, HALF - 1 - j, step, own_body=step)
        k = HALF + j

        def body(i, sums, step=step, j=j, k=k, last=last):
            made = step(i + WIDE, None)
            result = [list(s) for s in sums]
            for c in range(2):
                mid = made[c] if last else made[c][ROWS : ROWS + ny]
                new = 2.0 * mid - first[HALF - 1 - j, i, c]
                parts = [get(k, i, c) * new, get(k - 1, i, c) * new]
                if not last:
                    basis[j, i, c] = new
                    parts += [new * new, u[i, :, c * 128 : (c + 1) * 128] * new]
                for r, p in zip(result, parts):
                    r[c] = r[c] + p
            return tuple(tuple(r) for r in result)

        zero = jnp.zeros((ny, 128), jnp.float32)
        sums = lax.fori_loop(0, nx, body, ((zero, zero),) * (2 if last else 4), unroll=4)
        where = (2 * k + 1, CHECK_AT + k, 2 * k + 2, FIELD_AT + 2 + k)
        for at, (a, b) in zip(where, sums):
            row = put(row, at, jnp.concatenate([a, b], axis=0))
    dots[...] = jnp.broadcast_to(row[0:1], dots.shape)


def finish_kernel(gathered, tables, nodes, u, first, second, out, flag):
    nx, ny, nz = u.shape
    turned = gathered[...].T
    high, low = split_sum(turned[:LOW_AT], 1)
    high, low = two_sum(high, low + total(turned[LOW_AT:]))
    (lower, fine_low), (upper, fine_up) = coefficients(high, low, tables[...], nodes[...])
    level = lax.axis_index("level")
    part = jnp.where(level == 0, lower, upper)
    flag[...] = jnp.broadcast_to(jnp.where(fine_low & fine_up, 1.0, 0.0), flag.shape)
    factors = [jnp.broadcast_to(part[k : k + 1], (8, 128)) for k in range(TOP)]

    def body(i, _):
        for r in range(0, ny, 8):
            for c in range(2):
                value = u[i, r : r + 8, c * 128 : (c + 1) * 128]
                for k in range(TOP):
                    ref, n = (first, k) if k <= HALF else (second, k - HALF - 1)
                    value = value + factors[k] * ref[n, i, c, r : r + 8]
                out[i, r : r + 8, c * 128 : (c + 1) * 128] = value
        return 0

    lax.fori_loop(0, nx, body, 0, unroll=2)


def call(kernel, outs, args, scratch=(), limit=30 << 20):
    whole = pl.BlockSpec(memory_space=pltpu.VMEM)
    return pl.pallas_call(
        kernel,
        out_shape=[jax.ShapeDtypeStruct(s, jnp.float32) for s in outs],
        in_specs=[whole] * len(args),
        out_specs=[whole] * len(outs),
        scratch_shapes=[pltpu.VMEM(s, jnp.float32) for s in scratch],
        compiler_params=pltpu.CompilerParams(vmem_limit_bytes=limit),
        name=kernel.__name__,
    )(*args)


def both_ways(up, down, axis):
    size = lax.axis_size(axis)
    route = [(i, i + 1) for i in range(size - 1)]
    return lax.ppermute(up, axis, route), lax.ppermute(down, axis, [(b, a) for a, b in route])


def stencil(field, damping):
    low, high = both_ways(field[-1:], field[:1], "gx")
    left, right = both_ways(field[:, -1:], field[:, :1], "yz")
    tall = jnp.concatenate([low, field, high], axis=0)
    long = jnp.concatenate([left, field, right], axis=1)
    zero = jnp.zeros_like(field[:, :, :1])
    near = tall[2:] + tall[:-2] + long[:, 2:] + long[:, :-2]
    near = near + jnp.concatenate([field[:, :, 1:], zero], axis=2) + jnp.concatenate([zero, field[:, :, :-1]], axis=2)
    return damping * field + DIFFUSION * (6.0 * field - near)


def dot(a, b):
    value = jnp.sum(a * b)
    for axis in AXES:
        value = lax.psum(value, axis)
    return value


def solve(target, guess, damping):
    resid = target - (guess + stencil(guess, damping))

    def step(_, state):
        answer, resid, direction, norm_now = state
        image = direction + stencil(direction, damping)
        alpha = norm_now / dot(direction, image)
        answer = answer + alpha * direction
        resid = resid - alpha * image
        norm_next = dot(resid, resid)
        return answer, resid, resid + (norm_next / norm_now) * direction, norm_next

    return lax.fori_loop(0, ITERS, step, (guess, resid, resid, dot(resid, resid)))[0]


def step_by_step(init_field, source, damping):
    def body(_, carry):
        lower, upper = carry
        fresh = solve(lower + source, lower, damping)
        extra = 0.5 * stencil(fresh - lower, damping)
        return fresh, solve(upper + source + extra, upper, damping)

    lower, upper = lax.fori_loop(0, STEPS, body, (init_field, init_field))
    return jnp.where(lax.axis_index("level") == 1, upper, lower)


def per_device(u, f, d):
    nx, ny, nz = u.shape
    tall = 2 * ROWS + ny
    ups, downs = call(pack_rows_kernel, [(3 * nx, ROWS, 128)] * 2, (u, f, d))
    ylow, yhigh = both_ways(ups, downs, "yz")
    edge = (WIDE + 2 * HALF, tall, 128)
    ups, downs = call(pack_planes_kernel, [edge] * 2, (u, f, d, ylow, yhigh))
    mine = (ylow, yhigh) + both_ways(ups, downs, "gx")
    theirs = tuple(lax.ppermute(half, "level", [(0, 1), (1, 0)]) for half in mine)
    padded = (nx + 2 * WIDE, 2, tall + 2 * PAD, 128)
    first, scale, ups, downs = call(
        first_kernel,
        [(HALF + 1, nx, 2, ny, 128), padded, (nx, 2, ROWS, 128), (nx, 2, ROWS, 128)],
        (u, f, d) + mine + theirs,
        [padded] * 3,
    )
    ylow, yhigh = both_ways(ups, downs, "yz")
    (dots,) = call(first_dots_kernel, [(8, 128)], (u, first))
    ups, downs = call(pack_vector_kernel, [(HALF, 2, tall, 128)] * 2, (first[HALF], ylow, yhigh))
    xlow, xhigh = both_ways(ups, downs, "gx")
    parts = lax.axis_size(AXES)
    second, dots = call(
        second_kernel,
        [(HALF - 1, nx, 2, ny, 128), (parts, 128)],
        (u, first, scale, ylow, yhigh, xlow, xhigh, dots),
        [padded] * 2,
    )
    gathered = lax.all_to_all(dots.reshape(parts, 1, 128), AXES, 0, 0).reshape(parts, 128)
    tables, nodes = chebyshev_tables()
    fast, flag = call(
        finish_kernel,
        [(nx, ny, nz), (8, 128)],
        (gathered, jnp.asarray(tables), jnp.asarray(nodes), u, first, second),
    )
    state = lax.cond(flag[0, 0] > 0.5, lambda: fast, lambda: step_by_step(u, f, d))
    return state[None]


def solution(mesh):
    placed = P("gx", "yz", None)
    return jax.shard_map(
        per_device,
        mesh=mesh,
        in_specs=(placed, placed, placed),
        out_specs=P("level", "gx", "yz", None),
        check_vma=False,
    )
```

```python
import math

import jax
import jax.numpy as jnp
import numpy as np
from jax import lax
from jax.experimental import pallas as pl
from jax.experimental.pallas import tpu as pltpu
from jax.sharding import PartitionSpec as P

STEPS = 3
ITERS = 3
DIFFUSION = 1.0
CENTRE, RADIUS = 8.0, 7.0
HALF = 6
TOP = 2 * HALF
MOMENTS = 2 * TOP
NODES = 128
WIDE = HALF + 1
ROWS = 8
NOISE_GAIN = 4.0
ERROR_BOUND = 4e-5

AXES = ("gx", "yz")
CHECK_AT, FIELD_AT = 32, 47
LOW_AT = 64


def chebyshev_tables():
    angle = np.pi * (np.arange(NODES) + 0.5) / NODES
    exact = np.cos(np.arange(32)[:, None] * angle[None])
    first = np.round(exact * 2048.0) / 2048.0
    second = np.round((exact - first) * 2.0**23) / 2.0**23
    parts = np.concatenate([first, second, exact - first - second, exact])
    return parts.astype(np.float32), (CENTRE + RADIUS * exact[1:2]).astype(np.float32)


def total(values):
    return jnp.sum(values, axis=1, keepdims=True)


def two_sum(a, b):
    s = a + b
    t = s - a
    return s, (a - (s - t)) + (b - t)


def plus(a, b):
    s, e = two_sum(a[0], b[0])
    return two_sum(s, e + (a[1] + b[1]))


def times(scale, a):
    return scale * a[0], scale * a[1]


def halves(values):
    wide = 4097.0 * values
    high = wide - (wide - values)
    return high, values - high


def split_sum(values, axis=None):
    count = values.size if axis is None else values.shape[axis]
    most = jnp.max(jnp.abs(values), axis=axis, keepdims=True)
    unit = (4.0 * count) * most
    high = (values + unit) - unit
    return jnp.sum(high, axis=axis, keepdims=True), jnp.sum(values - high, axis=axis, keepdims=True)


def spectral_solve(resid, weight, nodes, noise):
    direction = resid
    answer = jnp.zeros_like(resid)
    norm_now = total(weight * resid * resid)
    noise_now = noise * total(resid * resid)
    error = jnp.zeros_like(norm_now)
    for step in range(ITERS):
        image = nodes * direction
        product = total(weight * direction * image)
        length = total(weight * direction * direction)
        noise_product = noise * total(direction * image)
        alpha = norm_now / product
        error = error + alpha * (noise_now / norm_now + noise_product / product) * jnp.sqrt(length)
        answer = answer + alpha * direction
        resid = resid - alpha * image
        if step + 1 < ITERS:
            norm_next = total(weight * resid * resid)
            noise_now = noise * total(resid * resid)
            direction = resid + (norm_next / norm_now) * direction
            norm_now = norm_next
    return answer, error


def coefficients(high, low, tables, nodes):
    table = tables[96:128]
    place = lax.broadcasted_iota(jnp.int32, (32, 1), 0)
    raw = high[:32], low[:32]
    base = tuple(jnp.where(place % 2 == 0, r[0:1], r[1:2]) for r in raw)
    shifted = plus(times(2.0, raw), times(-1.0, base))
    used = place < MOMENTS
    moment = tuple(jnp.where(used, jnp.where(place < 2, r, m), 0.0) for r, m in zip(raw, shifted))
    factor = jnp.where(place == 0, 1.0 / NODES, 2.0 / NODES)
    big, small = halves(factor * moment[0])
    small = small + factor * moment[1]
    parts = big * tables[:32]
    rest = big * tables[32:64] + small * tables[:32] + (big * tables[64:96] + small * tables[32:64])
    pieces = (parts, rest)
    count = 32
    while count > 1:
        count //= 2
        pieces = plus(tuple(p[:count] for p in pieces), tuple(p[count : 2 * count] for p in pieces))
    weight = pieces[0] + pieces[1]
    worst = jnp.zeros((1, 1), jnp.float32)
    at = lambda pair, k: (pair[0][k : k + 1], pair[1][k : k + 1])
    for k in range(1, TOP):
        gap = plus(times(2.0, at((high, low), CHECK_AT + k)), times(-1.0, at(moment, 2)))
        gap = plus(gap, times(-1.0, at(moment, 2 * k)))
        worst = jnp.maximum(worst, jnp.abs(gap[0] + gap[1]))
    noise = (worst + 1e-10 * high[0:1]) * (NOISE_GAIN / NODES)
    dots = high
    above = nodes - 1.0
    one = jnp.ones_like(nodes)
    path = [jnp.zeros_like(nodes)]
    second = path[0]
    errors = [jnp.zeros((1, 1), jnp.float32), jnp.zeros((1, 1), jnp.float32)]
    for rounds in range(STEPS + 1):
        lower = upper = one
        if rounds < STEPS:
            lower = one - above * path[-1]
        if rounds > 0:
            upper = one - above * second + 0.5 * above * (path[rounds] - path[rounds - 1])
        change, error = spectral_solve(jnp.concatenate([lower, upper], axis=0), weight, nodes, noise)
        if rounds > 0:
            second = second + change[1:2]
            errors[1] = errors[1] + error[1:2]
        if rounds < STEPS:
            path.append(path[-1] + change[0:1])
            errors[0] = errors[0] + error[0:1]
    results = []
    for values, error in ((path[-1], errors[0]), (second, errors[0] + errors[1])):
        part = total(table[:16] * values) * (2.0 / NODES)
        row = lax.broadcasted_iota(jnp.int32, (16, 1), 0)
        part = jnp.where(row == 0, 0.5 * part, part)
        part = jnp.where(row < TOP, part, 0.0)
        cross = jnp.sum(part * dots[FIELD_AT + 1 : FIELD_AT + 17], axis=0, keepdims=True)
        square = dots[FIELD_AT : FIELD_AT + 1] + 2.0 * cross + total(weight * values * values)
        fine = (error * error <= ERROR_BOUND * ERROR_BOUND * square) & (error >= 0.0)
        results.append((part, fine))
    return results


PAD = 8
OWN = PAD + ROWS


def by_level(lower, upper):
    return jnp.where(lax.axis_index("level") == 0, lower, upper)


def pack_rows_kernel(u, f, d, out):
    nx, ny, _ = u.shape
    for n, ref in enumerate((u, f, d)):
        for c in range(2):
            lanes = slice(c * 128, (c + 1) * 128)
            out[n * nx : (n + 1) * nx, c] = by_level(ref[:, ny - ROWS :, lanes], ref[:, :ROWS, lanes])


def pack_planes_kernel(u, f, d, halo, to_high, to_low):
    nx, ny, _ = u.shape
    at = 0
    for n, (ref, width) in enumerate(((u, WIDE), (f, HALF), (d, HALF))):
        for out, start in ((to_high, nx - width), (to_low, 0)):
            for c in range(2):
                lanes = slice(c * 128, (c + 1) * 128)
                outer = halo[n * nx + start : n * nx + start + width, c]
                out[at : at + width, c, :ROWS] = by_level(outer, ref[start : start + width, ny - ROWS :, lanes])
                out[at : at + width, c, ROWS:] = by_level(ref[start : start + width, :ROWS, lanes], outer)
        at += width


def pack_vector_kernel(v, halo, to_high, to_low):
    nx, _, ny, _ = v.shape
    for out, start in ((to_high, nx - HALF), (to_low, 0)):
        outer = halo[start : start + HALF]
        out[:, :, :ROWS] = by_level(outer, v[start : start + HALF, :, ny - ROWS :])
        out[:, :, ROWS:] = by_level(v[start : start + HALF, :, :ROWS], outer)


def row_spans(level, ny):
    halo = pl.multiple_of(PAD + level * (ROWS + ny), 8)
    half = pl.multiple_of(PAD + level * (2 * ROWS), 8)
    return pl.ds(halo, ROWS), pl.ds(half, 2 * ROWS)


def beside(ref, i, start, count):
    here = [ref[i, c, start : start + count] for c in range(2)]
    lane = lax.broadcasted_iota(jnp.int32, (count, 128), 1)
    left = [pltpu.roll(v, 1, 1) for v in here]
    right = [pltpu.roll(v, 127, 1) for v in here]
    along = (
        jnp.where(lane == 0, 0.0, left[0]) + jnp.where(lane == 127, right[1], right[0]),
        jnp.where(lane == 0, left[0], left[1]) + jnp.where(lane == 127, 0.0, right[1]),
    )
    around = []
    for c in range(2):
        planes = ref[i + 1, c, start : start + count] + ref[i - 1, c, start : start + count]
        rows = ref[i, c, start - 1 : start - 1 + count] + ref[i, c, start + 1 : start + 1 + count]
        around.append((planes + rows) + along[c])
    return here, around


def row_mask(ny):
    row = lax.broadcasted_iota(jnp.int32, (ny + 2 * ROWS, 128), 0)
    here, count = lax.axis_index("yz"), lax.axis_size("yz")
    low = jnp.where(here == 0, ROWS, 0)
    high = jnp.where(here == count - 1, ROWS + ny, 2 * ROWS + ny)
    return jnp.where((row >= low) & (row < high), 1.0, 0.0)


def over_planes(nx, halo, body, own_body=None):
    here, count = lax.axis_index("gx"), lax.axis_size("gx")
    below = jnp.where(here == 0, 0.0, 1.0)
    above = jnp.where(here == count - 1, 0.0, 1.0)
    for j in range(halo):
        body(WIDE - halo + j, below)
    for j in range(halo):
        body(WIDE + nx + j, above)

    def inner(i, _):
        body(i + WIDE, None)
        return 0

    if own_body is None:
        lax.fori_loop(0, nx, inner, 0, unroll=4)


def put(row, index, values):
    lane = lax.broadcasted_iota(jnp.int32, row.shape, 1)
    high, low = split_sum(values)
    return jnp.where(lane == index, high, jnp.where(lane == index + LOW_AT, low, row))


def clear(ref, nx, width):
    tall = ref.shape[2]
    side = jnp.zeros((2, PAD, 128), jnp.float32)
    whole = jnp.zeros((2, tall, 128), jnp.float32)

    def margins(i, _):
        ref[i, :, :PAD] = side
        ref[i, :, tall - PAD :] = side
        return 0

    lax.fori_loop(0, nx + 2 * WIDE, margins, 0)
    for j in range(width):
        ref[j] = whole
        ref[WIDE + nx + (WIDE - width) + j] = whole


def recur(src, dst, scale, pull, first_step, rows):
    start, count = rows
    offset = start - PAD
    factor = pull[offset : offset + count]

    def body(i, mask):
        here, around = beside(src, i, start, count)
        weight = factor if mask is None else factor * mask
        made = []
        for c in range(2):
            at = (i, c, slice(start, start + count))
            twice = scale[at] * here[c] - weight * around[c]
            new = 0.5 * twice if first_step else twice - dst[at]
            dst[at] = new
            made.append(new)
        return made

    return body


def first_kernel(u, f, d, *refs):
    mine, theirs = refs[:3], refs[3:6]
    basis, scale, edge, wide_u, va, vb = refs[6:]
    nx, ny, _ = u.shape
    level = lax.axis_index("level")
    for ref in (wide_u, va, vb):
        clear(ref, nx, WIDE if ref is vb else 0)
    va[0, :, PAD:-PAD] = jnp.zeros((2, ny + 2 * ROWS, 128), jnp.float32)
    va[2 * WIDE + nx - 1, :, PAD:-PAD] = jnp.zeros((2, ny + 2 * ROWS, 128), jnp.float32)
    at = 0
    for n, (ref, width, dst) in enumerate(((u, WIDE, wide_u), (f, HALF, va), (d, HALF, scale))):
        for (halo, xlow, xhigh), place in ((mine, level), (theirs, 1 - level)):
            outer, part = row_spans(place, ny)
            dst[WIDE - width : WIDE, :, part] = xlow[at : at + width]
            dst[WIDE + nx : WIDE + nx + width, :, part] = xhigh[at : at + width]
            dst[WIDE : WIDE + nx, :, outer] = halo[n * nx : (n + 1) * nx]
        for c in range(2):
            dst[WIDE : WIDE + nx, c, OWN : OWN + ny] = ref[:, :, c * 128 : (c + 1) * 128]
        at += width
    keep = row_mask(ny)
    pull = keep * (2.0 / RADIUS * DIFFUSION)
    rows = (PAD, ny + 2 * ROWS)

    def start(i, mask):
        here, around = beside(wide_u, i, *rows)
        inside = keep if mask is None else keep * mask
        for c in range(2):
            at = (i, c, slice(PAD, PAD + rows[1]))
            damp = scale[at]
            va[at] = inside * (va[at] - (damp * here[c] + DIFFUSION * (6.0 * here[c] - around[c])))
            scale[at] = inside * ((2.0 / RADIUS) * (damp + (1.0 + 6.0 * DIFFUSION - CENTRE)))

    over_planes(nx, HALF, start)

    def save(i, _):
        basis[0, i] = va[i + WIDE, :, OWN : OWN + ny]
        return 0

    lax.fori_loop(0, nx, save, 0, unroll=4)
    for k in range(HALF):
        src, dst = (va, vb) if k % 2 == 0 else (vb, va)
        last = k == HALF - 1
        step = recur(src, dst, scale, pull, k == 0, (OWN, ny) if last else rows)

        def body(i, mask, step=step, k=k, last=last):
            made = step(i, mask)
            if mask is None:
                for c in range(2):
                    basis[k + 1, i - WIDE, c] = made[c] if last else made[c][ROWS : ROWS + ny]

        over_planes(nx, HALF - 1 - k, body)
    edge[...] = by_level(basis[HALF, :, :, ny - ROWS :, :], basis[HALF, :, :, :ROWS, :])


def first_dots_kernel(u, basis, dots):
    count, nx, _, ny, _ = basis.shape
    row = jnp.zeros((8, 128), jnp.float32)
    for k in range(count):

        def body(i, sums, k=k):
            terms = [[] for _ in sums]
            for c in range(2):
                own = u[i, :, c * 128 : (c + 1) * 128]
                new = basis[k, i, c]
                parts = [own * new, new * new]
                if k == 0:
                    parts.append(own * own)
                else:
                    parts.append(basis[k - 1, i, c] * new)
                if k > 1:
                    parts.append(basis[k - 2, i, c] * new)
                for t, p in zip(terms, parts):
                    t.append(p)
            return tuple((s[0] + t[0], s[1] + t[1]) for s, t in zip(sums, terms))

        zero = jnp.zeros((ny, 128), jnp.float32)
        sums = lax.fori_loop(0, nx, body, ((zero, zero),) * (4 if k > 1 else 3), unroll=4)
        where = (FIELD_AT + 1 + k, 2 * k, FIELD_AT if k == 0 else 2 * k - 1, CHECK_AT + k - 1)
        for at, (a, b) in zip(where, sums):
            row = put(row, at, jnp.concatenate([a, b], axis=0))
    dots[...] = row


def second_kernel(u, first, scale, before, *refs):
    mine, theirs = refs[:3], refs[3:6]
    basis, dots, va, vb = refs[6:]
    _, nx, _, ny, _ = first.shape
    clear(va, nx, 0)
    clear(vb, nx, WIDE)
    va[0, :, PAD:-PAD] = jnp.zeros((2, ny + 2 * ROWS, 128), jnp.float32)
    va[2 * WIDE + nx - 1, :, PAD:-PAD] = jnp.zeros((2, ny + 2 * ROWS, 128), jnp.float32)
    level = lax.axis_index("level")
    for (halo, xlow, xhigh), place in ((mine, level), (theirs, 1 - level)):
        outer, part = row_spans(place, ny)
        va[WIDE - HALF : WIDE, :, part] = xlow[...]
        va[WIDE + nx : WIDE + nx + HALF, :, part] = xhigh[...]
        va[WIDE : WIDE + nx, :, outer] = halo[...]
    va[WIDE : WIDE + nx, :, OWN : OWN + ny] = first[HALF]
    pull = row_mask(ny) * (2.0 / RADIUS * DIFFUSION)
    rows = (PAD, ny + 2 * ROWS)
    row = before[...]
    get = lambda k, i, c: first[k, i, c] if k <= HALF else basis[k - HALF - 1, i, c]
    for j in range(HALF):
        src, dst = (va, vb) if j % 2 == 0 else (vb, va)
        last = j == HALF - 1
        step = recur(src, dst, scale, pull, j == 0, (OWN, ny) if last else rows)
        over_planes(nx, HALF - 1 - j, step, own_body=step)
        k = HALF + j

        def body(i, sums, step=step, j=j, k=k, last=last):
            made = step(i + WIDE, None)
            result = [list(s) for s in sums]
            for c in range(2):
                mid = made[c] if last else made[c][ROWS : ROWS + ny]
                new = 2.0 * mid - first[HALF - 1 - j, i, c]
                parts = [get(k, i, c) * new, get(k - 1, i, c) * new]
                if not last:
                    basis[j, i, c] = new
                    parts += [new * new, u[i, :, c * 128 : (c + 1) * 128] * new]
                for r, p in zip(result, parts):
                    r[c] = r[c] + p
            return tuple(tuple(r) for r in result)

        zero = jnp.zeros((ny, 128), jnp.float32)
        sums = lax.fori_loop(0, nx, body, ((zero, zero),) * (2 if last else 4), unroll=4)
        where = (2 * k + 1, CHECK_AT + k, 2 * k + 2, FIELD_AT + 2 + k)
        for at, (a, b) in zip(where, sums):
            row = put(row, at, jnp.concatenate([a, b], axis=0))
    dots[...] = jnp.broadcast_to(row[0:1], dots.shape)


def finish_kernel(gathered, tables, nodes, u, first, second, out, flag):
    nx, ny, nz = u.shape
    turned = gathered[...].T
    high, low = split_sum(turned[:LOW_AT], 1)
    high, low = two_sum(high, low + total(turned[LOW_AT:]))
    (lower, fine_low), (upper, fine_up) = coefficients(high, low, tables[...], nodes[...])
    level = lax.axis_index("level")
    part = jnp.where(level == 0, lower, upper)
    flag[0, 0] = jnp.where(jnp.min(jnp.where(fine_low & fine_up, 1.0, 0.0)) > 0.5, 1, 0)
    factors = [jnp.broadcast_to(part[k : k + 1], (8, 128)) for k in range(TOP)]

    def body(i, _):
        for r in range(0, ny, 8):
            for c in range(2):
                value = u[i, r : r + 8, c * 128 : (c + 1) * 128]
                for k in range(TOP):
                    ref, n = (first, k) if k <= HALF else (second, k - HALF - 1)
                    value = value + factors[k] * ref[n, i, c, r : r + 8]
                out[i, r : r + 8, c * 128 : (c + 1) * 128] = value
        return 0

    lax.fori_loop(0, nx, body, 0, unroll=2)


def call(kernel, outs, args, scratch=(), limit=16 << 20, flags=()):
    whole = pl.BlockSpec(memory_space=pltpu.VMEM)
    shapes = [jax.ShapeDtypeStruct(s, jnp.float32) for s in outs]
    return pl.pallas_call(
        kernel,
        out_shape=shapes + [jax.ShapeDtypeStruct(s, jnp.int32) for s in flags],
        in_specs=[whole] * len(args),
        out_specs=[whole] * len(outs) + [pl.BlockSpec(memory_space=pltpu.SMEM)] * len(flags),
        scratch_shapes=[pltpu.VMEM(s, jnp.float32) for s in scratch],
        compiler_params=pltpu.CompilerParams(vmem_limit_bytes=limit),
        name=kernel.__name__,
    )(*args)


def both_ways(up, down, axis):
    size = lax.axis_size(axis)
    route = [(i, i + 1) for i in range(size - 1)]
    return lax.ppermute(up, axis, route), lax.ppermute(down, axis, [(b, a) for a, b in route])


def stencil(field, damping):
    low, high = both_ways(field[-1:], field[:1], "gx")
    left, right = both_ways(field[:, -1:], field[:, :1], "yz")
    tall = jnp.concatenate([low, field, high], axis=0)
    long = jnp.concatenate([left, field, right], axis=1)
    zero = jnp.zeros_like(field[:, :, :1])
    near = tall[2:] + tall[:-2] + long[:, 2:] + long[:, :-2]
    near = near + jnp.concatenate([field[:, :, 1:], zero], axis=2) + jnp.concatenate([zero, field[:, :, :-1]], axis=2)
    return damping * field + DIFFUSION * (6.0 * field - near)


def dot(a, b):
    value = jnp.sum(a * b)
    for axis in AXES:
        value = lax.psum(value, axis)
    return value


def solve(target, guess, damping):
    resid = target - (guess + stencil(guess, damping))

    def step(_, state):
        answer, resid, direction, norm_now = state
        image = direction + stencil(direction, damping)
        alpha = norm_now / dot(direction, image)
        answer = answer + alpha * direction
        resid = resid - alpha * image
        norm_next = dot(resid, resid)
        return answer, resid, resid + (norm_next / norm_now) * direction, norm_next

    return lax.fori_loop(0, ITERS, step, (guess, resid, resid, dot(resid, resid)))[0]


def step_by_step(init_field, source, damping):
    def body(_, carry):
        lower, upper = carry
        fresh = solve(lower + source, lower, damping)
        extra = 0.5 * stencil(fresh - lower, damping)
        return fresh, solve(upper + source + extra, upper, damping)

    lower, upper = lax.fori_loop(0, STEPS, body, (init_field, init_field))
    return jnp.where(lax.axis_index("level") == 1, upper, lower)


def along_rows(block):
    size = lax.axis_size("yz")
    route = [(i, i + 1) for i in range(size - 1)] + [(size + i + 1, size + i) for i in range(size - 1)]
    return lax.ppermute(block, ("level", "yz"), route)


def swapped(block):
    return lax.ppermute(block, "level", [(0, 1), (1, 0)])


def per_device(u, f, d):
    nx, ny, nz = u.shape
    tall = 2 * ROWS + ny
    (edge,) = call(pack_rows_kernel, [(3 * nx, 2, ROWS, 128)], (u, f, d))
    halo = along_rows(edge)
    planes = (WIDE + 2 * HALF, 2, 2 * ROWS, 128)
    ups, downs = call(pack_planes_kernel, [planes] * 2, (u, f, d, halo))
    mine = (halo,) + both_ways(ups, downs, "gx")
    theirs = tuple(swapped(part) for part in mine)
    padded = (nx + 2 * WIDE, 2, tall + 2 * PAD, 128)
    first, scale, edge = call(
        first_kernel,
        [(HALF + 1, nx, 2, ny, 128), padded, (nx, 2, ROWS, 128)],
        (u, f, d) + mine + theirs,
        [padded] * 3,
    )
    halo = along_rows(edge)
    (dots,) = call(first_dots_kernel, [(8, 128)], (u, first))
    ups, downs = call(pack_vector_kernel, [(HALF, 2, 2 * ROWS, 128)] * 2, (first[HALF], halo))
    mine = (halo,) + both_ways(ups, downs, "gx")
    theirs = tuple(swapped(part) for part in mine)
    parts = lax.axis_size(AXES)
    second, dots = call(
        second_kernel,
        [(HALF - 1, nx, 2, ny, 128), (parts, 128)],
        (u, first, scale, dots) + mine + theirs,
        [padded] * 2,
    )
    gathered = lax.all_to_all(dots.reshape(parts, 1, 128), AXES, 0, 0).reshape(parts, 128)
    tables, nodes = chebyshev_tables()
    fast, flag = call(
        finish_kernel,
        [(nx, ny, nz)],
        (gathered, jnp.asarray(tables), jnp.asarray(nodes), u, first, second),
        flags=[(1, 1)],
    )
    state = lax.cond(flag.reshape(()), lambda: fast, lambda: step_by_step(u, f, d))
    return state[None]


def solution(mesh):
    placed = P("gx", "yz", None)
    return jax.shard_map(
        per_device,
        mesh=mesh,
        in_specs=(placed, placed, placed),
        out_specs=P("level", "gx", "yz", None),
        check_vma=False,
    )
```

```python
import jax
import jax.numpy as jnp
import numpy as np
from jax import lax
from jax.experimental import pallas as pl
from jax.experimental.pallas import tpu as pltpu
from jax.sharding import PartitionSpec as P

STEPS = 3
ITERS = 3
DIFFUSION = 1.0
CENTRE, RADIUS = 8.0, 7.0
HALF = 6
TOP = 2 * HALF
MOMENTS = 2 * TOP
NODES = 128
WIDE = HALF + 1
ROWS = 8
NOISE_GAIN = 4.0
ERROR_BOUND = 4e-5

AXES = ("gx", "yz")
CHECK_AT, FIELD_AT = 32, 47
LOW_AT = 64


def chebyshev_tables():
    angle = np.pi * (np.arange(NODES) + 0.5) / NODES
    exact = np.cos(np.arange(32)[:, None] * angle[None])
    first = np.round(exact * 2048.0) / 2048.0
    second = np.round((exact - first) * 2.0**23) / 2.0**23
    parts = np.concatenate([first, second, exact - first - second, exact])
    return parts.astype(np.float32), (CENTRE + RADIUS * exact[1:2]).astype(np.float32)


def total(values):
    return jnp.sum(values, axis=1, keepdims=True)


def two_sum(a, b):
    s = a + b
    t = s - a
    return s, (a - (s - t)) + (b - t)


def plus(a, b):
    s, e = two_sum(a[0], b[0])
    return two_sum(s, e + (a[1] + b[1]))


def times(scale, a):
    return scale * a[0], scale * a[1]


def halves(values):
    wide = 4097.0 * values
    high = wide - (wide - values)
    return high, values - high


def split_sum(values, axis=None):
    count = values.size if axis is None else values.shape[axis]
    most = jnp.max(jnp.abs(values), axis=axis, keepdims=True)
    unit = (4.0 * count) * most
    high = (values + unit) - unit
    return jnp.sum(high, axis=axis, keepdims=True), jnp.sum(values - high, axis=axis, keepdims=True)


def spectral_solve(resid, weight, nodes, noise):
    direction = resid
    answer = jnp.zeros_like(resid)
    norm_now = total(weight * resid * resid)
    noise_now = noise * total(resid * resid)
    error = jnp.zeros_like(norm_now)
    for step in range(ITERS):
        image = nodes * direction
        product = total(weight * direction * image)
        length = total(weight * direction * direction)
        noise_product = noise * total(direction * image)
        alpha = norm_now / product
        error = error + alpha * (noise_now / norm_now + noise_product / product) * jnp.sqrt(length)
        answer = answer + alpha * direction
        resid = resid - alpha * image
        if step + 1 < ITERS:
            norm_next = total(weight * resid * resid)
            noise_now = noise * total(resid * resid)
            direction = resid + (norm_next / norm_now) * direction
            norm_now = norm_next
    return answer, error


def coefficients(high, low, tables, nodes):
    table = tables[96:128]
    place = lax.broadcasted_iota(jnp.int32, (32, 1), 0)
    raw = high[:32], low[:32]
    base = tuple(jnp.where(place % 2 == 0, r[0:1], r[1:2]) for r in raw)
    shifted = plus(times(2.0, raw), times(-1.0, base))
    used = place < MOMENTS
    moment = tuple(jnp.where(used, jnp.where(place < 2, r, m), 0.0) for r, m in zip(raw, shifted))
    factor = jnp.where(place == 0, 1.0 / NODES, 2.0 / NODES)
    big, small = halves(factor * moment[0])
    small = small + factor * moment[1]
    parts = big * tables[:32]
    rest = big * tables[32:64] + small * tables[:32] + (big * tables[64:96] + small * tables[32:64])
    pieces = (parts, rest)
    count = 32
    while count > 1:
        count //= 2
        pieces = plus(tuple(p[:count] for p in pieces), tuple(p[count : 2 * count] for p in pieces))
    weight = pieces[0] + pieces[1]
    worst = jnp.zeros((1, 1), jnp.float32)
    at = lambda pair, k: (pair[0][k : k + 1], pair[1][k : k + 1])
    for k in range(1, TOP):
        gap = plus(times(2.0, at((high, low), CHECK_AT + k)), times(-1.0, at(moment, 2)))
        gap = plus(gap, times(-1.0, at(moment, 2 * k)))
        worst = jnp.maximum(worst, jnp.abs(gap[0] + gap[1]))
    noise = (worst + 1e-10 * high[0:1]) * (NOISE_GAIN / NODES)
    dots = high
    above = nodes - 1.0
    one = jnp.ones_like(nodes)
    path = [jnp.zeros_like(nodes)]
    second = path[0]
    errors = [jnp.zeros((1, 1), jnp.float32), jnp.zeros((1, 1), jnp.float32)]
    for rounds in range(STEPS + 1):
        lower = upper = one
        if rounds < STEPS:
            lower = one - above * path[-1]
        if rounds > 0:
            upper = one - above * second + 0.5 * above * (path[rounds] - path[rounds - 1])
        change, error = spectral_solve(jnp.concatenate([lower, upper], axis=0), weight, nodes, noise)
        if rounds > 0:
            second = second + change[1:2]
            errors[1] = errors[1] + error[1:2]
        if rounds < STEPS:
            path.append(path[-1] + change[0:1])
            errors[0] = errors[0] + error[0:1]
    results = []
    for values, error in ((path[-1], errors[0]), (second, errors[0] + errors[1])):
        part = total(table[:16] * values) * (2.0 / NODES)
        row = lax.broadcasted_iota(jnp.int32, (16, 1), 0)
        part = jnp.where(row == 0, 0.5 * part, part)
        part = jnp.where(row < TOP, part, 0.0)
        cross = jnp.sum(part * dots[FIELD_AT + 1 : FIELD_AT + 17], axis=0, keepdims=True)
        square = dots[FIELD_AT : FIELD_AT + 1] + 2.0 * cross + total(weight * values * values)
        fine = (error * error <= ERROR_BOUND * ERROR_BOUND * square) & (error >= 0.0)
        results.append((part, fine))
    return results


PAD = 8
OWN = PAD + ROWS


def by_level(lower, upper):
    return jnp.where(lax.axis_index("level") == 0, lower, upper)


def pack_rows_kernel(u, f, d, out, rows, arrived):
    nx, ny, _ = u.shape
    start = pl.multiple_of((ny - ROWS) * (1 - lax.axis_index("level")), ROWS)
    copies = [
        pltpu.make_async_copy(ref.at[:, pl.ds(start, ROWS), :], rows.at[n], arrived.at[n])
        for n, ref in enumerate((u, f, d))
    ]
    for copy in copies:
        copy.start()
    for n, copy in enumerate(copies):
        copy.wait()
        for c in range(2):
            out[n * nx : (n + 1) * nx, c] = rows[n, :, :, c * 128 : (c + 1) * 128]


def pack_planes_kernel(u, f, d, halo, to_high, to_low):
    nx, ny, _ = u.shape
    at = 0
    for n, (ref, width) in enumerate(((u, WIDE), (f, HALF), (d, HALF))):
        for out, start in ((to_high, nx - width), (to_low, 0)):
            for c in range(2):
                lanes = slice(c * 128, (c + 1) * 128)
                outer = halo[n * nx + start : n * nx + start + width, c]
                out[at : at + width, c, :ROWS] = by_level(outer, ref[start : start + width, ny - ROWS :, lanes])
                out[at : at + width, c, ROWS:] = by_level(ref[start : start + width, :ROWS, lanes], outer)
        at += width


def pack_vector_kernel(basis, halo, dots, to_high, to_low):
    _, nx, _, ny, _ = basis.shape
    for out, start in ((to_high, nx - HALF), (to_low, 0)):
        outer = halo[start : start + HALF]
        own = slice(start, start + HALF)
        out[:, :, :ROWS] = by_level(outer, basis[HALF, own, :, ny - ROWS :])
        out[:, :, ROWS:] = by_level(basis[HALF, own, :, :ROWS], outer)


def row_spans(level, ny):
    halo = pl.multiple_of(PAD + level * (ROWS + ny), 8)
    half = pl.multiple_of(PAD + level * (2 * ROWS), 8)
    return pl.ds(halo, ROWS), pl.ds(half, 2 * ROWS)


def beside(ref, i, start, count):
    here = [ref[i, c, start : start + count] for c in range(2)]
    lane = lax.broadcasted_iota(jnp.int32, (count, 128), 1)
    left = [pltpu.roll(v, 1, 1) for v in here]
    right = [pltpu.roll(v, 127, 1) for v in here]
    along = (
        jnp.where(lane == 0, 0.0, left[0]) + jnp.where(lane == 127, right[1], right[0]),
        jnp.where(lane == 0, left[0], left[1]) + jnp.where(lane == 127, 0.0, right[1]),
    )
    around = []
    for c in range(2):
        planes = ref[i + 1, c, start : start + count] + ref[i - 1, c, start : start + count]
        rows = ref[i, c, start - 1 : start - 1 + count] + ref[i, c, start + 1 : start + 1 + count]
        around.append((planes + rows) + along[c])
    return here, around


def row_mask(ny):
    row = lax.broadcasted_iota(jnp.int32, (ny + 2 * ROWS, 128), 0)
    here, count = lax.axis_index("yz"), lax.axis_size("yz")
    low = jnp.where(here == 0, ROWS, 0)
    high = jnp.where(here == count - 1, ROWS + ny, 2 * ROWS + ny)
    return jnp.where((row >= low) & (row < high), 1.0, 0.0)


def over_inner(nx, skip, body):
    def inner(i, _):
        body(i, None)
        return 0

    lax.fori_loop(WIDE + skip, WIDE + nx - skip, inner, 0, unroll=4 if (nx - 2 * skip) % 4 == 0 else 2)


def over_wedges(nx, halo, skip, body):
    here, count = lax.axis_index("gx"), lax.axis_size("gx")
    below = jnp.where(here == 0, 0.0, 1.0)
    above = jnp.where(here == count - 1, 0.0, 1.0)
    for j in range(-halo, skip):
        body(WIDE + j, below if j < 0 else None)
        body(WIDE + nx - 1 - j, above if j < 0 else None)


def put(row, index, values):
    lane = lax.broadcasted_iota(jnp.int32, row.shape, 1)
    high, low = split_sum(values)
    return jnp.where(lane == index, high, jnp.where(lane == index + LOW_AT, low, row))


def clear_margins(refs):
    count, _, tall, _ = refs[0].shape
    side = jnp.zeros((2, PAD, 128), jnp.float32)

    def margins(i, _):
        for ref in refs:
            ref[i, :, :PAD] = side
            ref[i, :, tall - PAD :] = side
        return 0

    lax.fori_loop(0, count, margins, 0, unroll=2)


def recur(src, dst, scale, pull, first_step, rows):
    start, count = rows
    offset = start - PAD
    factor = pull[offset : offset + count]

    def body(i, mask):
        here, around = beside(src, i, start, count)
        weight = factor if mask is None else factor * mask
        made = []
        for c in range(2):
            at = (i, c, slice(start, start + count))
            twice = scale[at] * here[c] - weight * around[c]
            new = 0.5 * twice if first_step else twice - dst[at]
            dst[at] = new
            made.append(new)
        return made

    return body


def first_start(wide_u, va, scale, ny):
    keep = row_mask(ny)
    rows = (PAD, ny + 2 * ROWS)

    def body(i, mask):
        here, around = beside(wide_u, i, *rows)
        inside = keep if mask is None else keep * mask
        for c in range(2):
            at = (i, c, slice(PAD, PAD + rows[1]))
            damp = scale[at]
            va[at] = inside * (va[at] - (damp * here[c] + DIFFUSION * (6.0 * here[c] - around[c])))
            scale[at] = inside * ((2.0 / RADIUS) * (damp + (1.0 + 6.0 * DIFFUSION - CENTRE)))

    return body


def first_steps(ny, wide_u, va, vb, scale, basis, over):
    pull = row_mask(ny) * (2.0 / RADIUS * DIFFUSION)
    rows = (PAD, ny + 2 * ROWS)
    begin = first_start(wide_u, va, scale, ny)

    def start(i, mask):
        begin(i, mask)
        if mask is None:
            basis[0, i - WIDE] = va[i, :, OWN : OWN + ny]

    over(HALF, 1, start)
    for k in range(HALF):
        src, dst = (va, vb) if k % 2 == 0 else (vb, va)
        last = k == HALF - 1
        step = recur(src, dst, scale, pull, k == 0, (OWN, ny) if last else rows)

        def body(i, mask, step=step, k=k, last=last):
            made = step(i, mask)
            if mask is None:
                for c in range(2):
                    basis[k + 1, i - WIDE, c] = made[c] if last else made[c][ROWS : ROWS + ny]

        over(HALF - 1 - k, k + 2, body)


def first_inner_kernel(u, f, d, mine, theirs, wide_u, va, vb, scale, basis):
    nx, ny, _ = u.shape
    level = lax.axis_index("level")
    clear_margins((wide_u, va, vb))
    for n, (ref, dst) in enumerate(((u, wide_u), (f, va), (d, scale))):
        for halo, place in ((mine, level), (theirs, 1 - level)):
            outer, _ = row_spans(place, ny)
            dst[WIDE : WIDE + nx, :, outer] = halo[n * nx : (n + 1) * nx]
        for c in range(2):
            dst[WIDE : WIDE + nx, c, OWN : OWN + ny] = ref[:, :, c * 128 : (c + 1) * 128]
    first_steps(ny, wide_u, va, vb, scale, basis, lambda halo, skip, body: over_inner(nx, skip, body))


def first_outer_kernel(*refs):
    mine, theirs = refs[:2], refs[2:4]
    wide_u, va, vb, scale, basis, edge = refs[9:]
    _, nx, _, ny, _ = basis.shape
    level = lax.axis_index("level")
    at = 0
    for width, dst in ((WIDE, wide_u), (HALF, va), (HALF, scale)):
        for (xlow, xhigh), place in ((mine, level), (theirs, 1 - level)):
            _, part = row_spans(place, ny)
            dst[WIDE - width : WIDE, :, part] = xlow[at : at + width]
            dst[WIDE + nx : WIDE + nx + width, :, part] = xhigh[at : at + width]
        at += width
    over = lambda halo, skip, body: over_wedges(nx, halo, skip, body)
    first_steps(ny, wide_u, va, vb, scale, basis, over)
    edge[...] = by_level(basis[HALF, :, :, ny - ROWS :, :], basis[HALF, :, :, :ROWS, :])


def first_dots_kernel(u, basis, dots):
    count, nx, _, ny, _ = basis.shape
    row = jnp.zeros((8, 128), jnp.float32)
    for k in range(count):

        def body(i, sums, k=k):
            terms = [[] for _ in sums]
            for c in range(2):
                own = u[i, :, c * 128 : (c + 1) * 128]
                new = basis[k, i, c]
                parts = [own * new, new * new]
                if k == 0:
                    parts.append(own * own)
                else:
                    parts.append(basis[k - 1, i, c] * new)
                if k > 1:
                    parts.append(basis[k - 2, i, c] * new)
                for t, p in zip(terms, parts):
                    t.append(p)
            return tuple((s[0] + t[0], s[1] + t[1]) for s, t in zip(sums, terms))

        zero = jnp.zeros((ny, 128), jnp.float32)
        sums = lax.fori_loop(0, nx, body, ((zero, zero),) * (4 if k > 1 else 3), unroll=4)
        where = (FIELD_AT + 1 + k, 2 * k, FIELD_AT if k == 0 else 2 * k - 1, CHECK_AT + k - 1)
        for at, (a, b) in zip(where, sums):
            row = put(row, at, jnp.concatenate([a, b], axis=0))
    dots[...] = row


def second_step(j, ny, va, vb, scale, pull, u, first, basis):
    src, dst = (va, vb) if j % 2 == 0 else (vb, va)
    last = j == HALF - 1
    step = recur(src, dst, scale, pull, j == 0, (OWN, ny) if last else (PAD, ny + 2 * ROWS))
    k = HALF + j
    get = lambda n, i, c: first[n, i, c] if n <= HALF else basis[n - HALF - 1, i, c]

    def body(i, mask, sums):
        made = step(i, mask)
        if mask is not None:
            return sums
        at = i - WIDE
        result = [list(s) for s in sums]
        for c in range(2):
            mid = made[c] if last else made[c][ROWS : ROWS + ny]
            new = 2.0 * mid - first[HALF - 1 - j, at, c]
            parts = [get(k, at, c) * new, get(k - 1, at, c) * new]
            if not last:
                basis[j, at, c] = new
                parts += [new * new, u[at, :, c * 128 : (c + 1) * 128] * new]
            for r, p in zip(result, parts):
                r[c] = r[c] + p
        return tuple(tuple(r) for r in result)

    return body, 2 if last else 4


def second_inner_kernel(mine, theirs, scale, u, first, basis, va, vb, sums):
    _, nx, _, ny, _ = basis.shape
    level = lax.axis_index("level")
    clear_margins((va, vb))
    for halo, place in ((mine, level), (theirs, 1 - level)):
        outer, _ = row_spans(place, ny)
        va[WIDE : WIDE + nx, :, outer] = halo[...]
    va[WIDE : WIDE + nx, :, OWN : OWN + ny] = first[HALF]
    pull = row_mask(ny) * (2.0 / RADIUS * DIFFUSION)
    for j in range(HALF):
        body, count = second_step(j, ny, va, vb, scale, pull, u, first, basis)
        zero = jnp.zeros((ny, 128), jnp.float32)
        low, high = WIDE + j + 1, WIDE + nx - j - 1
        run = lambda i, made, body=body: body(i, None, made)
        unroll = 4 if (high - low) % 4 == 0 else 2
        made = lax.fori_loop(low, high, run, ((zero, zero),) * count, unroll=unroll)
        for n in range(count):
            for c in range(2):
                sums[j, n, c] = made[n][c]


def second_outer_kernel(*refs):
    mine, theirs = refs[:2], refs[2:4]
    scale, u, first, before, sums = refs[4:9]
    basis, va, vb, dots = refs[12:]
    _, nx, _, ny, _ = basis.shape
    level = lax.axis_index("level")
    for (xlow, xhigh), place in ((mine, level), (theirs, 1 - level)):
        _, part = row_spans(place, ny)
        va[WIDE - HALF : WIDE, :, part] = xlow[...]
        va[WIDE + nx : WIDE + nx + HALF, :, part] = xhigh[...]
    pull = row_mask(ny) * (2.0 / RADIUS * DIFFUSION)
    row = before[...]
    for j in range(HALF):
        body, count = second_step(j, ny, va, vb, scale, pull, u, first, basis)
        made = [tuple(tuple(sums[j, n, c] for c in range(2)) for n in range(count))]

        def run(i, mask, body=body, made=made):
            made[0] = body(i, mask, made[0])

        over_wedges(nx, HALF - 1 - j, j + 1, run)
        k = HALF + j
        where = (2 * k + 1, CHECK_AT + k, 2 * k + 2, FIELD_AT + 2 + k)
        for at, (a, b) in zip(where, made[0]):
            row = put(row, at, jnp.concatenate([a, b], axis=0))
    dots[...] = jnp.broadcast_to(row[0:1], dots.shape)


def finish_kernel(gathered, tables, nodes, second, far_u, far_first, out, flag, u, first, arrived):
    nx, ny, _ = out.shape
    copies = [
        pltpu.make_async_copy(far_u, u, arrived.at[0]),
        pltpu.make_async_copy(far_first, first, arrived.at[1]),
    ]
    for copy in copies:
        copy.start()
    turned = gathered[...].T
    high, low = split_sum(turned[:LOW_AT], 1)
    high, low = two_sum(high, low + total(turned[LOW_AT:]))
    (lower, fine_low), (upper, fine_up) = coefficients(high, low, tables[...], nodes[...])
    level = lax.axis_index("level")
    part = jnp.where(level == 0, lower, upper)
    flag[0, 0] = jnp.where(jnp.min(jnp.where(fine_low & fine_up, 1.0, 0.0)) > 0.5, 1, 0)
    for copy in copies:
        copy.wait()
    factors = [jnp.broadcast_to(part[k : k + 1], (8, 128)) for k in range(TOP)]

    def body(i, _):
        for r in range(0, ny, 8):
            for c in range(2):
                value = u[i, r : r + 8, c * 128 : (c + 1) * 128]
                for k in range(TOP):
                    ref, n = (first, k) if k <= HALF else (second, k - HALF - 1)
                    value = value + factors[k] * ref[n, i, c, r : r + 8]
                out[i, r : r + 8, c * 128 : (c + 1) * 128] = value
        return 0

    lax.fori_loop(0, nx, body, 0, unroll=2)


def call(kernel, outs, args, limit=16 << 20, flags=(), alias=None, far=0, scratch=()):
    whole = pl.BlockSpec(memory_space=pltpu.VMEM)
    shapes = [jax.ShapeDtypeStruct(s, jnp.float32) for s in outs]
    return pl.pallas_call(
        kernel,
        out_shape=shapes + [jax.ShapeDtypeStruct(s, jnp.int32) for s in flags],
        in_specs=[whole] * (len(args) - far) + [pl.BlockSpec(memory_space=pltpu.HBM)] * far,
        scratch_shapes=scratch,
        out_specs=[whole] * len(outs) + [pl.BlockSpec(memory_space=pltpu.SMEM)] * len(flags),
        input_output_aliases=alias or {},
        compiler_params=pltpu.CompilerParams(vmem_limit_bytes=limit),
    )(*args)


def both_ways(up, down, axis):
    size = lax.axis_size(axis)
    route = [(i, i + 1) for i in range(size - 1)]
    high = lax.ppermute(up, axis, route)
    low = lax.ppermute(down, axis, [(b, a) for a, b in route])
    return high, low


def stencil(field, damping):
    low, high = both_ways(field[-1:], field[:1], "gx")
    left, right = both_ways(field[:, -1:], field[:, :1], "yz")
    tall = jnp.concatenate([low, field, high], axis=0)
    long = jnp.concatenate([left, field, right], axis=1)
    zero = jnp.zeros_like(field[:, :, :1])
    near = tall[2:] + tall[:-2] + long[:, 2:] + long[:, :-2]
    near = near + jnp.concatenate([field[:, :, 1:], zero], axis=2) + jnp.concatenate([zero, field[:, :, :-1]], axis=2)
    return damping * field + DIFFUSION * (6.0 * field - near)


def dot(a, b):
    value = jnp.sum(a * b)
    for axis in AXES:
        value = lax.psum(value, axis)
    return value


def solve(target, guess, damping):
    resid = target - (guess + stencil(guess, damping))

    def step(_, state):
        answer, resid, direction, norm_now = state
        image = direction + stencil(direction, damping)
        alpha = norm_now / dot(direction, image)
        answer = answer + alpha * direction
        resid = resid - alpha * image
        norm_next = dot(resid, resid)
        return answer, resid, resid + (norm_next / norm_now) * direction, norm_next

    return lax.fori_loop(0, ITERS, step, (guess, resid, resid, dot(resid, resid)))[0]


def step_by_step(init_field, source, damping):
    def body(_, carry):
        lower, upper = carry
        fresh = solve(lower + source, lower, damping)
        extra = 0.5 * stencil(fresh - lower, damping)
        return fresh, solve(upper + source + extra, upper, damping)

    lower, upper = lax.fori_loop(0, STEPS, body, (init_field, init_field))
    return jnp.where(lax.axis_index("level") == 1, upper, lower)


def along_rows(block):
    size = lax.axis_size("yz")
    route = [(i, i + 1) for i in range(size - 1)] + [(size + i + 1, size + i) for i in range(size - 1)]
    return lax.ppermute(block, ("level", "yz"), route)


def swapped(block):
    return lax.ppermute(block, "level", [(0, 1), (1, 0)])


def per_device(u, f, d):
    nx, ny, nz = u.shape
    tall = 2 * ROWS + ny
    (edge,) = call(
        pack_rows_kernel,
        [(3 * nx, 2, ROWS, 128)],
        (u, f, d),
        far=3,
        scratch=[pltpu.VMEM((3, nx, ROWS, nz), jnp.float32), pltpu.SemaphoreType.DMA((3,))],
    )
    halo = along_rows(edge)
    planes = (WIDE + 2 * HALF, 2, 2 * ROWS, 128)
    ups, downs = call(pack_planes_kernel, [planes] * 2, (u, f, d, halo))
    theirs = swapped(halo)
    wide = (nx + 2 * WIDE, 2, tall + 2 * PAD, 128)
    block = (nx, 2, ny, 128)
    mine = both_ways(ups, downs, "gx")
    buffers = call(first_inner_kernel, [wide] * 4 + [(HALF + 1,) + block], (u, f, d, halo, theirs))
    *_, scale, first, edge = call(
        first_outer_kernel,
        [wide] * 4 + [(HALF + 1,) + block, (nx, 2, ROWS, 128)],
        mine + tuple(swapped(part) for part in mine) + tuple(buffers),
        alias={4 + n: n for n in range(5)},
    )
    halo = along_rows(edge)
    theirs = swapped(halo)
    (dots,) = call(first_dots_kernel, [(8, 128)], (u, first))
    ups, downs = call(pack_vector_kernel, [(HALF, 2, 2 * ROWS, 128)] * 2, (first, halo, dots))
    mine = both_ways(ups, downs, "gx")
    second, va, vb, sums = call(
        second_inner_kernel,
        [(HALF - 1,) + block, wide, wide, (HALF, 4, 2, ny, 128)],
        (halo, theirs, scale, u, first),
    )
    parts = lax.axis_size(AXES)
    second, _, _, dots = call(
        second_outer_kernel,
        [(HALF - 1,) + block, wide, wide, (parts, 128)],
        mine + tuple(swapped(part) for part in mine) + (scale, u, first, dots, sums, second, va, vb),
        alias={9: 0, 10: 1, 11: 2},
    )
    gathered = lax.all_to_all(dots.reshape(parts, 1, 128), AXES, 0, 0).reshape(parts, 128)
    tables, nodes = chebyshev_tables()
    fast, flag = call(
        finish_kernel,
        [(nx, ny, nz)],
        (gathered, jnp.asarray(tables), jnp.asarray(nodes), second, u, first),
        flags=[(1, 1)],
        far=2,
        scratch=[
            pltpu.VMEM((nx, ny, nz), jnp.float32),
            pltpu.VMEM((HALF + 1,) + block, jnp.float32),
            pltpu.SemaphoreType.DMA((2,)),
        ],
    )
    state = lax.cond(flag.reshape(()), lambda: fast, lambda: step_by_step(u, f, d))
    return state[None]


def solution(mesh):
    placed = P("gx", "yz", None)
    return jax.shard_map(
        per_device,
        mesh=mesh,
        in_specs=(placed, placed, placed),
        out_specs=P("level", "gx", "yz", None),
        check_vma=False,
    )
```

```python
import functools

import jax
import jax.numpy as jnp
import numpy as np
from jax import lax
from jax.experimental import pallas as pl
from jax.experimental.pallas import tpu as pltpu
from jax.sharding import PartitionSpec as P

STEPS = 3
ITERS = 3
DIFFUSION = 1.0
CENTRE, RADIUS = 8.0, 7.0
HALF = 6
TOP = 2 * HALF
MOMENTS = 2 * TOP
NODES = 128
WIDE = HALF + 1
ROWS = 8
NOISE_GAIN = 4.0
ERROR_BOUND = 4e-5

AXES = ("gx", "yz")
CHECK_AT, FIELD_AT = 32, 47
LOW_AT = 64


def chebyshev_tables():
    angle = np.pi * (np.arange(NODES) + 0.5) / NODES
    exact = np.cos(np.arange(32)[:, None] * angle[None])
    first = np.round(exact * 2048.0) / 2048.0
    second = np.round((exact - first) * 2.0**23) / 2.0**23
    parts = np.concatenate([first, second, exact - first - second, exact])
    return parts.astype(np.float32), (CENTRE + RADIUS * exact[1:2]).astype(np.float32)


def total(values):
    return jnp.sum(values, axis=1, keepdims=True)


def two_sum(a, b):
    s = a + b
    t = s - a
    return s, (a - (s - t)) + (b - t)


def plus(a, b):
    s, e = two_sum(a[0], b[0])
    return two_sum(s, e + (a[1] + b[1]))


def times(scale, a):
    return scale * a[0], scale * a[1]


def halves(values):
    wide = 4097.0 * values
    high = wide - (wide - values)
    return high, values - high


def split_sum(values, axis):
    most = jnp.max(jnp.abs(values), axis=axis, keepdims=True)
    unit = (4.0 * values.shape[axis]) * most
    high = (values + unit) - unit
    return jnp.sum(high, axis=axis, keepdims=True), jnp.sum(values - high, axis=axis, keepdims=True)


def spectral_solve(resid, weight, nodes, noise):
    direction = resid
    answer = jnp.zeros_like(resid)
    norm_now = total(weight * resid * resid)
    noise_now = noise * total(resid * resid)
    error = jnp.zeros_like(norm_now)
    for step in range(ITERS):
        image = nodes * direction
        product = total(weight * direction * image)
        length = total(weight * direction * direction)
        noise_product = noise * total(direction * image)
        alpha = norm_now / product
        error = error + alpha * (noise_now / norm_now + noise_product / product) * jnp.sqrt(length)
        answer = answer + alpha * direction
        resid = resid - alpha * image
        if step + 1 < ITERS:
            norm_next = total(weight * resid * resid)
            noise_now = noise * total(resid * resid)
            direction = resid + (norm_next / norm_now) * direction
            norm_now = norm_next
    return answer, error


def coefficients(high, low, tables, nodes):
    table = tables[96:128]
    place = lax.broadcasted_iota(jnp.int32, (32, 1), 0)
    raw = high[:32], low[:32]
    base = tuple(jnp.where(place % 2 == 0, r[0:1], r[1:2]) for r in raw)
    shifted = plus(times(2.0, raw), times(-1.0, base))
    used = place < MOMENTS
    moment = tuple(jnp.where(used, jnp.where(place < 2, r, m), 0.0) for r, m in zip(raw, shifted))
    factor = jnp.where(place == 0, 1.0 / NODES, 2.0 / NODES)
    big, small = halves(factor * moment[0])
    small = small + factor * moment[1]
    parts = big * tables[:32]
    rest = big * tables[32:64] + small * tables[:32] + (big * tables[64:96] + small * tables[32:64])
    pieces = (parts, rest)
    count = 32
    while count > 1:
        count //= 2
        pieces = plus(tuple(p[:count] for p in pieces), tuple(p[count : 2 * count] for p in pieces))
    weight = pieces[0] + pieces[1]
    worst = jnp.zeros((1, 1), jnp.float32)
    at = lambda pair, k: (pair[0][k : k + 1], pair[1][k : k + 1])
    for k in range(1, TOP):
        gap = plus(times(2.0, at((high, low), CHECK_AT + k)), times(-1.0, at(moment, 2)))
        gap = plus(gap, times(-1.0, at(moment, 2 * k)))
        worst = jnp.maximum(worst, jnp.abs(gap[0] + gap[1]))
    noise = (worst + 1e-10 * high[0:1]) * (NOISE_GAIN / NODES)
    dots = high
    above = nodes - 1.0
    one = jnp.ones_like(nodes)
    path = [jnp.zeros_like(nodes)]
    second = path[0]
    errors = [jnp.zeros((1, 1), jnp.float32), jnp.zeros((1, 1), jnp.float32)]
    for rounds in range(STEPS + 1):
        lower = upper = one
        if rounds < STEPS:
            lower = one - above * path[-1]
        if rounds > 0:
            upper = one - above * second + 0.5 * above * (path[rounds] - path[rounds - 1])
        change, error = spectral_solve(jnp.concatenate([lower, upper], axis=0), weight, nodes, noise)
        if rounds > 0:
            second = second + change[1:2]
            errors[1] = errors[1] + error[1:2]
        if rounds < STEPS:
            path.append(path[-1] + change[0:1])
            errors[0] = errors[0] + error[0:1]
    results = []
    for values, error in ((path[-1], errors[0]), (second, errors[0] + errors[1])):
        part = total(table[:16] * values) * (2.0 / NODES)
        row = lax.broadcasted_iota(jnp.int32, (16, 1), 0)
        part = jnp.where(row == 0, 0.5 * part, part)
        part = jnp.where(row < TOP, part, 0.0)
        cross = jnp.sum(part * dots[FIELD_AT + 1 : FIELD_AT + 17], axis=0, keepdims=True)
        square = dots[FIELD_AT : FIELD_AT + 1] + 2.0 * cross + total(weight * values * values)
        fine = (error * error <= ERROR_BOUND * ERROR_BOUND * square) & (error >= 0.0)
        results.append((part, fine))
    return results


PAD = 8
OWN = PAD + ROWS


def by_level(lower, upper):
    return jnp.where(lax.axis_index("level") == 0, lower, upper)


def pack_first_kernel(u, f, d, rows_out, planes_out, rows, planes, arrived):
    nx, ny, _ = u.shape
    level = lax.axis_index("level")
    start = pl.multiple_of((ny - ROWS) * (1 - level), ROWS)
    copies = []
    for n, (ref, width) in enumerate(((u, WIDE), (f, HALF), (d, HALF))):
        begin = (nx - width) * (1 - level)
        copies += [
            pltpu.make_async_copy(ref.at[:, pl.ds(start, ROWS), :], rows.at[n], arrived.at[2 * n]),
            pltpu.make_async_copy(ref.at[pl.ds(begin, width)], planes.at[n, :width], arrived.at[2 * n + 1]),
        ]
    for copy in copies:
        copy.start()
    at = 0
    for n, width in enumerate((WIDE, HALF, HALF)):
        copies[2 * n].wait()
        copies[2 * n + 1].wait()
        for c in range(2):
            lanes = slice(c * 128, (c + 1) * 128)
            rows_out[n * nx : (n + 1) * nx, c] = rows[n, :, :, lanes]
            planes_out[at : at + width, c] = planes[n, :width, :, lanes]
        at += width


def pack_corners_kernel(mine, theirs, out):
    width, _, ny, _ = mine.shape
    for n, planes in enumerate((by_level(mine[...], theirs[...]), by_level(theirs[...], mine[...]))):
        out[n * width : (n + 1) * width] = by_level(planes[:, :, ny - ROWS :], planes[:, :, :ROWS])


def pack_vector_kernel(basis, halo, dots, to_high, to_low):
    _, nx, _, ny, _ = basis.shape
    for out, start in ((to_high, nx - HALF), (to_low, 0)):
        outer = halo[start : start + HALF]
        own = slice(start, start + HALF)
        out[:, :, :ROWS] = by_level(outer, basis[HALF, own, :, ny - ROWS :])
        out[:, :, ROWS:] = by_level(basis[HALF, own, :, :ROWS], outer)


def row_spans(level, ny):
    halo = pl.multiple_of(PAD + level * (ROWS + ny), 8)
    half = pl.multiple_of(PAD + level * (2 * ROWS), 8)
    return pl.ds(halo, ROWS), pl.ds(half, 2 * ROWS)


def beside(ref, i, start, count):
    here = [ref[i, c, start : start + count] for c in range(2)]
    lane = lax.broadcasted_iota(jnp.int32, (count, 128), 1)
    left = [pltpu.roll(v, 1, 1) for v in here]
    right = [pltpu.roll(v, 127, 1) for v in here]
    along = (
        jnp.where(lane == 0, 0.0, left[0]) + jnp.where(lane == 127, right[1], right[0]),
        jnp.where(lane == 0, left[0], left[1]) + jnp.where(lane == 127, 0.0, right[1]),
    )
    around = []
    for c in range(2):
        planes = ref[i + 1, c, start : start + count] + ref[i - 1, c, start : start + count]
        rows = ref[i, c, start - 1 : start - 1 + count] + ref[i, c, start + 1 : start + 1 + count]
        around.append((planes + rows) + along[c])
    return here, around


def row_mask(ny):
    row = lax.broadcasted_iota(jnp.int32, (ny + 2 * ROWS, 128), 0)
    here, count = lax.axis_index("yz"), lax.axis_size("yz")
    low = jnp.where(here == 0, ROWS, 0)
    high = jnp.where(here == count - 1, ROWS + ny, 2 * ROWS + ny)
    return jnp.where((row >= low) & (row < high), 1.0, 0.0)


def over_inner(nx, skip, body):
    def inner(i, _):
        body(i, None)
        return 0

    lax.fori_loop(WIDE + skip, WIDE + nx - skip, inner, 0, unroll=4 if (nx - 2 * skip) % 4 == 0 else 2)


def over_wedges(nx, halo, skip, body):
    here, count = lax.axis_index("gx"), lax.axis_size("gx")
    below = jnp.where(here == 0, 0.0, 1.0)
    above = jnp.where(here == count - 1, 0.0, 1.0)
    for j in range(-halo, skip):
        body(WIDE + j, below if j < 0 else None)
        body(WIDE + nx - 1 - j, above if j < 0 else None)


def put(row, entries):
    lane = lax.broadcasted_iota(jnp.int32, row.shape, 1)
    most = functools.reduce(jnp.maximum, [jnp.abs(half) for _, halves_ in entries for half in halves_])
    unit = (8.0 * most.size) * jnp.max(most, keepdims=True)
    for at, pair in entries:
        rounded = [(half + unit) - unit for half in pair]
        high = jnp.sum(rounded[0] + rounded[1], keepdims=True)
        low = jnp.sum((pair[0] - rounded[0]) + (pair[1] - rounded[1]), keepdims=True)
        row = jnp.where(lane == at, high, jnp.where(lane == at + LOW_AT, low, row))
    return row


def clear_margins(refs):
    count, _, tall, _ = refs[0].shape
    side = jnp.zeros((2, PAD, 128), jnp.float32)

    def margins(i, _):
        for ref in refs:
            ref[i, :, :PAD] = side
            ref[i, :, tall - PAD :] = side
        return 0

    lax.fori_loop(0, count, margins, 0, unroll=2)


def recur(src, dst, scale, pull, first_step, rows):
    start, count = rows
    offset = start - PAD
    factor = pull[offset : offset + count]

    def body(i, mask):
        here, around = beside(src, i, start, count)
        weight = factor if mask is None else factor * mask
        made = []
        for c in range(2):
            at = (i, c, slice(start, start + count))
            twice = scale[at] * here[c] - weight * around[c]
            new = 0.5 * twice if first_step else twice - dst[at]
            dst[at] = new
            made.append(new)
        return made

    return body


def first_start(wide_u, va, scale, ny):
    keep = row_mask(ny)
    rows = (PAD, ny + 2 * ROWS)

    def body(i, mask):
        here, around = beside(wide_u, i, *rows)
        inside = keep if mask is None else keep * mask
        for c in range(2):
            at = (i, c, slice(PAD, PAD + rows[1]))
            damp = scale[at]
            va[at] = inside * (va[at] - (damp * here[c] + DIFFUSION * (6.0 * here[c] - around[c])))
            scale[at] = inside * ((2.0 / RADIUS) * (damp + (1.0 + 6.0 * DIFFUSION - CENTRE)))

    return body


def first_steps(ny, wide_u, va, vb, scale, basis, over):
    pull = row_mask(ny) * (2.0 / RADIUS * DIFFUSION)
    rows = (PAD, ny + 2 * ROWS)
    begin = first_start(wide_u, va, scale, ny)

    def start(i, mask):
        begin(i, mask)
        if mask is None:
            basis[0, i - WIDE] = va[i, :, OWN : OWN + ny]

    over(HALF, 1, start)
    for k in range(HALF):
        src, dst = (va, vb) if k % 2 == 0 else (vb, va)
        last = k == HALF - 1
        step = recur(src, dst, scale, pull, k == 0, (OWN, ny) if last else rows)

        def body(i, mask, step=step, k=k, last=last):
            made = step(i, mask)
            if mask is None:
                for c in range(2):
                    basis[k + 1, i - WIDE, c] = made[c] if last else made[c][ROWS : ROWS + ny]

        over(HALF - 1 - k, k + 2, body)


def first_inner_kernel(u, f, d, mine, theirs, wide_u, va, vb, scale, basis):
    nx, ny, _ = u.shape
    level = lax.axis_index("level")
    clear_margins((wide_u, va, vb))
    for n, (ref, dst) in enumerate(((u, wide_u), (f, va), (d, scale))):
        for halo, place in ((mine, level), (theirs, 1 - level)):
            outer, _ = row_spans(place, ny)
            dst[WIDE : WIDE + nx, :, outer] = halo[n * nx : (n + 1) * nx]
        for c in range(2):
            dst[WIDE : WIDE + nx, c, OWN : OWN + ny] = ref[:, :, c * 128 : (c + 1) * 128]
    first_steps(ny, wide_u, va, vb, scale, basis, lambda halo, skip, body: over_inner(nx, skip, body))


def first_outer_kernel(*refs):
    mine, theirs = refs[:2], refs[2:4]
    wide_u, va, vb, scale, basis, edge = refs[9:]
    _, nx, _, ny, _ = basis.shape
    level = lax.axis_index("level")
    at = 0
    corner = WIDE + 2 * HALF
    for width, dst in ((WIDE, wide_u), (HALF, va), (HALF, scale)):
        for (planes, corners), place in ((mine, level), (theirs, 1 - level)):
            outer, _ = row_spans(place, ny)
            begin = WIDE - width + place * (nx + width)
            dst[pl.ds(begin, width), :, OWN : OWN + ny] = planes[at : at + width]
            dst[WIDE - width : WIDE, :, outer] = corners[at : at + width]
            dst[WIDE + nx : WIDE + nx + width, :, outer] = corners[corner + at : corner + at + width]
        at += width
    over = lambda halo, skip, body: over_wedges(nx, halo, skip, body)
    first_steps(ny, wide_u, va, vb, scale, basis, over)
    edge[...] = by_level(basis[HALF, :, :, ny - ROWS :, :], basis[HALF, :, :, :ROWS, :])


def first_dots_kernel(u, basis, dots):
    count, nx, _, ny, _ = basis.shape
    row = jnp.zeros((8, 128), jnp.float32)
    entries = []
    for k in range(count):

        def body(i, sums, k=k):
            terms = [[] for _ in sums]
            for c in range(2):
                own = u[i, :, c * 128 : (c + 1) * 128]
                new = basis[k, i, c]
                parts = [own * new, new * new]
                if k == 0:
                    parts.append(own * own)
                else:
                    parts.append(basis[k - 1, i, c] * new)
                if k > 1:
                    parts.append(basis[k - 2, i, c] * new)
                for t, p in zip(terms, parts):
                    t.append(p)
            return tuple((s[0] + t[0], s[1] + t[1]) for s, t in zip(sums, terms))

        zero = jnp.zeros((ny, 128), jnp.float32)
        sums = lax.fori_loop(0, nx, body, ((zero, zero),) * (4 if k > 1 else 3), unroll=4)
        where = (FIELD_AT + 1 + k, 2 * k, FIELD_AT if k == 0 else 2 * k - 1, CHECK_AT + k - 1)
        entries += zip(where, sums)
    dots[...] = put(row, entries)


def second_step(j, ny, va, vb, scale, pull, u, first, basis):
    src, dst = (va, vb) if j % 2 == 0 else (vb, va)
    last = j == HALF - 1
    step = recur(src, dst, scale, pull, j == 0, (OWN, ny) if last else (PAD, ny + 2 * ROWS))
    k = HALF + j
    get = lambda n, i, c: first[n, i, c] if n <= HALF else basis[n - HALF - 1, i, c]

    def body(i, mask, sums):
        made = step(i, mask)
        if mask is not None:
            return sums
        at = i - WIDE
        result = [list(s) for s in sums]
        for c in range(2):
            mid = made[c] if last else made[c][ROWS : ROWS + ny]
            new = 2.0 * mid - first[HALF - 1 - j, at, c]
            parts = [get(k, at, c) * new, get(k - 1, at, c) * new]
            if not last:
                basis[j, at, c] = new
                parts += [new * new, u[at, :, c * 128 : (c + 1) * 128] * new]
            for r, p in zip(result, parts):
                r[c] = r[c] + p
        return tuple(tuple(r) for r in result)

    return body, 2 if last else 4


def second_inner_kernel(mine, theirs, scale, u, first, basis, va, vb, sums):
    _, nx, _, ny, _ = basis.shape
    level = lax.axis_index("level")
    clear_margins((va, vb))
    for halo, place in ((mine, level), (theirs, 1 - level)):
        outer, _ = row_spans(place, ny)
        va[WIDE : WIDE + nx, :, outer] = halo[...]
    va[WIDE : WIDE + nx, :, OWN : OWN + ny] = first[HALF]
    pull = row_mask(ny) * (2.0 / RADIUS * DIFFUSION)
    for j in range(HALF):
        body, count = second_step(j, ny, va, vb, scale, pull, u, first, basis)
        zero = jnp.zeros((ny, 128), jnp.float32)
        low, high = WIDE + j + 1, WIDE + nx - j - 1
        run = lambda i, made, body=body: body(i, None, made)
        unroll = 4 if (high - low) % 4 == 0 else 2
        made = lax.fori_loop(low, high, run, ((zero, zero),) * count, unroll=unroll)
        for n in range(count):
            for c in range(2):
                sums[j, n, c] = made[n][c]


def second_outer_kernel(*refs):
    mine, theirs = refs[:2], refs[2:4]
    scale, u, first, before, sums = refs[4:9]
    basis, va, vb, dots = refs[12:]
    _, nx, _, ny, _ = basis.shape
    level = lax.axis_index("level")
    for (xlow, xhigh), place in ((mine, level), (theirs, 1 - level)):
        _, part = row_spans(place, ny)
        va[WIDE - HALF : WIDE, :, part] = xlow[...]
        va[WIDE + nx : WIDE + nx + HALF, :, part] = xhigh[...]
    pull = row_mask(ny) * (2.0 / RADIUS * DIFFUSION)
    entries = []
    for j in range(HALF):
        body, count = second_step(j, ny, va, vb, scale, pull, u, first, basis)
        made = [tuple(tuple(sums[j, n, c] for c in range(2)) for n in range(count))]

        def run(i, mask, body=body, made=made):
            made[0] = body(i, mask, made[0])

        over_wedges(nx, HALF - 1 - j, j + 1, run)
        k = HALF + j
        where = (2 * k + 1, CHECK_AT + k, 2 * k + 2, FIELD_AT + 2 + k)
        entries += zip(where, made[0])
    row = put(before[...], entries)
    dots[...] = jnp.broadcast_to(row[0:1], dots.shape)


def finish_kernel(gathered, tables, nodes, second, far_u, far_first, out, flag, u, first, arrived):
    nx, ny, _ = out.shape
    copies = [
        pltpu.make_async_copy(far_u, u, arrived.at[0]),
        pltpu.make_async_copy(far_first, first, arrived.at[1]),
    ]
    for copy in copies:
        copy.start()
    turned = gathered[...].T
    high, low = split_sum(turned[:LOW_AT], 1)
    high, low = two_sum(high, low + total(turned[LOW_AT:]))
    (lower, fine_low), (upper, fine_up) = coefficients(high, low, tables[...], nodes[...])
    level = lax.axis_index("level")
    part = jnp.where(level == 0, lower, upper)
    flag[0, 0] = jnp.where(jnp.min(jnp.where(fine_low & fine_up, 1.0, 0.0)) > 0.5, 1, 0)
    for copy in copies:
        copy.wait()
    factors = [jnp.broadcast_to(part[k : k + 1], (8, 128)) for k in range(TOP)]

    def body(i, _):
        for r in range(0, ny, 8):
            for c in range(2):
                value = u[i, r : r + 8, c * 128 : (c + 1) * 128]
                for k in range(TOP):
                    ref, n = (first, k) if k <= HALF else (second, k - HALF - 1)
                    value = value + factors[k] * ref[n, i, c, r : r + 8]
                out[i, r : r + 8, c * 128 : (c + 1) * 128] = value
        return 0

    lax.fori_loop(0, nx, body, 0, unroll=2)


def call(kernel, outs, args, limit=16 << 20, flags=(), alias=None, far=0, scratch=()):
    whole = pl.BlockSpec(memory_space=pltpu.VMEM)
    shapes = [jax.ShapeDtypeStruct(s, jnp.float32) for s in outs]
    near = len(args) - far
    args = tuple(args[:near]) + tuple(pltpu.with_memory_space_constraint(a, pltpu.HBM) for a in args[near:])
    return pl.pallas_call(
        kernel,
        out_shape=shapes + [jax.ShapeDtypeStruct(s, jnp.int32) for s in flags],
        in_specs=[whole] * near + [pl.BlockSpec(memory_space=pltpu.HBM)] * far,
        scratch_shapes=scratch,
        out_specs=[whole] * len(outs) + [pl.BlockSpec(memory_space=pltpu.SMEM)] * len(flags),
        input_output_aliases=alias or {},
        compiler_params=pltpu.CompilerParams(vmem_limit_bytes=limit),
    )(*args)


def both_ways(up, down, axis):
    size = lax.axis_size(axis)
    route = [(i, i + 1) for i in range(size - 1)]
    high = lax.ppermute(up, axis, route)
    low = lax.ppermute(down, axis, [(b, a) for a, b in route])
    return high, low


def stencil(field, damping):
    low, high = both_ways(field[-1:], field[:1], "gx")
    left, right = both_ways(field[:, -1:], field[:, :1], "yz")
    tall = jnp.concatenate([low, field, high], axis=0)
    long = jnp.concatenate([left, field, right], axis=1)
    zero = jnp.zeros_like(field[:, :, :1])
    near = tall[2:] + tall[:-2] + long[:, 2:] + long[:, :-2]
    near = near + jnp.concatenate([field[:, :, 1:], zero], axis=2) + jnp.concatenate([zero, field[:, :, :-1]], axis=2)
    return damping * field + DIFFUSION * (6.0 * field - near)


def dot(a, b):
    value = jnp.sum(a * b)
    for axis in AXES:
        value = lax.psum(value, axis)
    return value


def solve(target, guess, damping):
    resid = target - (guess + stencil(guess, damping))

    def step(_, state):
        answer, resid, direction, norm_now = state
        image = direction + stencil(direction, damping)
        alpha = norm_now / dot(direction, image)
        answer = answer + alpha * direction
        resid = resid - alpha * image
        norm_next = dot(resid, resid)
        return answer, resid, resid + (norm_next / norm_now) * direction, norm_next

    return lax.fori_loop(0, ITERS, step, (guess, resid, resid, dot(resid, resid)))[0]


def step_by_step(init_field, source, damping):
    def body(_, carry):
        lower, upper = carry
        fresh = solve(lower + source, lower, damping)
        extra = 0.5 * stencil(fresh - lower, damping)
        return fresh, solve(upper + source + extra, upper, damping)

    begin = jnp.minimum(init_field, jnp.finfo(jnp.float32).max)
    lower, upper = lax.fori_loop(0, STEPS, body, (begin, begin))
    return jnp.where(lax.axis_index("level") == 1, upper, lower)


def shifted(block, axis):
    size = lax.axis_size(axis)
    route = [(i, i + 1) for i in range(size - 1)] + [(size + i + 1, size + i) for i in range(size - 1)]
    return lax.ppermute(block, ("level", axis), route)


def swapped(block):
    return lax.ppermute(block, "level", [(0, 1), (1, 0)])


def per_device(u, f, d):
    nx, ny, nz = u.shape
    tall = 2 * ROWS + ny
    deep = WIDE + 2 * HALF
    rows, planes = call(
        pack_first_kernel,
        [(3 * nx, 2, ROWS, 128), (deep, 2, ny, 128)],
        (u, f, d),
        far=3,
        scratch=[
            pltpu.VMEM((3, nx, ROWS, nz), jnp.float32),
            pltpu.VMEM((3, WIDE, ny, nz), jnp.float32),
            pltpu.SemaphoreType.DMA((6,)),
        ],
    )
    planes = shifted(planes, "gx")
    halo = shifted(rows, "yz")
    others = swapped(planes)
    (corners,) = call(pack_corners_kernel, [(2 * deep, 2, ROWS, 128)], (planes, others))
    corners = shifted(corners, "yz")
    theirs = swapped(halo)
    wide = (nx + 2 * WIDE, 2, tall + 2 * PAD, 128)
    block = (nx, 2, ny, 128)
    opposite = swapped(corners)
    buffers = call(first_inner_kernel, [wide] * 4 + [(HALF + 1,) + block], (u, f, d, halo, theirs))
    *_, scale, first, edge = call(
        first_outer_kernel,
        [wide] * 4 + [(HALF + 1,) + block, (nx, 2, ROWS, 128)],
        (planes, corners, others, opposite) + tuple(buffers),
        alias={4 + n: n for n in range(5)},
    )
    halo = shifted(edge, "yz")
    theirs = swapped(halo)
    (dots,) = call(first_dots_kernel, [(8, 128)], (u, first))
    ups, downs = call(pack_vector_kernel, [(HALF, 2, 2 * ROWS, 128)] * 2, (first, halo, dots))
    mine = both_ways(ups, downs, "gx")
    second, va, vb, sums = call(
        second_inner_kernel,
        [(HALF - 1,) + block, wide, wide, (HALF, 4, 2, ny, 128)],
        (halo, theirs, scale, u, first),
    )
    parts = lax.axis_size(AXES)
    second, _, _, dots = call(
        second_outer_kernel,
        [(HALF - 1,) + block, wide, wide, (parts, 128)],
        mine + tuple(swapped(part) for part in mine) + (scale, u, first, dots, sums, second, va, vb),
        alias={9: 0, 10: 1, 11: 2},
    )
    gathered = lax.all_to_all(dots.reshape(parts, 1, 128), AXES, 0, 0).reshape(parts, 128)
    tables, nodes = chebyshev_tables()
    fast, flag = call(
        finish_kernel,
        [(nx, ny, nz)],
        (gathered, jnp.asarray(tables), jnp.asarray(nodes), second, u, first),
        flags=[(1, 1)],
        far=2,
        scratch=[
            pltpu.VMEM((nx, ny, nz), jnp.float32),
            pltpu.VMEM((HALF + 1,) + block, jnp.float32),
            pltpu.SemaphoreType.DMA((2,)),
        ],
    )
    state = lax.cond(flag.reshape(()), lambda: fast, lambda: step_by_step(u, f, d))
    return state[None]


def solution(mesh):
    placed = P("gx", "yz", None)
    return jax.shard_map(
        per_device,
        mesh=mesh,
        in_specs=(placed, placed, placed),
        out_specs=P("level", "gx", "yz", None),
        check_vma=False,
    )
```

```python
import functools

import jax
import jax.numpy as jnp
import numpy as np
from jax import lax
from jax.experimental import pallas as pl
from jax.experimental.pallas import tpu as pltpu
from jax.sharding import PartitionSpec as P

STEPS = 3
ITERS = 3
DIFFUSION = 1.0
CENTRE, RADIUS = 8.0, 7.0
HALF = 6
TOP = 2 * HALF
MOMENTS = 2 * TOP
NODES = 128
WIDE = HALF + 1
ROWS = 8
FIRST_CUT, SECOND_CUT = 2, 2
NOISE_GAIN = 4.0
ERROR_BOUND = 4e-5

AXES = ("gx", "yz")
CHECK_AT, FIELD_AT = 32, 47
LOW_AT = 64


def chebyshev_tables():
    angle = np.pi * (np.arange(NODES) + 0.5) / NODES
    exact = np.cos(np.arange(32)[:, None] * angle[None])
    first = np.round(exact * 2048.0) / 2048.0
    second = np.round((exact - first) * 2.0**23) / 2.0**23
    parts = np.concatenate([first, second, exact - first - second, exact])
    return parts.astype(np.float32), (CENTRE + RADIUS * exact[1:2]).astype(np.float32)


def total(values):
    return jnp.sum(values, axis=1, keepdims=True)


def two_sum(a, b):
    s = a + b
    t = s - a
    return s, (a - (s - t)) + (b - t)


def plus(a, b):
    s, e = two_sum(a[0], b[0])
    return two_sum(s, e + (a[1] + b[1]))


def times(scale, a):
    return scale * a[0], scale * a[1]


def halves(values):
    wide = 4097.0 * values
    high = wide - (wide - values)
    return high, values - high


def split_sum(values, axis):
    most = jnp.max(jnp.abs(values), axis=axis, keepdims=True)
    unit = (4.0 * values.shape[axis]) * most
    high = (values + unit) - unit
    return jnp.sum(high, axis=axis, keepdims=True), jnp.sum(values - high, axis=axis, keepdims=True)


def spectral_solve(resid, weight, nodes, noise):
    direction = resid
    answer = jnp.zeros_like(resid)
    norm_now = total(weight * resid * resid)
    noise_now = noise * total(resid * resid)
    error = jnp.zeros_like(norm_now)
    for step in range(ITERS):
        image = nodes * direction
        product = total(weight * direction * image)
        length = total(weight * direction * direction)
        noise_product = noise * total(direction * image)
        alpha = norm_now / product
        error = error + alpha * (noise_now / norm_now + noise_product / product) * jnp.sqrt(length)
        answer = answer + alpha * direction
        resid = resid - alpha * image
        if step + 1 < ITERS:
            norm_next = total(weight * resid * resid)
            noise_now = noise * total(resid * resid)
            direction = resid + (norm_next / norm_now) * direction
            norm_now = norm_next
    return answer, error


def coefficients(high, low, tables, nodes):
    table = tables[96:128]
    place = lax.broadcasted_iota(jnp.int32, (32, 1), 0)
    raw = high[:32], low[:32]
    base = tuple(jnp.where(place % 2 == 0, r[0:1], r[1:2]) for r in raw)
    shifted = plus(times(2.0, raw), times(-1.0, base))
    used = place < MOMENTS
    moment = tuple(jnp.where(used, jnp.where(place < 2, r, m), 0.0) for r, m in zip(raw, shifted))
    factor = jnp.where(place == 0, 1.0 / NODES, 2.0 / NODES)
    big, small = halves(factor * moment[0])
    small = small + factor * moment[1]
    parts = big * tables[:32]
    rest = big * tables[32:64] + small * tables[:32] + (big * tables[64:96] + small * tables[32:64])
    pieces = (parts, rest)
    count = 32
    while count > 1:
        count //= 2
        pieces = plus(tuple(p[:count] for p in pieces), tuple(p[count : 2 * count] for p in pieces))
    weight = pieces[0] + pieces[1]
    worst = jnp.zeros((1, 1), jnp.float32)
    at = lambda pair, k: (pair[0][k : k + 1], pair[1][k : k + 1])
    for k in range(1, TOP):
        gap = plus(times(2.0, at((high, low), CHECK_AT + k)), times(-1.0, at(moment, 2)))
        gap = plus(gap, times(-1.0, at(moment, 2 * k)))
        worst = jnp.maximum(worst, jnp.abs(gap[0] + gap[1]))
    noise = (worst + 1e-10 * high[0:1]) * (NOISE_GAIN / NODES)
    dots = high
    above = nodes - 1.0
    one = jnp.ones_like(nodes)
    path = [jnp.zeros_like(nodes)]
    second = path[0]
    errors = [jnp.zeros((1, 1), jnp.float32), jnp.zeros((1, 1), jnp.float32)]
    for rounds in range(STEPS + 1):
        lower = upper = one
        if rounds < STEPS:
            lower = one - above * path[-1]
        if rounds > 0:
            upper = one - above * second + 0.5 * above * (path[rounds] - path[rounds - 1])
        change, error = spectral_solve(jnp.concatenate([lower, upper], axis=0), weight, nodes, noise)
        if rounds > 0:
            second = second + change[1:2]
            errors[1] = errors[1] + error[1:2]
        if rounds < STEPS:
            path.append(path[-1] + change[0:1])
            errors[0] = errors[0] + error[0:1]
    results = []
    for values, error in ((path[-1], errors[0]), (second, errors[0] + errors[1])):
        part = total(table[:16] * values) * (2.0 / NODES)
        row = lax.broadcasted_iota(jnp.int32, (16, 1), 0)
        part = jnp.where(row == 0, 0.5 * part, part)
        part = jnp.where(row < TOP, part, 0.0)
        cross = jnp.sum(part * dots[FIELD_AT + 1 : FIELD_AT + 17], axis=0, keepdims=True)
        square = dots[FIELD_AT : FIELD_AT + 1] + 2.0 * cross + total(weight * values * values)
        fine = (error * error <= ERROR_BOUND * ERROR_BOUND * square) & (error >= 0.0)
        results.append((part, fine))
    return results


PAD = 8
OWN = PAD + ROWS


def by_level(lower, upper):
    return jnp.where(lax.axis_index("level") == 0, lower, upper)


def pack_first_kernel(u, f, d, rows_out, planes_out, rows, planes, arrived):
    nx, ny, _ = u.shape
    level = lax.axis_index("level")
    start = pl.multiple_of((ny - ROWS) * (1 - level), ROWS)
    copies = []
    for n, (ref, width) in enumerate(((u, WIDE), (f, HALF), (d, HALF))):
        begin = (nx - width) * (1 - level)
        copies += [
            pltpu.make_async_copy(ref.at[:, pl.ds(start, ROWS), :], rows.at[n], arrived.at[2 * n]),
            pltpu.make_async_copy(ref.at[pl.ds(begin, width)], planes.at[n, :width], arrived.at[2 * n + 1]),
        ]
    for copy in copies:
        copy.start()
    at = 0
    for n, width in enumerate((WIDE, HALF, HALF)):
        copies[2 * n].wait()
        copies[2 * n + 1].wait()
        for c in range(2):
            lanes = slice(c * 128, (c + 1) * 128)
            rows_out[n * nx : (n + 1) * nx, c] = rows[n, :, :, lanes]
            planes_out[at : at + width, c] = planes[n, :width, :, lanes]
        at += width


def pack_corners_kernel(mine, theirs, out):
    width, _, ny, _ = mine.shape
    for n, planes in enumerate((by_level(mine[...], theirs[...]), by_level(theirs[...], mine[...]))):
        out[n * width : (n + 1) * width] = by_level(planes[:, :, ny - ROWS :], planes[:, :, :ROWS])


def row_span(level, ny):
    return pl.ds(pl.multiple_of(PAD + level * (ROWS + ny), 8), ROWS)


def beside(ref, i, start, count):
    here = [ref[i, c, start : start + count] for c in range(2)]
    lane = lax.broadcasted_iota(jnp.int32, (count, 128), 1)
    left = [pltpu.roll(v, 1, 1) for v in here]
    right = [pltpu.roll(v, 127, 1) for v in here]
    along = (
        jnp.where(lane == 0, 0.0, left[0]) + jnp.where(lane == 127, right[1], right[0]),
        jnp.where(lane == 0, left[0], left[1]) + jnp.where(lane == 127, 0.0, right[1]),
    )
    around = []
    for c in range(2):
        planes = ref[i + 1, c, start : start + count] + ref[i - 1, c, start : start + count]
        rows = ref[i, c, start - 1 : start - 1 + count] + ref[i, c, start + 1 : start + 1 + count]
        around.append((planes + rows) + along[c])
    return here, around


def row_mask(ny):
    row = lax.broadcasted_iota(jnp.int32, (ny + 2 * ROWS, 128), 0)
    here, count = lax.axis_index("yz"), lax.axis_size("yz")
    low = jnp.where(here == 0, ROWS, 0)
    high = jnp.where(here == count - 1, ROWS + ny, 2 * ROWS + ny)
    return jnp.where((row >= low) & (row < high), 1.0, 0.0)


def over_inner(nx, skip, body):
    def inner(i, _):
        body(i, None)
        return 0

    lax.fori_loop(WIDE + skip, WIDE + nx - skip, inner, 0, unroll=4 if (nx - 2 * skip) % 4 == 0 else 2)


def over_wedges(nx, halo, skip, body):
    here, count = lax.axis_index("gx"), lax.axis_size("gx")
    below = jnp.where(here == 0, 0.0, 1.0)
    above = jnp.where(here == count - 1, 0.0, 1.0)
    for j in range(-halo, skip):
        body(WIDE + j, below if j < 0 else None)
        body(WIDE + nx - 1 - j, above if j < 0 else None)


def put(row, entries):
    lane = lax.broadcasted_iota(jnp.int32, row.shape, 1)
    most = functools.reduce(jnp.maximum, [jnp.abs(half) for _, halves_ in entries for half in halves_])
    unit = (8.0 * most.size) * jnp.max(most, keepdims=True)
    for at, pair in entries:
        rounded = [(half + unit) - unit for half in pair]
        high = jnp.sum(rounded[0] + rounded[1], keepdims=True)
        low = jnp.sum((pair[0] - rounded[0]) + (pair[1] - rounded[1]), keepdims=True)
        row = jnp.where(lane == at, high, jnp.where(lane == at + LOW_AT, low, row))
    return row


def clear_margins(refs):
    count, _, tall, _ = refs[0].shape
    side = jnp.zeros((2, PAD, 128), jnp.float32)

    def margins(i, _):
        for ref in refs:
            ref[i, :, :PAD] = side
            ref[i, :, tall - PAD :] = side
        return 0

    lax.fori_loop(0, count, margins, 0, unroll=2)


def recur(src, dst, scale, pull, first_step, rows):
    start, count = rows
    offset = start - PAD
    factor = pull[offset : offset + count]

    def body(i, mask):
        here, around = beside(src, i, start, count)
        weight = factor if mask is None else factor * mask
        made = []
        for c in range(2):
            at = (i, c, slice(start, start + count))
            twice = scale[at] * here[c] - weight * around[c]
            new = 0.5 * twice if first_step else twice - dst[at]
            dst[at] = new
            made.append(new)
        return made

    return body


def first_start(wide_u, va, scale, ny):
    keep = row_mask(ny)
    rows = (PAD, ny + 2 * ROWS)

    def body(i, mask):
        here, around = beside(wide_u, i, *rows)
        inside = keep if mask is None else keep * mask
        for c in range(2):
            at = (i, c, slice(PAD, PAD + rows[1]))
            damp = scale[at]
            va[at] = inside * (va[at] - (damp * here[c] + DIFFUSION * (6.0 * here[c] - around[c])))
            scale[at] = inside * ((2.0 / RADIUS) * (damp + (1.0 + 6.0 * DIFFUSION - CENTRE)))

    return body


def first_steps(ny, wide_u, va, vb, scale, basis, over, steps=range(HALF + 1)):
    pull = row_mask(ny) * (2.0 / RADIUS * DIFFUSION)
    rows = (PAD, ny + 2 * ROWS)
    begin = first_start(wide_u, va, scale, ny)

    def start(i, mask):
        begin(i, mask)
        if mask is None:
            basis[0, i - WIDE] = va[i, :, OWN : OWN + ny]

    if 0 in steps:
        over(HALF, 1, start)
    for k in range(HALF):
        if k + 1 not in steps:
            continue
        src, dst = (va, vb) if k % 2 == 0 else (vb, va)
        last = k == HALF - 1
        step = recur(src, dst, scale, pull, k == 0, (OWN, ny) if last else rows)

        def body(i, mask, step=step, k=k, last=last):
            made = step(i, mask)
            if mask is None:
                for c in range(2):
                    basis[k + 1, i - WIDE, c] = made[c] if last else made[c][ROWS : ROWS + ny]

        over(HALF - 1 - k, k + 2, body)


def first_inner_kernel(u, f, d, mine, theirs, wide_u, va, vb, scale, basis):
    nx, ny, _ = u.shape
    level = lax.axis_index("level")
    clear_margins((wide_u, va, vb))
    for n, (ref, dst) in enumerate(((u, wide_u), (f, va), (d, scale))):
        for halo, place in ((mine, level), (theirs, 1 - level)):
            outer = row_span(place, ny)
            dst[WIDE : WIDE + nx, :, outer] = halo[n * nx : (n + 1) * nx]
        for c in range(2):
            dst[WIDE : WIDE + nx, c, OWN : OWN + ny] = ref[:, :, c * 128 : (c + 1) * 128]
    over = lambda halo, skip, body: over_inner(nx, skip, body)
    first_steps(ny, wide_u, va, vb, scale, basis, over, range(FIRST_CUT))


def first_rest_kernel(*refs):
    wide_u, va, vb, scale, basis = refs[5:]
    _, nx, _, ny, _ = basis.shape
    over = lambda halo, skip, body: over_inner(nx, skip, body)
    first_steps(ny, wide_u, va, vb, scale, basis, over, range(FIRST_CUT, HALF + 1))


def first_outer_kernel(*refs):
    mine, theirs = refs[:2], refs[2:4]
    wide_u, va, vb, scale, basis, edge_rows, edge_planes = refs[9:]
    _, nx, _, ny, _ = basis.shape
    level = lax.axis_index("level")
    at = 0
    corner = WIDE + 2 * HALF
    for width, dst in ((WIDE, wide_u), (HALF, va), (HALF, scale)):
        for (planes, corners), place in ((mine, level), (theirs, 1 - level)):
            outer = row_span(place, ny)
            begin = WIDE - width + place * (nx + width)
            dst[pl.ds(begin, width), :, OWN : OWN + ny] = planes[at : at + width]
            dst[WIDE - width : WIDE, :, outer] = corners[at : at + width]
            dst[WIDE + nx : WIDE + nx + width, :, outer] = corners[corner + at : corner + at + width]
        at += width
    over = lambda halo, skip, body: over_wedges(nx, halo, skip, body)
    first_steps(ny, wide_u, va, vb, scale, basis, over)
    edge_rows[...] = by_level(basis[HALF, :, :, ny - ROWS :, :], basis[HALF, :, :, :ROWS, :])
    edge_planes[...] = by_level(basis[HALF, nx - HALF :], basis[HALF, :HALF])


def first_dots_kernel(u, basis, dots):
    count, nx, _, ny, _ = basis.shape
    row = jnp.zeros((8, 128), jnp.float32)
    entries = []
    for k in range(count):

        def body(i, sums, k=k):
            terms = [[] for _ in sums]
            for c in range(2):
                own = u[i, :, c * 128 : (c + 1) * 128]
                new = basis[k, i, c]
                parts = [own * new, new * new]
                if k == 0:
                    parts.append(own * own)
                else:
                    parts.append(basis[k - 1, i, c] * new)
                if k > 1:
                    parts.append(basis[k - 2, i, c] * new)
                for t, p in zip(terms, parts):
                    t.append(p)
            return tuple((s[0] + t[0], s[1] + t[1]) for s, t in zip(sums, terms))

        zero = jnp.zeros((ny, 128), jnp.float32)
        sums = lax.fori_loop(0, nx, body, ((zero, zero),) * (4 if k > 1 else 3), unroll=4)
        where = (FIELD_AT + 1 + k, 2 * k, FIELD_AT if k == 0 else 2 * k - 1, CHECK_AT + k - 1)
        entries += zip(where, sums)
    dots[...] = put(row, entries)


def second_step(j, ny, va, vb, scale, pull, u, first, basis):
    src, dst = (va, vb) if j % 2 == 0 else (vb, va)
    last = j == HALF - 1
    step = recur(src, dst, scale, pull, j == 0, (OWN, ny) if last else (PAD, ny + 2 * ROWS))
    k = HALF + j
    get = lambda n, i, c: first[n, i, c] if n <= HALF else basis[n - HALF - 1, i, c]

    def body(i, mask, sums):
        made = step(i, mask)
        if mask is not None:
            return sums
        at = i - WIDE
        result = [list(s) for s in sums]
        for c in range(2):
            mid = made[c] if last else made[c][ROWS : ROWS + ny]
            new = 2.0 * mid - first[HALF - 1 - j, at, c]
            parts = [get(k, at, c) * new, get(k - 1, at, c) * new]
            if not last:
                basis[j, at, c] = new
                parts += [new * new, u[at, :, c * 128 : (c + 1) * 128] * new]
            for r, p in zip(result, parts):
                r[c] = r[c] + p
        return tuple(tuple(r) for r in result)

    return body, 2 if last else 4


def second_inner_kernel(mine, theirs, scale, u, first, basis, va, vb, sums):
    _, nx, _, ny, _ = basis.shape
    level = lax.axis_index("level")
    clear_margins((va, vb))
    for halo, place in ((mine, level), (theirs, 1 - level)):
        outer = row_span(place, ny)
        va[WIDE : WIDE + nx, :, outer] = halo[...]
    va[WIDE : WIDE + nx, :, OWN : OWN + ny] = first[HALF]
    second_inner_steps(range(SECOND_CUT), scale, u, first, basis, va, vb, sums)


def second_rest_kernel(scale, u, first, *refs):
    second_inner_steps(range(SECOND_CUT, HALF), scale, u, first, *refs[4:])


def second_inner_steps(steps, scale, u, first, basis, va, vb, sums):
    _, nx, _, ny, _ = basis.shape
    pull = row_mask(ny) * (2.0 / RADIUS * DIFFUSION)
    for j in steps:
        body, count = second_step(j, ny, va, vb, scale, pull, u, first, basis)
        zero = jnp.zeros((ny, 128), jnp.float32)
        low, high = WIDE + j + 1, WIDE + nx - j - 1
        run = lambda i, made, body=body: body(i, None, made)
        unroll = 4 if (high - low) % 4 == 0 else 2
        made = lax.fori_loop(low, high, run, ((zero, zero),) * count, unroll=unroll)
        for n in range(count):
            for c in range(2):
                sums[j, n, c] = made[n][c]


def second_outer_kernel(*refs):
    mine, theirs = refs[:2], refs[2:4]
    scale, u, first, before, sums = refs[4:9]
    basis, va, vb, dots = refs[12:]
    _, nx, _, ny, _ = basis.shape
    level = lax.axis_index("level")
    for (planes, corners), place in ((mine, level), (theirs, 1 - level)):
        outer = row_span(place, ny)
        va[pl.ds(WIDE - HALF + place * (nx + HALF), HALF), :, OWN : OWN + ny] = planes[...]
        va[WIDE - HALF : WIDE, :, outer] = corners[:HALF]
        va[WIDE + nx : WIDE + nx + HALF, :, outer] = corners[HALF:]
    pull = row_mask(ny) * (2.0 / RADIUS * DIFFUSION)
    entries = []
    for j in range(HALF):
        body, count = second_step(j, ny, va, vb, scale, pull, u, first, basis)
        made = [tuple(tuple(sums[j, n, c] for c in range(2)) for n in range(count))]

        def run(i, mask, body=body, made=made):
            made[0] = body(i, mask, made[0])

        over_wedges(nx, HALF - 1 - j, j + 1, run)
        k = HALF + j
        where = (2 * k + 1, CHECK_AT + k, 2 * k + 2, FIELD_AT + 2 + k)
        entries += zip(where, made[0])
    row = put(before[...], entries)
    dots[...] = jnp.broadcast_to(row[0:1], dots.shape)


def finish_kernel(gathered, tables, nodes, second, far_u, far_first, out, flag, u, first, arrived):
    nx, ny, _ = out.shape
    copies = [
        pltpu.make_async_copy(far_u, u, arrived.at[0]),
        pltpu.make_async_copy(far_first, first, arrived.at[1]),
    ]
    for copy in copies:
        copy.start()
    turned = gathered[...].T
    high, low = split_sum(turned[:LOW_AT], 1)
    high, low = two_sum(high, low + total(turned[LOW_AT:]))
    (lower, fine_low), (upper, fine_up) = coefficients(high, low, tables[...], nodes[...])
    level = lax.axis_index("level")
    part = jnp.where(level == 0, lower, upper)
    flag[0, 0] = jnp.where(jnp.min(jnp.where(fine_low & fine_up, 1.0, 0.0)) > 0.5, 1, 0)
    for copy in copies:
        copy.wait()
    factors = [jnp.broadcast_to(part[k : k + 1], (8, 128)) for k in range(TOP)]

    def body(i, _):
        for r in range(0, ny, 8):
            for c in range(2):
                value = u[i, r : r + 8, c * 128 : (c + 1) * 128]
                for k in range(TOP):
                    ref, n = (first, k) if k <= HALF else (second, k - HALF - 1)
                    value = value + factors[k] * ref[n, i, c, r : r + 8]
                out[i, r : r + 8, c * 128 : (c + 1) * 128] = value
        return 0

    lax.fori_loop(0, nx, body, 0, unroll=2)


def call(kernel, outs, args, limit=16 << 20, flags=(), alias=None, far=0, scratch=()):
    whole = pl.BlockSpec(memory_space=pltpu.VMEM)
    shapes = [jax.ShapeDtypeStruct(s, jnp.float32) for s in outs]
    near = len(args) - far
    args = tuple(args[:near]) + tuple(pltpu.with_memory_space_constraint(a, pltpu.HBM) for a in args[near:])
    return pl.pallas_call(
        kernel,
        out_shape=shapes + [jax.ShapeDtypeStruct(s, jnp.int32) for s in flags],
        in_specs=[whole] * near + [pl.BlockSpec(memory_space=pltpu.HBM)] * far,
        scratch_shapes=scratch,
        out_specs=[whole] * len(outs) + [pl.BlockSpec(memory_space=pltpu.SMEM)] * len(flags),
        input_output_aliases=alias or {},
        compiler_params=pltpu.CompilerParams(vmem_limit_bytes=limit),
    )(*args)


def both_ways(up, down, axis):
    size = lax.axis_size(axis)
    route = [(i, i + 1) for i in range(size - 1)]
    high = lax.ppermute(up, axis, route)
    low = lax.ppermute(down, axis, [(b, a) for a, b in route])
    return high, low


def stencil(field, damping):
    low, high = both_ways(field[-1:], field[:1], "gx")
    left, right = both_ways(field[:, -1:], field[:, :1], "yz")
    tall = jnp.concatenate([low, field, high], axis=0)
    long = jnp.concatenate([left, field, right], axis=1)
    zero = jnp.zeros_like(field[:, :, :1])
    near = tall[2:] + tall[:-2] + long[:, 2:] + long[:, :-2]
    near = near + jnp.concatenate([field[:, :, 1:], zero], axis=2) + jnp.concatenate([zero, field[:, :, :-1]], axis=2)
    return damping * field + DIFFUSION * (6.0 * field - near)


def dot(a, b):
    value = jnp.sum(a * b)
    for axis in AXES:
        value = lax.psum(value, axis)
    return value


def solve(target, guess, damping):
    resid = target - (guess + stencil(guess, damping))

    def step(_, state):
        answer, resid, direction, norm_now = state
        image = direction + stencil(direction, damping)
        alpha = norm_now / dot(direction, image)
        answer = answer + alpha * direction
        resid = resid - alpha * image
        norm_next = dot(resid, resid)
        return answer, resid, resid + (norm_next / norm_now) * direction, norm_next

    return lax.fori_loop(0, ITERS, step, (guess, resid, resid, dot(resid, resid)))[0]


def step_by_step(init_field, source, damping):
    def body(_, carry):
        lower, upper = carry
        fresh = solve(lower + source, lower, damping)
        extra = 0.5 * stencil(fresh - lower, damping)
        return fresh, solve(upper + source + extra, upper, damping)

    begin = jnp.minimum(init_field, jnp.finfo(jnp.float32).max)
    lower, upper = lax.fori_loop(0, STEPS, body, (begin, begin))
    return jnp.where(lax.axis_index("level") == 1, upper, lower)


def shifted(block, axis):
    size = lax.axis_size(axis)
    route = [(i, i + 1) for i in range(size - 1)] + [(size + i + 1, size + i) for i in range(size - 1)]
    return lax.ppermute(block, ("level", axis), route)


def swapped(block):
    return lax.ppermute(block, "level", [(0, 1), (1, 0)])


def exchange(rows, planes):
    planes = shifted(planes, "gx")
    halo = shifted(rows, "yz")
    others = swapped(planes)
    width = planes.shape[0]
    (corners,) = call(pack_corners_kernel, [(2 * width, 2, ROWS, 128)], (planes, others))
    corners = shifted(corners, "yz")
    theirs = swapped(halo)
    opposite = swapped(corners)
    return halo, theirs, (planes, corners, others, opposite)


def per_device(u, f, d):
    nx, ny, nz = u.shape
    tall = 2 * ROWS + ny
    deep = WIDE + 2 * HALF
    rows, planes = call(
        pack_first_kernel,
        [(3 * nx, 2, ROWS, 128), (deep, 2, ny, 128)],
        (u, f, d),
        far=3,
        scratch=[
            pltpu.VMEM((3, nx, ROWS, nz), jnp.float32),
            pltpu.VMEM((3, WIDE, ny, nz), jnp.float32),
            pltpu.SemaphoreType.DMA((6,)),
        ],
    )
    halo, theirs, outside = exchange(rows, planes)
    wide = (nx + 2 * WIDE, 2, tall + 2 * PAD, 128)
    block = (nx, 2, ny, 128)
    buffers = call(first_inner_kernel, [wide] * 4 + [(HALF + 1,) + block], (u, f, d, halo, theirs))
    shapes = [b.shape for b in buffers]
    buffers = call(first_rest_kernel, shapes, buffers, alias={n: n for n in range(5)})
    *_, scale, first, rows, planes = call(
        first_outer_kernel,
        [wide] * 4 + [(HALF + 1,) + block, (nx, 2, ROWS, 128), (HALF, 2, ny, 128)],
        outside + tuple(buffers),
        alias={4 + n: n for n in range(5)},
    )
    halo, theirs, outside = exchange(rows, planes)
    (dots,) = call(first_dots_kernel, [(8, 128)], (u, first))
    buffers = call(
        second_inner_kernel,
        [(HALF - 1,) + block, wide, wide, (HALF, 4, 2, ny, 128)],
        (halo, theirs, scale, u, first),
    )
    shapes = [b.shape for b in buffers]
    args = (scale, u, first) + tuple(buffers)
    second, va, vb, sums = call(second_rest_kernel, shapes, args, alias={3 + n: n for n in range(4)})
    parts = lax.axis_size(AXES)
    second, _, _, dots = call(
        second_outer_kernel,
        [(HALF - 1,) + block, wide, wide, (parts, 128)],
        outside + (scale, u, first, dots, sums, second, va, vb),
        alias={9: 0, 10: 1, 11: 2},
    )
    gathered = lax.all_to_all(dots.reshape(parts, 1, 128), AXES, 0, 0).reshape(parts, 128)
    tables, nodes = chebyshev_tables()
    fast, flag = call(
        finish_kernel,
        [(nx, ny, nz)],
        (gathered, jnp.asarray(tables), jnp.asarray(nodes), second, u, first),
        flags=[(1, 1)],
        far=2,
        scratch=[
            pltpu.VMEM((nx, ny, nz), jnp.float32),
            pltpu.VMEM((HALF + 1,) + block, jnp.float32),
            pltpu.SemaphoreType.DMA((2,)),
        ],
    )
    state = lax.cond(flag.reshape(()), lambda: fast, lambda: step_by_step(u, f, d))
    return state[None]


def solution(mesh):
    placed = P("gx", "yz", None)
    return jax.shard_map(
        per_device,
        mesh=mesh,
        in_specs=(placed, placed, placed),
        out_specs=P("level", "gx", "yz", None),
        check_vma=False,
    )
```

```python
import functools

import jax
import jax.numpy as jnp
import numpy as np
from jax import lax
from jax.experimental import pallas as pl
from jax.experimental.pallas import tpu as pltpu
from jax.sharding import PartitionSpec as P

STEPS = 3
ITERS = 3
DIFFUSION = 1.0
CENTRE, RADIUS = 8.0, 7.0
HALF = 6
TOP = 2 * HALF
MOMENTS = 2 * TOP
NODES = 128
WIDE = HALF + 1
ROWS = 8
FIRST_CUT, SECOND_CUT = 2, 2
NOISE_GAIN = 4.0
ERROR_BOUND = 4e-5

AXES = ("gx", "yz")
CHECK_AT, FIELD_AT = 32, 47
LOW_AT = 64


def chebyshev_tables():
    angle = np.pi * (np.arange(NODES) + 0.5) / NODES
    exact = np.cos(np.arange(32)[:, None] * angle[None])
    first = np.round(exact * 2048.0) / 2048.0
    second = np.round((exact - first) * 2.0**23) / 2.0**23
    parts = np.concatenate([first, second, exact - first - second, exact])
    return parts.astype(np.float32), (CENTRE + RADIUS * exact[1:2]).astype(np.float32)


def total(values):
    return jnp.sum(values, axis=1, keepdims=True)


def two_sum(a, b):
    s = a + b
    t = s - a
    return s, (a - (s - t)) + (b - t)


def plus(a, b):
    s, e = two_sum(a[0], b[0])
    return two_sum(s, e + (a[1] + b[1]))


def times(scale, a):
    return scale * a[0], scale * a[1]


def halves(values):
    wide = 4097.0 * values
    high = wide - (wide - values)
    return high, values - high


def split_sum(values, axis):
    most = jnp.max(jnp.abs(values), axis=axis, keepdims=True)
    unit = (4.0 * values.shape[axis]) * most
    high = (values + unit) - unit
    return jnp.sum(high, axis=axis, keepdims=True), jnp.sum(values - high, axis=axis, keepdims=True)


def spectral_solve(resid, weight, nodes, noise):
    direction = resid
    answer = jnp.zeros_like(resid)
    norm_now = total(weight * resid * resid)
    noise_now = noise * total(resid * resid)
    error = jnp.zeros_like(norm_now)
    for step in range(ITERS):
        image = nodes * direction
        product = total(weight * direction * image)
        length = total(weight * direction * direction)
        noise_product = noise * total(direction * image)
        alpha = norm_now / product
        error = error + alpha * (noise_now / norm_now + noise_product / product) * jnp.sqrt(length)
        answer = answer + alpha * direction
        resid = resid - alpha * image
        if step + 1 < ITERS:
            norm_next = total(weight * resid * resid)
            noise_now = noise * total(resid * resid)
            direction = resid + (norm_next / norm_now) * direction
            norm_now = norm_next
    return answer, error


def coefficients(high, low, tables, nodes):
    table = tables[96:128]
    place = lax.broadcasted_iota(jnp.int32, (32, 1), 0)
    raw = high[:32], low[:32]
    base = tuple(jnp.where(place % 2 == 0, r[0:1], r[1:2]) for r in raw)
    shifted = plus(times(2.0, raw), times(-1.0, base))
    used = place < MOMENTS
    moment = tuple(jnp.where(used, jnp.where(place < 2, r, m), 0.0) for r, m in zip(raw, shifted))
    factor = jnp.where(place == 0, 1.0 / NODES, 2.0 / NODES)
    big, small = halves(factor * moment[0])
    small = small + factor * moment[1]
    parts = big * tables[:32]
    rest = big * tables[32:64] + small * tables[:32] + (big * tables[64:96] + small * tables[32:64])
    pieces = (parts, rest)
    count = 32
    while count > 1:
        count //= 2
        pieces = plus(tuple(p[:count] for p in pieces), tuple(p[count : 2 * count] for p in pieces))
    weight = pieces[0] + pieces[1]
    worst = jnp.zeros((1, 1), jnp.float32)
    at = lambda pair, k: (pair[0][k : k + 1], pair[1][k : k + 1])
    for k in range(1, TOP):
        gap = plus(times(2.0, at((high, low), CHECK_AT + k)), times(-1.0, at(moment, 2)))
        gap = plus(gap, times(-1.0, at(moment, 2 * k)))
        worst = jnp.maximum(worst, jnp.abs(gap[0] + gap[1]))
    noise = (worst + 1e-10 * high[0:1]) * (NOISE_GAIN / NODES)
    dots = high
    above = nodes - 1.0
    one = jnp.ones_like(nodes)
    path = [jnp.zeros_like(nodes)]
    second = path[0]
    errors = [jnp.zeros((1, 1), jnp.float32), jnp.zeros((1, 1), jnp.float32)]
    for rounds in range(STEPS + 1):
        lower = upper = one
        if rounds < STEPS:
            lower = one - above * path[-1]
        if rounds > 0:
            upper = one - above * second + 0.5 * above * (path[rounds] - path[rounds - 1])
        change, error = spectral_solve(jnp.concatenate([lower, upper], axis=0), weight, nodes, noise)
        if rounds > 0:
            second = second + change[1:2]
            errors[1] = errors[1] + error[1:2]
        if rounds < STEPS:
            path.append(path[-1] + change[0:1])
            errors[0] = errors[0] + error[0:1]
    results = []
    for values, error in ((path[-1], errors[0]), (second, errors[0] + errors[1])):
        part = total(table[:16] * values) * (2.0 / NODES)
        row = lax.broadcasted_iota(jnp.int32, (16, 1), 0)
        part = jnp.where(row == 0, 0.5 * part, part)
        part = jnp.where(row < TOP, part, 0.0)
        cross = jnp.sum(part * dots[FIELD_AT + 1 : FIELD_AT + 17], axis=0, keepdims=True)
        square = dots[FIELD_AT : FIELD_AT + 1] + 2.0 * cross + total(weight * values * values)
        fine = (error * error <= ERROR_BOUND * ERROR_BOUND * square) & (error >= 0.0)
        results.append((part, fine))
    return results


PAD = 8
OWN = PAD + ROWS


def by_level(lower, upper):
    return jnp.where(lax.axis_index("level") == 0, lower, upper)


def pack_first_kernel(u, f, d, rows_out, planes_out, rows, planes, arrived):
    nx, ny, _ = u.shape
    level = lax.axis_index("level")
    start = pl.multiple_of((ny - ROWS) * (1 - level), ROWS)
    copies = []
    for n, (ref, width) in enumerate(((u, WIDE), (f, HALF), (d, HALF))):
        begin = (nx - width) * (1 - level)
        copies += [
            pltpu.make_async_copy(ref.at[:, pl.ds(start, ROWS), :], rows.at[n], arrived.at[2 * n]),
            pltpu.make_async_copy(ref.at[pl.ds(begin, width)], planes.at[n, :width], arrived.at[2 * n + 1]),
        ]
    for copy in copies:
        copy.start()
    at = 0
    for n, width in enumerate((WIDE, HALF, HALF)):
        copies[2 * n].wait()
        copies[2 * n + 1].wait()
        for c in range(2):
            lanes = slice(c * 128, (c + 1) * 128)
            rows_out[n * nx : (n + 1) * nx, c] = rows[n, :, :, lanes]
            planes_out[at : at + width, c] = planes[n, :width, :, lanes]
        at += width


def pack_corners_kernel(mine, theirs, out):
    width, _, ny, _ = mine.shape
    for n, planes in enumerate((by_level(mine[...], theirs[...]), by_level(theirs[...], mine[...]))):
        out[n * width : (n + 1) * width] = by_level(planes[:, :, ny - ROWS :], planes[:, :, :ROWS])


def row_span(level, ny):
    return pl.ds(pl.multiple_of(PAD + level * (ROWS + ny), 8), ROWS)


def beside(ref, i, start, count):
    here = [ref[i, c, start : start + count] for c in range(2)]
    lane = lax.broadcasted_iota(jnp.int32, (count, 128), 1)
    left = [pltpu.roll(v, 1, 1) for v in here]
    right = [pltpu.roll(v, 127, 1) for v in here]
    along = (
        jnp.where(lane == 0, 0.0, left[0]) + jnp.where(lane == 127, right[1], right[0]),
        jnp.where(lane == 0, left[0], left[1]) + jnp.where(lane == 127, 0.0, right[1]),
    )
    around = []
    for c in range(2):
        planes = ref[i + 1, c, start : start + count] + ref[i - 1, c, start : start + count]
        rows = ref[i, c, start - 1 : start - 1 + count] + ref[i, c, start + 1 : start + 1 + count]
        around.append((planes + rows) + along[c])
    return here, around


def row_mask(ny):
    row = lax.broadcasted_iota(jnp.int32, (ny + 2 * ROWS, 128), 0)
    here, count = lax.axis_index("yz"), lax.axis_size("yz")
    low = jnp.where(here == 0, ROWS, 0)
    high = jnp.where(here == count - 1, ROWS + ny, 2 * ROWS + ny)
    return jnp.where((row >= low) & (row < high), 1.0, 0.0)


def over_inner(nx, skip, body):
    def inner(i, _):
        body(i, None)
        return 0

    lax.fori_loop(WIDE + skip, WIDE + nx - skip, inner, 0, unroll=4 if (nx - 2 * skip) % 4 == 0 else 2)


def over_wedges(nx, halo, skip, body):
    here, count = lax.axis_index("gx"), lax.axis_size("gx")
    below = jnp.where(here == 0, 0.0, 1.0)
    above = jnp.where(here == count - 1, 0.0, 1.0)
    for j in range(-halo, skip):
        body(WIDE + j, below if j < 0 else None)
        body(WIDE + nx - 1 - j, above if j < 0 else None)


def put(row, entries):
    lane = lax.broadcasted_iota(jnp.int32, row.shape, 1)
    most = functools.reduce(jnp.maximum, [jnp.abs(half) for _, halves_ in entries for half in halves_])
    unit = (8.0 * most.size) * jnp.max(most, keepdims=True)
    for at, pair in entries:
        rounded = [(half + unit) - unit for half in pair]
        high = jnp.sum(rounded[0] + rounded[1], keepdims=True)
        low = jnp.sum((pair[0] - rounded[0]) + (pair[1] - rounded[1]), keepdims=True)
        row = jnp.where(lane == at, high, jnp.where(lane == at + LOW_AT, low, row))
    return row


def clear_margins(refs):
    count, _, tall, _ = refs[0].shape
    side = jnp.zeros((2, PAD, 128), jnp.float32)

    def margins(i, _):
        for ref in refs:
            ref[i, :, :PAD] = side
            ref[i, :, tall - PAD :] = side
        return 0

    lax.fori_loop(0, count, margins, 0, unroll=2)


def recur(src, dst, scale, pull, first_step, rows):
    start, count = rows
    offset = start - PAD
    factor = pull[offset : offset + count]

    def body(i, mask):
        here, around = beside(src, i, start, count)
        weight = factor if mask is None else factor * mask
        made = []
        for c in range(2):
            at = (i, c, slice(start, start + count))
            twice = scale[at] * here[c] - weight * around[c]
            new = 0.5 * twice if first_step else twice - dst[at]
            dst[at] = new
            made.append(new)
        return made

    return body


def first_start(wide_u, va, scale, ny):
    keep = row_mask(ny)
    rows = (PAD, ny + 2 * ROWS)

    def body(i, mask):
        here, around = beside(wide_u, i, *rows)
        inside = keep if mask is None else keep * mask
        for c in range(2):
            at = (i, c, slice(PAD, PAD + rows[1]))
            damp = scale[at]
            va[at] = inside * (va[at] - (damp * here[c] + DIFFUSION * (6.0 * here[c] - around[c])))
            scale[at] = inside * ((2.0 / RADIUS) * (damp + (1.0 + 6.0 * DIFFUSION - CENTRE)))

    return body


def first_steps(ny, wide_u, va, vb, scale, basis, over, steps=range(HALF + 1)):
    pull = row_mask(ny) * (2.0 / RADIUS * DIFFUSION)
    rows = (PAD, ny + 2 * ROWS)
    begin = first_start(wide_u, va, scale, ny)

    def start(i, mask):
        begin(i, mask)
        if mask is None:
            basis[0, i - WIDE] = va[i, :, OWN : OWN + ny]

    if 0 in steps:
        over(HALF, 1, start)
    for k in range(HALF):
        if k + 1 not in steps:
            continue
        src, dst = (va, vb) if k % 2 == 0 else (vb, va)
        last = k == HALF - 1
        step = recur(src, dst, scale, pull, k == 0, (OWN, ny) if last else rows)

        def body(i, mask, step=step, k=k, last=last):
            made = step(i, mask)
            if mask is None:
                for c in range(2):
                    basis[k + 1, i - WIDE, c] = made[c] if last else made[c][ROWS : ROWS + ny]

        over(HALF - 1 - k, k + 2, body)


def first_own_kernel(u, f, d, wide_u, va, vb, scale):
    nx, ny, _ = u.shape
    clear_margins((wide_u, va, vb))
    for ref, dst in ((u, wide_u), (f, va), (d, scale)):
        for c in range(2):
            dst[WIDE : WIDE + nx, c, OWN : OWN + ny] = ref[:, :, c * 128 : (c + 1) * 128]


def first_inner_kernel(mine, theirs, *refs):
    wide_u, va, vb, scale, basis = refs[4:]
    _, nx, _, ny, _ = basis.shape
    level = lax.axis_index("level")
    for n, dst in enumerate((wide_u, va, scale)):
        for halo, place in ((mine, level), (theirs, 1 - level)):
            dst[WIDE : WIDE + nx, :, row_span(place, ny)] = halo[n * nx : (n + 1) * nx]
    over = lambda halo, skip, body: over_inner(nx, skip, body)
    first_steps(ny, wide_u, va, vb, scale, basis, over, range(FIRST_CUT))


def first_rest_kernel(*refs):
    wide_u, va, vb, scale, basis = refs[5:]
    _, nx, _, ny, _ = basis.shape
    over = lambda halo, skip, body: over_inner(nx, skip, body)
    first_steps(ny, wide_u, va, vb, scale, basis, over, range(FIRST_CUT, HALF + 1))


def first_outer_kernel(*refs):
    mine, theirs = refs[:2], refs[2:4]
    wide_u, va, vb, scale, basis, edge_rows, edge_planes = refs[9:]
    _, nx, _, ny, _ = basis.shape
    level = lax.axis_index("level")
    at = 0
    corner = WIDE + 2 * HALF
    for width, dst in ((WIDE, wide_u), (HALF, va), (HALF, scale)):
        for (planes, corners), place in ((mine, level), (theirs, 1 - level)):
            outer = row_span(place, ny)
            begin = WIDE - width + place * (nx + width)
            dst[pl.ds(begin, width), :, OWN : OWN + ny] = planes[at : at + width]
            dst[WIDE - width : WIDE, :, outer] = corners[at : at + width]
            dst[WIDE + nx : WIDE + nx + width, :, outer] = corners[corner + at : corner + at + width]
        at += width
    over = lambda halo, skip, body: over_wedges(nx, halo, skip, body)
    first_steps(ny, wide_u, va, vb, scale, basis, over)
    edge_rows[...] = by_level(basis[HALF, :, :, ny - ROWS :, :], basis[HALF, :, :, :ROWS, :])
    edge_planes[...] = by_level(basis[HALF, nx - HALF :], basis[HALF, :HALF])


def first_dots_kernel(u, basis, dots):
    count, nx, _, ny, _ = basis.shape
    row = jnp.zeros((8, 128), jnp.float32)
    entries = []
    for k in range(count):

        def body(i, sums, k=k):
            terms = [[] for _ in sums]
            for c in range(2):
                own = u[i, :, c * 128 : (c + 1) * 128]
                new = basis[k, i, c]
                parts = [own * new, new * new]
                if k == 0:
                    parts.append(own * own)
                else:
                    parts.append(basis[k - 1, i, c] * new)
                if k > 1:
                    parts.append(basis[k - 2, i, c] * new)
                for t, p in zip(terms, parts):
                    t.append(p)
            return tuple((s[0] + t[0], s[1] + t[1]) for s, t in zip(sums, terms))

        zero = jnp.zeros((ny, 128), jnp.float32)
        sums = lax.fori_loop(0, nx, body, ((zero, zero),) * (4 if k > 1 else 3), unroll=4)
        where = (FIELD_AT + 1 + k, 2 * k, FIELD_AT if k == 0 else 2 * k - 1, CHECK_AT + k - 1)
        entries += zip(where, sums)
    dots[...] = put(row, entries)


def second_step(j, ny, va, vb, scale, pull, u, first, basis):
    src, dst = (va, vb) if j % 2 == 0 else (vb, va)
    last = j == HALF - 1
    step = recur(src, dst, scale, pull, j == 0, (OWN, ny) if last else (PAD, ny + 2 * ROWS))
    k = HALF + j
    get = lambda n, i, c: first[n, i, c] if n <= HALF else basis[n - HALF - 1, i, c]

    def body(i, mask, sums):
        made = step(i, mask)
        if mask is not None:
            return sums
        at = i - WIDE
        result = [list(s) for s in sums]
        for c in range(2):
            mid = made[c] if last else made[c][ROWS : ROWS + ny]
            new = 2.0 * mid - first[HALF - 1 - j, at, c]
            parts = [get(k, at, c) * new, get(k - 1, at, c) * new]
            if not last:
                basis[j, at, c] = new
                parts += [new * new, u[at, :, c * 128 : (c + 1) * 128] * new]
            for r, p in zip(result, parts):
                r[c] = r[c] + p
        return tuple(tuple(r) for r in result)

    return body, 2 if last else 4


def second_own_kernel(first, dots, va, vb):
    _, nx, _, ny, _ = first.shape
    clear_margins((va, vb))
    va[WIDE : WIDE + nx, :, OWN : OWN + ny] = first[HALF]


def second_inner_kernel(mine, theirs, scale, u, first, *refs):
    basis, va, vb, sums = refs[2:]
    _, nx, _, ny, _ = basis.shape
    level = lax.axis_index("level")
    for halo, place in ((mine, level), (theirs, 1 - level)):
        outer = row_span(place, ny)
        va[WIDE : WIDE + nx, :, outer] = halo[...]
    second_inner_steps(range(SECOND_CUT), scale, u, first, basis, va, vb, sums)


def second_rest_kernel(scale, u, first, *refs):
    second_inner_steps(range(SECOND_CUT, HALF), scale, u, first, *refs[4:])


def second_inner_steps(steps, scale, u, first, basis, va, vb, sums):
    _, nx, _, ny, _ = basis.shape
    pull = row_mask(ny) * (2.0 / RADIUS * DIFFUSION)
    for j in steps:
        body, count = second_step(j, ny, va, vb, scale, pull, u, first, basis)
        zero = jnp.zeros((ny, 128), jnp.float32)
        low, high = WIDE + j + 1, WIDE + nx - j - 1
        run = lambda i, made, body=body: body(i, None, made)
        unroll = 4 if (high - low) % 4 == 0 else 2
        made = lax.fori_loop(low, high, run, ((zero, zero),) * count, unroll=unroll)
        for n in range(count):
            for c in range(2):
                sums[j, n, c] = made[n][c]


def second_outer_kernel(*refs):
    mine, theirs = refs[:2], refs[2:4]
    scale, u, first, before, sums = refs[4:9]
    basis, va, vb, dots = refs[12:]
    _, nx, _, ny, _ = basis.shape
    level = lax.axis_index("level")
    for (planes, corners), place in ((mine, level), (theirs, 1 - level)):
        outer = row_span(place, ny)
        va[pl.ds(WIDE - HALF + place * (nx + HALF), HALF), :, OWN : OWN + ny] = planes[...]
        va[WIDE - HALF : WIDE, :, outer] = corners[:HALF]
        va[WIDE + nx : WIDE + nx + HALF, :, outer] = corners[HALF:]
    pull = row_mask(ny) * (2.0 / RADIUS * DIFFUSION)
    entries = []
    for j in range(HALF):
        body, count = second_step(j, ny, va, vb, scale, pull, u, first, basis)
        made = [tuple(tuple(sums[j, n, c] for c in range(2)) for n in range(count))]

        def run(i, mask, body=body, made=made):
            made[0] = body(i, mask, made[0])

        over_wedges(nx, HALF - 1 - j, j + 1, run)
        k = HALF + j
        where = (2 * k + 1, CHECK_AT + k, 2 * k + 2, FIELD_AT + 2 + k)
        entries += zip(where, made[0])
    row = put(before[...], entries)
    dots[...] = jnp.broadcast_to(row[0:1], dots.shape)


def finish_kernel(gathered, tables, nodes, second, far_u, far_first, out, flag, u, first, arrived):
    nx, ny, _ = out.shape
    copies = [
        pltpu.make_async_copy(far_u, u, arrived.at[0]),
        pltpu.make_async_copy(far_first, first, arrived.at[1]),
    ]
    for copy in copies:
        copy.start()
    turned = gathered[...].T
    high, low = split_sum(turned[:LOW_AT], 1)
    high, low = two_sum(high, low + total(turned[LOW_AT:]))
    (lower, fine_low), (upper, fine_up) = coefficients(high, low, tables[...], nodes[...])
    level = lax.axis_index("level")
    part = jnp.where(level == 0, lower, upper)
    flag[0, 0] = jnp.where(jnp.min(jnp.where(fine_low & fine_up, 1.0, 0.0)) > 0.5, 1, 0)
    for copy in copies:
        copy.wait()
    factors = [jnp.broadcast_to(part[k : k + 1], (8, 128)) for k in range(TOP)]

    def body(i, _):
        for r in range(0, ny, 8):
            for c in range(2):
                value = u[i, r : r + 8, c * 128 : (c + 1) * 128]
                for k in range(TOP):
                    ref, n = (first, k) if k <= HALF else (second, k - HALF - 1)
                    value = value + factors[k] * ref[n, i, c, r : r + 8]
                out[i, r : r + 8, c * 128 : (c + 1) * 128] = value
        return 0

    lax.fori_loop(0, nx, body, 0, unroll=2)


def call(kernel, outs, args, limit=16 << 20, flags=(), alias=None, far=0, scratch=()):
    whole = pl.BlockSpec(memory_space=pltpu.VMEM)
    shapes = [jax.ShapeDtypeStruct(s, jnp.float32) for s in outs]
    near = len(args) - far
    args = tuple(args[:near]) + tuple(pltpu.with_memory_space_constraint(a, pltpu.HBM) for a in args[near:])
    return pl.pallas_call(
        kernel,
        out_shape=shapes + [jax.ShapeDtypeStruct(s, jnp.int32) for s in flags],
        in_specs=[whole] * near + [pl.BlockSpec(memory_space=pltpu.HBM)] * far,
        scratch_shapes=scratch,
        out_specs=[whole] * len(outs) + [pl.BlockSpec(memory_space=pltpu.SMEM)] * len(flags),
        input_output_aliases=alias or {},
        compiler_params=pltpu.CompilerParams(vmem_limit_bytes=limit),
    )(*args)


def both_ways(up, down, axis):
    size = lax.axis_size(axis)
    route = [(i, i + 1) for i in range(size - 1)]
    high = lax.ppermute(up, axis, route)
    low = lax.ppermute(down, axis, [(b, a) for a, b in route])
    return high, low


def stencil(field, damping):
    low, high = both_ways(field[-1:], field[:1], "gx")
    left, right = both_ways(field[:, -1:], field[:, :1], "yz")
    tall = jnp.concatenate([low, field, high], axis=0)
    long = jnp.concatenate([left, field, right], axis=1)
    zero = jnp.zeros_like(field[:, :, :1])
    near = tall[2:] + tall[:-2] + long[:, 2:] + long[:, :-2]
    near = near + jnp.concatenate([field[:, :, 1:], zero], axis=2) + jnp.concatenate([zero, field[:, :, :-1]], axis=2)
    return damping * field + DIFFUSION * (6.0 * field - near)


def dot(a, b):
    value = jnp.sum(a * b)
    for axis in AXES:
        value = lax.psum(value, axis)
    return value


def solve(target, guess, damping):
    resid = target - (guess + stencil(guess, damping))

    def step(_, state):
        answer, resid, direction, norm_now = state
        image = direction + stencil(direction, damping)
        alpha = norm_now / dot(direction, image)
        answer = answer + alpha * direction
        resid = resid - alpha * image
        norm_next = dot(resid, resid)
        return answer, resid, resid + (norm_next / norm_now) * direction, norm_next

    return lax.fori_loop(0, ITERS, step, (guess, resid, resid, dot(resid, resid)))[0]


def step_by_step(init_field, source, damping):
    def body(_, carry):
        lower, upper = carry
        fresh = solve(lower + source, lower, damping)
        extra = 0.5 * stencil(fresh - lower, damping)
        return fresh, solve(upper + source + extra, upper, damping)

    begin = jnp.minimum(init_field, jnp.finfo(jnp.float32).max)
    lower, upper = lax.fori_loop(0, STEPS, body, (begin, begin))
    return jnp.where(lax.axis_index("level") == 1, upper, lower)


def shifted(block, axis):
    size = lax.axis_size(axis)
    route = [(i, i + 1) for i in range(size - 1)] + [(size + i + 1, size + i) for i in range(size - 1)]
    return lax.ppermute(block, ("level", axis), route)


def swapped(block):
    return lax.ppermute(block, "level", [(0, 1), (1, 0)])


def exchange(rows, planes):
    planes = shifted(planes, "gx")
    halo = shifted(rows, "yz")
    others = swapped(planes)
    width = planes.shape[0]
    (corners,) = call(pack_corners_kernel, [(2 * width, 2, ROWS, 128)], (planes, others))
    corners = shifted(corners, "yz")
    theirs = swapped(halo)
    opposite = swapped(corners)
    return halo, theirs, (planes, corners, others, opposite)


def per_device(u, f, d):
    nx, ny, nz = u.shape
    tall = 2 * ROWS + ny
    deep = WIDE + 2 * HALF
    rows, planes = call(
        pack_first_kernel,
        [(3 * nx, 2, ROWS, 128), (deep, 2, ny, 128)],
        (u, f, d),
        far=3,
        scratch=[
            pltpu.VMEM((3, nx, ROWS, nz), jnp.float32),
            pltpu.VMEM((3, WIDE, ny, nz), jnp.float32),
            pltpu.SemaphoreType.DMA((6,)),
        ],
    )
    halo, theirs, outside = exchange(rows, planes)
    wide = (nx + 2 * WIDE, 2, tall + 2 * PAD, 128)
    block = (nx, 2, ny, 128)
    own = call(first_own_kernel, [wide] * 4, (u, f, d))
    args = (halo, theirs) + tuple(own)
    shapes = [wide] * 4 + [(HALF + 1,) + block]
    buffers = call(first_inner_kernel, shapes, args, alias={2 + n: n for n in range(4)})
    shapes = [b.shape for b in buffers]
    buffers = call(first_rest_kernel, shapes, buffers, alias={n: n for n in range(5)})
    *_, scale, first, rows, planes = call(
        first_outer_kernel,
        [wide] * 4 + [(HALF + 1,) + block, (nx, 2, ROWS, 128), (HALF, 2, ny, 128)],
        outside + tuple(buffers),
        alias={4 + n: n for n in range(5)},
    )
    halo, theirs, outside = exchange(rows, planes)
    (dots,) = call(first_dots_kernel, [(8, 128)], (u, first))
    own = call(second_own_kernel, [wide] * 2, (first, dots))
    buffers = call(
        second_inner_kernel,
        [(HALF - 1,) + block, wide, wide, (HALF, 4, 2, ny, 128)],
        (halo, theirs, scale, u, first) + tuple(own),
        alias={5: 1, 6: 2},
    )
    shapes = [b.shape for b in buffers]
    args = (scale, u, first) + tuple(buffers)
    second, va, vb, sums = call(second_rest_kernel, shapes, args, alias={3 + n: n for n in range(4)})
    parts = lax.axis_size(AXES)
    second, _, _, dots = call(
        second_outer_kernel,
        [(HALF - 1,) + block, wide, wide, (parts, 128)],
        outside + (scale, u, first, dots, sums, second, va, vb),
        alias={9: 0, 10: 1, 11: 2},
    )
    gathered = lax.all_to_all(dots.reshape(parts, 1, 128), AXES, 0, 0).reshape(parts, 128)
    tables, nodes = chebyshev_tables()
    fast, flag = call(
        finish_kernel,
        [(nx, ny, nz)],
        (gathered, jnp.asarray(tables), jnp.asarray(nodes), second, u, first),
        flags=[(1, 1)],
        far=2,
        scratch=[
            pltpu.VMEM((nx, ny, nz), jnp.float32),
            pltpu.VMEM((HALF + 1,) + block, jnp.float32),
            pltpu.SemaphoreType.DMA((2,)),
        ],
    )
    state = lax.cond(flag.reshape(()), lambda: fast, lambda: step_by_step(u, f, d))
    return state[None]


def solution(mesh):
    placed = P("gx", "yz", None)
    return jax.shard_map(
        per_device,
        mesh=mesh,
        in_specs=(placed, placed, placed),
        out_specs=P("level", "gx", "yz", None),
        check_vma=False,
    )
```

```python
import functools

import jax
import jax.numpy as jnp
import numpy as np
from jax import lax
from jax.experimental import pallas as pl
from jax.experimental.pallas import tpu as pltpu
from jax.sharding import PartitionSpec as P

STEPS = 3
ITERS = 3
DIFFUSION = 1.0
CENTRE, RADIUS = 8.0, 7.0
HALF = 6
TOP = 2 * HALF
MOMENTS = 2 * TOP
NODES = 128
WIDE = HALF + 1
ROWS = 8
FIRST_CUT, SECOND_CUT = 2, 2
NOISE_GAIN = 4.0
ERROR_BOUND = 4e-5

AXES = ("gx", "yz")
CHECK_AT, FIELD_AT = 32, 47
LOW_AT = 64


def chebyshev_tables():
    angle = np.pi * (np.arange(NODES) + 0.5) / NODES
    exact = np.cos(np.arange(32)[:, None] * angle[None])
    first = np.round(exact * 2048.0) / 2048.0
    second = np.round((exact - first) * 2.0**23) / 2.0**23
    parts = np.concatenate([first, second, exact - first - second, exact])
    return parts.astype(np.float32), (CENTRE + RADIUS * exact[1:2]).astype(np.float32)


def total(values):
    return jnp.sum(values, axis=1, keepdims=True)


def two_sum(a, b):
    s = a + b
    t = s - a
    return s, (a - (s - t)) + (b - t)


def plus(a, b):
    s, e = two_sum(a[0], b[0])
    return two_sum(s, e + (a[1] + b[1]))


def times(scale, a):
    return scale * a[0], scale * a[1]


def halves(values):
    wide = 4097.0 * values
    high = wide - (wide - values)
    return high, values - high


def split_sum(values, axis):
    most = jnp.max(jnp.abs(values), axis=axis, keepdims=True)
    unit = (4.0 * values.shape[axis]) * most
    high = (values + unit) - unit
    return jnp.sum(high, axis=axis, keepdims=True), jnp.sum(values - high, axis=axis, keepdims=True)


def spectral_solve(resid, weight, nodes, noise):
    direction = resid
    answer = jnp.zeros_like(resid)
    norm_now = total(weight * resid * resid)
    noise_now = noise * total(resid * resid)
    error = jnp.zeros_like(norm_now)
    for step in range(ITERS):
        image = nodes * direction
        product = total(weight * direction * image)
        length = total(weight * direction * direction)
        noise_product = noise * total(direction * image)
        alpha = norm_now / product
        error = error + alpha * (noise_now / norm_now + noise_product / product) * jnp.sqrt(length)
        answer = answer + alpha * direction
        resid = resid - alpha * image
        if step + 1 < ITERS:
            norm_next = total(weight * resid * resid)
            noise_now = noise * total(resid * resid)
            direction = resid + (norm_next / norm_now) * direction
            norm_now = norm_next
    return answer, error


def coefficients(high, low, tables, nodes):
    table = tables[96:128]
    place = lax.broadcasted_iota(jnp.int32, (32, 1), 0)
    raw = high[:32], low[:32]
    base = tuple(jnp.where(place % 2 == 0, r[0:1], r[1:2]) for r in raw)
    shifted = plus(times(2.0, raw), times(-1.0, base))
    used = place < MOMENTS
    moment = tuple(jnp.where(used, jnp.where(place < 2, r, m), 0.0) for r, m in zip(raw, shifted))
    factor = jnp.where(place == 0, 1.0 / NODES, 2.0 / NODES)
    big, small = halves(factor * moment[0])
    small = small + factor * moment[1]
    parts = big * tables[:32]
    rest = big * tables[32:64] + small * tables[:32] + (big * tables[64:96] + small * tables[32:64])
    pieces = (parts, rest)
    count = 32
    while count > 1:
        count //= 2
        pieces = plus(tuple(p[:count] for p in pieces), tuple(p[count : 2 * count] for p in pieces))
    weight = pieces[0] + pieces[1]
    worst = jnp.zeros((1, 1), jnp.float32)
    at = lambda pair, k: (pair[0][k : k + 1], pair[1][k : k + 1])
    for k in range(1, TOP):
        gap = plus(times(2.0, at((high, low), CHECK_AT + k)), times(-1.0, at(moment, 2)))
        gap = plus(gap, times(-1.0, at(moment, 2 * k)))
        worst = jnp.maximum(worst, jnp.abs(gap[0] + gap[1]))
    noise = (worst + 1e-10 * high[0:1]) * (NOISE_GAIN / NODES)
    dots = high
    above = nodes - 1.0
    one = jnp.ones_like(nodes)
    path = [jnp.zeros_like(nodes)]
    second = path[0]
    errors = [jnp.zeros((1, 1), jnp.float32), jnp.zeros((1, 1), jnp.float32)]
    for rounds in range(STEPS + 1):
        lower = upper = one
        if rounds < STEPS:
            lower = one - above * path[-1]
        if rounds > 0:
            upper = one - above * second + 0.5 * above * (path[rounds] - path[rounds - 1])
        change, error = spectral_solve(jnp.concatenate([lower, upper], axis=0), weight, nodes, noise)
        if rounds > 0:
            second = second + change[1:2]
            errors[1] = errors[1] + error[1:2]
        if rounds < STEPS:
            path.append(path[-1] + change[0:1])
            errors[0] = errors[0] + error[0:1]
    results = []
    for values, error in ((path[-1], errors[0]), (second, errors[0] + errors[1])):
        part = total(table[:16] * values) * (2.0 / NODES)
        row = lax.broadcasted_iota(jnp.int32, (16, 1), 0)
        part = jnp.where(row == 0, 0.5 * part, part)
        part = jnp.where(row < TOP, part, 0.0)
        cross = jnp.sum(part * dots[FIELD_AT + 1 : FIELD_AT + 17], axis=0, keepdims=True)
        square = dots[FIELD_AT : FIELD_AT + 1] + 2.0 * cross + total(weight * values * values)
        fine = (error * error <= ERROR_BOUND * ERROR_BOUND * square) & (error >= 0.0)
        results.append((part, fine))
    return results


PAD = 8
OWN = PAD + ROWS


def by_level(lower, upper):
    return jnp.where(lax.axis_index("level") == 0, lower, upper)


def pack_first_kernel(u, f, d, rows_out, planes_out, rows, planes, arrived):
    nx, ny, _ = u.shape
    level = lax.axis_index("level")
    start = pl.multiple_of((ny - ROWS) * (1 - level), ROWS)
    copies = []
    for n, (ref, width) in enumerate(((u, WIDE), (f, HALF), (d, HALF))):
        begin = (nx - width) * (1 - level)
        copies += [
            pltpu.make_async_copy(ref.at[:, pl.ds(start, ROWS), :], rows.at[n], arrived.at[2 * n]),
            pltpu.make_async_copy(ref.at[pl.ds(begin, width)], planes.at[n, :width], arrived.at[2 * n + 1]),
        ]
    for copy in copies:
        copy.start()
    at = 0
    for n, width in enumerate((WIDE, HALF, HALF)):
        copies[2 * n].wait()
        copies[2 * n + 1].wait()
        for c in range(2):
            lanes = slice(c * 128, (c + 1) * 128)
            rows_out[n * nx : (n + 1) * nx, c] = rows[n, :, :, lanes]
            planes_out[at : at + width, c] = planes[n, :width, :, lanes]
        at += width


def pack_corners_kernel(mine, theirs, out):
    width, _, ny, _ = mine.shape
    for n, planes in enumerate((by_level(mine[...], theirs[...]), by_level(theirs[...], mine[...]))):
        out[n * width : (n + 1) * width] = by_level(planes[:, :, ny - ROWS :], planes[:, :, :ROWS])


def row_span(level, ny):
    return pl.ds(pl.multiple_of(PAD + level * (ROWS + ny), 8), ROWS)


def beside(ref, i, start, count):
    here = [ref[i, c, start : start + count] for c in range(2)]
    lane = lax.broadcasted_iota(jnp.int32, (count, 128), 1)
    left = [pltpu.roll(v, 1, 1) for v in here]
    right = [pltpu.roll(v, 127, 1) for v in here]
    along = (
        jnp.where(lane == 0, 0.0, left[0]) + jnp.where(lane == 127, right[1], right[0]),
        jnp.where(lane == 0, left[0], left[1]) + jnp.where(lane == 127, 0.0, right[1]),
    )
    around = []
    for c in range(2):
        planes = ref[i + 1, c, start : start + count] + ref[i - 1, c, start : start + count]
        rows = ref[i, c, start - 1 : start - 1 + count] + ref[i, c, start + 1 : start + 1 + count]
        around.append((planes + rows) + along[c])
    return here, around


def row_mask(ny):
    row = lax.broadcasted_iota(jnp.int32, (ny + 2 * ROWS, 128), 0)
    here, count = lax.axis_index("yz"), lax.axis_size("yz")
    low = jnp.where(here == 0, ROWS, 0)
    high = jnp.where(here == count - 1, ROWS + ny, 2 * ROWS + ny)
    return jnp.where((row >= low) & (row < high), 1.0, 0.0)


def over_inner(nx, skip, body):
    def inner(i, _):
        body(i, None)
        return 0

    lax.fori_loop(WIDE + skip, WIDE + nx - skip, inner, 0, unroll=next(n for n in (6, 5, 4, 3, 2, 1) if (nx - 2 * skip) % n == 0))


def over_wedges(nx, halo, skip, body):
    here, count = lax.axis_index("gx"), lax.axis_size("gx")
    below = jnp.where(here == 0, 0.0, 1.0)
    above = jnp.where(here == count - 1, 0.0, 1.0)
    for j in range(-halo, skip):
        body(WIDE + j, below if j < 0 else None)
        body(WIDE + nx - 1 - j, above if j < 0 else None)


def put(row, entries):
    lane = lax.broadcasted_iota(jnp.int32, row.shape, 1)
    most = functools.reduce(jnp.maximum, [jnp.abs(half) for _, halves_ in entries for half in halves_])
    unit = (8.0 * most.size) * jnp.max(most, keepdims=True)
    for at, pair in entries:
        rounded = [(half + unit) - unit for half in pair]
        high = jnp.sum(rounded[0] + rounded[1], keepdims=True)
        low = jnp.sum((pair[0] - rounded[0]) + (pair[1] - rounded[1]), keepdims=True)
        row = jnp.where(lane == at, high, jnp.where(lane == at + LOW_AT, low, row))
    return row


def clear_margins(refs):
    count, _, tall, _ = refs[0].shape
    side = jnp.zeros((2, PAD, 128), jnp.float32)

    def margins(i, _):
        for ref in refs:
            ref[i, :, :PAD] = side
            ref[i, :, tall - PAD :] = side
        return 0

    lax.fori_loop(0, count, margins, 0, unroll=2)


def recur(src, dst, scale, pull, first_step, rows):
    start, count = rows
    offset = start - PAD
    factor = pull[offset : offset + count]

    def body(i, mask):
        here, around = beside(src, i, start, count)
        weight = factor if mask is None else factor * mask
        made = []
        for c in range(2):
            at = (i, c, slice(start, start + count))
            twice = scale[at] * here[c] - weight * around[c]
            new = 0.5 * twice if first_step else twice - dst[at]
            dst[at] = new
            made.append(new)
        return made

    return body


def first_start(wide_u, va, scale, ny):
    keep = row_mask(ny)
    rows = (PAD, ny + 2 * ROWS)

    def body(i, mask):
        here, around = beside(wide_u, i, *rows)
        inside = keep if mask is None else keep * mask
        for c in range(2):
            at = (i, c, slice(PAD, PAD + rows[1]))
            damp = scale[at]
            va[at] = inside * (va[at] - (damp * here[c] + DIFFUSION * (6.0 * here[c] - around[c])))
            scale[at] = inside * ((2.0 / RADIUS) * (damp + (1.0 + 6.0 * DIFFUSION - CENTRE)))

    return body


def first_steps(ny, wide_u, va, vb, scale, basis, over, steps=range(HALF + 1)):
    pull = row_mask(ny) * (2.0 / RADIUS * DIFFUSION)
    rows = (PAD, ny + 2 * ROWS)
    begin = first_start(wide_u, va, scale, ny)

    def start(i, mask):
        begin(i, mask)
        if mask is None:
            basis[0, i - WIDE] = va[i, :, OWN : OWN + ny]

    if 0 in steps:
        over(HALF, 1, start)
    for k in range(HALF):
        if k + 1 not in steps:
            continue
        src, dst = (va, vb) if k % 2 == 0 else (vb, va)
        last = k == HALF - 1
        step = recur(src, dst, scale, pull, k == 0, (OWN, ny) if last else rows)

        def body(i, mask, step=step, k=k, last=last):
            made = step(i, mask)
            if mask is None:
                for c in range(2):
                    basis[k + 1, i - WIDE, c] = made[c] if last else made[c][ROWS : ROWS + ny]

        over(HALF - 1 - k, k + 2, body)


def first_own_kernel(u, f, d, wide_u, va, vb, scale):
    nx, ny, _ = u.shape
    clear_margins((wide_u, va, vb))
    for ref, dst in ((u, wide_u), (f, va), (d, scale)):
        for c in range(2):
            dst[WIDE : WIDE + nx, c, OWN : OWN + ny] = ref[:, :, c * 128 : (c + 1) * 128]


def first_inner_kernel(mine, theirs, *refs):
    wide_u, va, vb, scale, basis = refs[4:]
    _, nx, _, ny, _ = basis.shape
    level = lax.axis_index("level")
    for n, dst in enumerate((wide_u, va, scale)):
        for halo, place in ((mine, level), (theirs, 1 - level)):
            dst[WIDE : WIDE + nx, :, row_span(place, ny)] = halo[n * nx : (n + 1) * nx]
    over = lambda halo, skip, body: over_inner(nx, skip, body)
    first_steps(ny, wide_u, va, vb, scale, basis, over, range(FIRST_CUT))


def first_rest_kernel(*refs):
    wide_u, va, vb, scale, basis = refs[5:]
    _, nx, _, ny, _ = basis.shape
    over = lambda halo, skip, body: over_inner(nx, skip, body)
    first_steps(ny, wide_u, va, vb, scale, basis, over, range(FIRST_CUT, HALF + 1))


def first_outer_kernel(*refs):
    mine, theirs = refs[:2], refs[2:4]
    wide_u, va, vb, scale, basis, edge_rows, edge_planes = refs[9:]
    _, nx, _, ny, _ = basis.shape
    level = lax.axis_index("level")
    at = 0
    corner = WIDE + 2 * HALF
    for width, dst in ((WIDE, wide_u), (HALF, va), (HALF, scale)):
        for (planes, corners), place in ((mine, level), (theirs, 1 - level)):
            outer = row_span(place, ny)
            begin = WIDE - width + place * (nx + width)
            dst[pl.ds(begin, width), :, OWN : OWN + ny] = planes[at : at + width]
            dst[WIDE - width : WIDE, :, outer] = corners[at : at + width]
            dst[WIDE + nx : WIDE + nx + width, :, outer] = corners[corner + at : corner + at + width]
        at += width
    over = lambda halo, skip, body: over_wedges(nx, halo, skip, body)
    first_steps(ny, wide_u, va, vb, scale, basis, over)
    edge_rows[...] = by_level(basis[HALF, :, :, ny - ROWS :, :], basis[HALF, :, :, :ROWS, :])
    edge_planes[...] = by_level(basis[HALF, nx - HALF :], basis[HALF, :HALF])


def first_dots_kernel(u, basis, dots):
    count, nx, _, ny, _ = basis.shape
    row = jnp.zeros((8, 128), jnp.float32)
    entries = []
    for k in range(count):

        def body(i, sums, k=k):
            terms = [[] for _ in sums]
            for c in range(2):
                own = u[i, :, c * 128 : (c + 1) * 128]
                new = basis[k, i, c]
                parts = [own * new, new * new]
                if k == 0:
                    parts.append(own * own)
                else:
                    parts.append(basis[k - 1, i, c] * new)
                if k > 1:
                    parts.append(basis[k - 2, i, c] * new)
                for t, p in zip(terms, parts):
                    t.append(p)
            return tuple((s[0] + t[0], s[1] + t[1]) for s, t in zip(sums, terms))

        zero = jnp.zeros((ny, 128), jnp.float32)
        sums = lax.fori_loop(0, nx, body, ((zero, zero),) * (4 if k > 1 else 3), unroll=4)
        where = (FIELD_AT + 1 + k, 2 * k, FIELD_AT if k == 0 else 2 * k - 1, CHECK_AT + k - 1)
        entries += zip(where, sums)
    dots[...] = put(row, entries)


def second_step(j, ny, va, vb, scale, pull, u, first, basis):
    src, dst = (va, vb) if j % 2 == 0 else (vb, va)
    last = j == HALF - 1
    step = recur(src, dst, scale, pull, j == 0, (OWN, ny) if last else (PAD, ny + 2 * ROWS))
    k = HALF + j
    get = lambda n, i, c: first[n, i, c] if n <= HALF else basis[n - HALF - 1, i, c]

    def body(i, mask, sums):
        made = step(i, mask)
        if mask is not None:
            return sums
        at = i - WIDE
        result = [list(s) for s in sums]
        for c in range(2):
            mid = made[c] if last else made[c][ROWS : ROWS + ny]
            new = 2.0 * mid - first[HALF - 1 - j, at, c]
            parts = [get(k, at, c) * new, get(k - 1, at, c) * new]
            if not last:
                basis[j, at, c] = new
                parts += [new * new, u[at, :, c * 128 : (c + 1) * 128] * new]
            for r, p in zip(result, parts):
                r[c] = r[c] + p
        return tuple(tuple(r) for r in result)

    return body, 2 if last else 4


def second_own_kernel(first, dots, va, vb):
    _, nx, _, ny, _ = first.shape
    clear_margins((va, vb))
    va[WIDE : WIDE + nx, :, OWN : OWN + ny] = first[HALF]


def second_inner_kernel(mine, theirs, scale, u, first, *refs):
    basis, va, vb, sums = refs[2:]
    _, nx, _, ny, _ = basis.shape
    level = lax.axis_index("level")
    for halo, place in ((mine, level), (theirs, 1 - level)):
        outer = row_span(place, ny)
        va[WIDE : WIDE + nx, :, outer] = halo[...]
    second_inner_steps(range(SECOND_CUT), scale, u, first, basis, va, vb, sums)


def second_rest_kernel(scale, u, first, *refs):
    second_inner_steps(range(SECOND_CUT, HALF), scale, u, first, *refs[4:])


def second_inner_steps(steps, scale, u, first, basis, va, vb, sums):
    _, nx, _, ny, _ = basis.shape
    pull = row_mask(ny) * (2.0 / RADIUS * DIFFUSION)
    for j in steps:
        body, count = second_step(j, ny, va, vb, scale, pull, u, first, basis)
        zero = jnp.zeros((ny, 128), jnp.float32)
        low, high = WIDE + j + 1, WIDE + nx - j - 1
        run = lambda i, made, body=body: body(i, None, made)
        unroll = next(n for n in (6, 5, 4, 3, 2, 1) if (high - low) % n == 0)
        made = lax.fori_loop(low, high, run, ((zero, zero),) * count, unroll=unroll)
        for n in range(count):
            for c in range(2):
                sums[j, n, c] = made[n][c]


def second_outer_kernel(*refs):
    mine, theirs = refs[:2], refs[2:4]
    scale, u, first, before, sums = refs[4:9]
    basis, va, vb, dots = refs[12:]
    _, nx, _, ny, _ = basis.shape
    level = lax.axis_index("level")
    for (planes, corners), place in ((mine, level), (theirs, 1 - level)):
        outer = row_span(place, ny)
        va[pl.ds(WIDE - HALF + place * (nx + HALF), HALF), :, OWN : OWN + ny] = planes[...]
        va[WIDE - HALF : WIDE, :, outer] = corners[:HALF]
        va[WIDE + nx : WIDE + nx + HALF, :, outer] = corners[HALF:]
    pull = row_mask(ny) * (2.0 / RADIUS * DIFFUSION)
    entries = []
    for j in range(HALF):
        body, count = second_step(j, ny, va, vb, scale, pull, u, first, basis)
        made = [tuple(tuple(sums[j, n, c] for c in range(2)) for n in range(count))]

        def run(i, mask, body=body, made=made):
            made[0] = body(i, mask, made[0])

        over_wedges(nx, HALF - 1 - j, j + 1, run)
        k = HALF + j
        where = (2 * k + 1, CHECK_AT + k, 2 * k + 2, FIELD_AT + 2 + k)
        entries += zip(where, made[0])
    row = put(before[...], entries)
    dots[...] = jnp.broadcast_to(row[0:1], dots.shape)


def finish_kernel(gathered, tables, nodes, second, far_u, far_first, out, flag, u, first, arrived):
    nx, ny, _ = out.shape
    copies = [
        pltpu.make_async_copy(far_u, u, arrived.at[0]),
        pltpu.make_async_copy(far_first, first, arrived.at[1]),
    ]
    for copy in copies:
        copy.start()
    turned = gathered[...].T
    high, low = split_sum(turned[:LOW_AT], 1)
    high, low = two_sum(high, low + total(turned[LOW_AT:]))
    (lower, fine_low), (upper, fine_up) = coefficients(high, low, tables[...], nodes[...])
    level = lax.axis_index("level")
    part = jnp.where(level == 0, lower, upper)
    flag[0, 0] = jnp.where(jnp.min(jnp.where(fine_low & fine_up, 1.0, 0.0)) > 0.5, 1, 0)
    for copy in copies:
        copy.wait()
    factors = [jnp.broadcast_to(part[k : k + 1], (8, 128)) for k in range(TOP)]

    def body(i, _):
        for r in range(0, ny, 8):
            for c in range(2):
                value = u[i, r : r + 8, c * 128 : (c + 1) * 128]
                for k in range(TOP):
                    ref, n = (first, k) if k <= HALF else (second, k - HALF - 1)
                    value = value + factors[k] * ref[n, i, c, r : r + 8]
                out[i, r : r + 8, c * 128 : (c + 1) * 128] = value
        return 0

    lax.fori_loop(0, nx, body, 0, unroll=4)


def call(kernel, outs, args, limit=16 << 20, flags=(), alias=None, far=0, scratch=()):
    whole = pl.BlockSpec(memory_space=pltpu.VMEM)
    shapes = [jax.ShapeDtypeStruct(s, jnp.float32) for s in outs]
    near = len(args) - far
    args = tuple(args[:near]) + tuple(pltpu.with_memory_space_constraint(a, pltpu.HBM) for a in args[near:])
    return pl.pallas_call(
        kernel,
        out_shape=shapes + [jax.ShapeDtypeStruct(s, jnp.int32) for s in flags],
        in_specs=[whole] * near + [pl.BlockSpec(memory_space=pltpu.HBM)] * far,
        scratch_shapes=scratch,
        out_specs=[whole] * len(outs) + [pl.BlockSpec(memory_space=pltpu.SMEM)] * len(flags),
        input_output_aliases=alias or {},
        compiler_params=pltpu.CompilerParams(vmem_limit_bytes=limit),
    )(*args)


def both_ways(up, down, axis):
    size = lax.axis_size(axis)
    route = [(i, i + 1) for i in range(size - 1)]
    high = lax.ppermute(up, axis, route)
    low = lax.ppermute(down, axis, [(b, a) for a, b in route])
    return high, low


def stencil(field, damping):
    low, high = both_ways(field[-1:], field[:1], "gx")
    left, right = both_ways(field[:, -1:], field[:, :1], "yz")
    tall = jnp.concatenate([low, field, high], axis=0)
    long = jnp.concatenate([left, field, right], axis=1)
    zero = jnp.zeros_like(field[:, :, :1])
    near = tall[2:] + tall[:-2] + long[:, 2:] + long[:, :-2]
    near = near + jnp.concatenate([field[:, :, 1:], zero], axis=2) + jnp.concatenate([zero, field[:, :, :-1]], axis=2)
    return damping * field + DIFFUSION * (6.0 * field - near)


def dot(a, b):
    value = jnp.sum(a * b)
    for axis in AXES:
        value = lax.psum(value, axis)
    return value


def solve(target, guess, damping):
    resid = target - (guess + stencil(guess, damping))

    def step(_, state):
        answer, resid, direction, norm_now = state
        image = direction + stencil(direction, damping)
        alpha = norm_now / dot(direction, image)
        answer = answer + alpha * direction
        resid = resid - alpha * image
        norm_next = dot(resid, resid)
        return answer, resid, resid + (norm_next / norm_now) * direction, norm_next

    return lax.fori_loop(0, ITERS, step, (guess, resid, resid, dot(resid, resid)))[0]


def step_by_step(init_field, source, damping):
    def body(_, carry):
        lower, upper = carry
        fresh = solve(lower + source, lower, damping)
        extra = 0.5 * stencil(fresh - lower, damping)
        return fresh, solve(upper + source + extra, upper, damping)

    begin = jnp.minimum(init_field, jnp.finfo(jnp.float32).max)
    lower, upper = lax.fori_loop(0, STEPS, body, (begin, begin))
    return jnp.where(lax.axis_index("level") == 1, upper, lower)


def shifted(block, axis):
    size = lax.axis_size(axis)
    route = [(i, i + 1) for i in range(size - 1)] + [(size + i + 1, size + i) for i in range(size - 1)]
    return lax.ppermute(block, ("level", axis), route)


def swapped(block):
    return lax.ppermute(block, "level", [(0, 1), (1, 0)])


def exchange(rows, planes):
    planes = shifted(planes, "gx")
    halo = shifted(rows, "yz")
    others = swapped(planes)
    width = planes.shape[0]
    (corners,) = call(pack_corners_kernel, [(2 * width, 2, ROWS, 128)], (planes, others))
    corners = shifted(corners, "yz")
    theirs = swapped(halo)
    opposite = swapped(corners)
    return halo, theirs, (planes, corners, others, opposite)


def per_device(u, f, d):
    nx, ny, nz = u.shape
    tall = 2 * ROWS + ny
    deep = WIDE + 2 * HALF
    rows, planes = call(
        pack_first_kernel,
        [(3 * nx, 2, ROWS, 128), (deep, 2, ny, 128)],
        (u, f, d),
        far=3,
        scratch=[
            pltpu.VMEM((3, nx, ROWS, nz), jnp.float32),
            pltpu.VMEM((3, WIDE, ny, nz), jnp.float32),
            pltpu.SemaphoreType.DMA((6,)),
        ],
    )
    halo, theirs, outside = exchange(rows, planes)
    wide = (nx + 2 * WIDE, 2, tall + 2 * PAD, 128)
    block = (nx, 2, ny, 128)
    own = call(first_own_kernel, [wide] * 4, (u, f, d))
    args = (halo, theirs) + tuple(own)
    shapes = [wide] * 4 + [(HALF + 1,) + block]
    buffers = call(first_inner_kernel, shapes, args, alias={2 + n: n for n in range(4)})
    shapes = [b.shape for b in buffers]
    buffers = call(first_rest_kernel, shapes, buffers, alias={n: n for n in range(5)})
    *_, scale, first, rows, planes = call(
        first_outer_kernel,
        [wide] * 4 + [(HALF + 1,) + block, (nx, 2, ROWS, 128), (HALF, 2, ny, 128)],
        outside + tuple(buffers),
        alias={4 + n: n for n in range(5)},
    )
    halo, theirs, outside = exchange(rows, planes)
    (dots,) = call(first_dots_kernel, [(8, 128)], (u, first))
    own = call(second_own_kernel, [wide] * 2, (first, dots))
    buffers = call(
        second_inner_kernel,
        [(HALF - 1,) + block, wide, wide, (HALF, 4, 2, ny, 128)],
        (halo, theirs, scale, u, first) + tuple(own),
        alias={5: 1, 6: 2},
    )
    shapes = [b.shape for b in buffers]
    args = (scale, u, first) + tuple(buffers)
    second, va, vb, sums = call(second_rest_kernel, shapes, args, alias={3 + n: n for n in range(4)})
    parts = lax.axis_size(AXES)
    second, _, _, dots = call(
        second_outer_kernel,
        [(HALF - 1,) + block, wide, wide, (parts, 128)],
        outside + (scale, u, first, dots, sums, second, va, vb),
        alias={9: 0, 10: 1, 11: 2},
    )
    gathered = lax.all_to_all(dots.reshape(parts, 1, 128), AXES, 0, 0).reshape(parts, 128)
    tables, nodes = chebyshev_tables()
    fast, flag = call(
        finish_kernel,
        [(nx, ny, nz)],
        (gathered, jnp.asarray(tables), jnp.asarray(nodes), second, u, first),
        flags=[(1, 1)],
        far=2,
        scratch=[
            pltpu.VMEM((nx, ny, nz), jnp.float32),
            pltpu.VMEM((HALF + 1,) + block, jnp.float32),
            pltpu.SemaphoreType.DMA((2,)),
        ],
    )
    state = lax.cond(flag.reshape(()), lambda: fast, lambda: step_by_step(u, f, d))
    return state[None]


def solution(mesh):
    placed = P("gx", "yz", None)
    return jax.shard_map(
        per_device,
        mesh=mesh,
        in_specs=(placed, placed, placed),
        out_specs=P("level", "gx", "yz", None),
        check_vma=False,
    )
```
